256 devices in a mesh: dp: 16 (over y_hi, x, core), mp: 16 (over z, y_lo).
Axes of the slice: x: 4, y: 4 (y_hi: 2, y_lo: 2; y = y_hi * 2 + y_lo), z: 8, core: 2. Of those that a mesh axis runs over, the one named last changes fastest.
Arguments:
- tokens: bfloat16 [8192, 8192], P(('dp', 'mp')), parts along dimension 0, may hold values from -6 to 6
- norm_gain: float32 [8192], replicated, may hold values from 0.5 to 1.5
- qkv_weight: bfloat16 [8192, 10240], P(None, 'mp'), may hold values from -0.0625 to 0.0625
- qkv_bias: float32 [10240], P('mp'), may hold values from -3 to 3
- qkv_grad: bfloat16 [8192, 10240], P('dp', 'mp'), parts along dimension 0, may hold values from -6 to 6
Outputs:
- qkv: bfloat16 [8192, 10240], P('dp', 'mp'), parts along dimension 0
- tokens_grad: float32 [8192, 8192], P(('dp', 'mp')), parts along dimension 0
- gain_grad: float32 [131072], P('dp'), parts along dimension 0
- bias_grad: float32 [163840], P(('dp', 'mp')), parts along dimension 0
The draws below stay inside these ranges and needn't reach their ends.
There are 16 independent parts, one for each index of `dp`. The reference program is written for one: setup_inputs(seed, part) draws one part's arguments, and reference() takes and returns one part's arrays. A program takes and returns all parts, laid end to end along the dimension named above; an argument that names none is the same for every part. Nothing has to cross between parts.
All inputs are finite; a program needn't handle non-finite values.
Results may differ from the reference program's by a relative error of at most 0.0046.
Values may be sent and summed in bfloat16 or wider, within the bound.
A program may use at most 128 MiB of HBM per device.

```python
import jax
import jax.numpy as jnp
from jax import lax

D = 8192
HEAD_DIM = 128
GROUP = 10
COLS = 10240
STRIDE = 2048
TOK_DEV = 32
TOKENS = 512


def strengthened(values, own_key, source, target, shards_of, factor):
    def block_of(axis_at):
        return (jnp.arange(values.shape[axis_at]) // (values.shape[axis_at] // shards_of)).reshape((-1,) + (1,) * (values.ndim - 1 - axis_at))

    first = jax.random.permutation(own_key, shards_of)[block_of(target)]
    far = (block_of(target) + shards_of // 2) % shards_of
    return jnp.where((block_of(source) == first) | (block_of(source) == far), factor * values, values)


def shard_levels(stream_key, shape, cuts, smallest, top_value):
    def one(axis_at, blocks):
        heights = jax.random.uniform(jax.random.fold_in(jax.random.fold_in(stream_key, 6), axis_at), (blocks,), jnp.float32, smallest / len(cuts), top_value / len(cuts))
        return jnp.repeat(jnp.exp(heights), shape[axis_at] // blocks).reshape((-1,) + (1,) * (len(shape) - axis_at - 1))

    factor_of = one(*cuts[0])
    for cut in cuts[1:]:
        factor_of = factor_of * one(*cut)
    return factor_of


def gaussian(own_key, dims, deviation, bound, shards=(), kind=jnp.bfloat16):
    array = deviation * jax.random.normal(own_key, dims, jnp.float32)
    if shards:
        array = array * shard_levels(own_key, dims, shards, -0.22, 0.18)
    return jnp.clip(array, -bound, bound).astype(kind)


def gaussian_with(stream_key, extent, deviation, limit, cuts, heavy, kind=jnp.bfloat16):
    array = deviation * jax.random.normal(stream_key, extent, jnp.float32)
    if cuts:
        array = array * shard_levels(stream_key, extent, cuts, -0.22, 0.18)
    return jnp.clip(strengthened(array, jax.random.fold_in(stream_key, 3), *heavy), -limit, limit).astype(kind)


def setup_inputs(seed: int = 0, part: int = 0) -> dict:
    key_list = jax.random.split(jax.random.key(seed), 6)
    part_keys = jax.random.split(jax.random.fold_in(key_list[5], part), 6)
    return {
        "tokens": gaussian(part_keys[0], (TOKENS, D), 1.0, 6.0, ((0, 16),)),
        "norm_gain": jnp.clip(1.0 + 0.1 * jax.random.normal(key_list[1], (D,), jnp.float32), 0.5, 1.5),
        "qkv_weight": gaussian(key_list[2], (D, COLS), D ** -0.5, 0.0625, ((1, 16),)),
        "qkv_bias": gaussian(key_list[3], (COLS,), 0.5, 3.0, ((0, 16),), jnp.float32),
        "qkv_grad": gaussian_with(part_keys[4], (TOKENS, COLS), 1.0, 6.0, ((1, 16),), (1, 0, 16, 2.0)),
    }


def rotate_heads(joined, first_col, position, sign):
    rows, cols = joined.shape
    heads = cols // HEAD_DIM
    half = HEAD_DIM // 2
    parts = joined.reshape(rows, heads, 2, half)
    inverse = jnp.exp(-jnp.log(jnp.float32(1000000.0)) * (2.0 * jnp.arange(half).astype(jnp.float32) / HEAD_DIM))
    angle = position.astype(jnp.float32)[:, None] * inverse[None, :]
    cosine = jnp.cos(angle)[:, None, :]
    sine = sign * jnp.sin(angle)[:, None, :]
    first = parts[:, :, 0, :]
    second = parts[:, :, 1, :]
    turned = jnp.stack([first * cosine - second * sine, second * cosine + first * sine], axis=2)
    head_index = first_col // HEAD_DIM + jnp.arange(heads)
    rotated = head_index % GROUP != GROUP - 1
    result = jnp.where(rotated[None, :, None, None], turned, parts)
    return result.reshape(rows, cols)

def reference(tokens, norm_gain, qkv_weight, qkv_bias, qkv_grad):
    row_index = jnp.arange(TOKENS).astype(jnp.int32)
    position = row_index // TOK_DEV * STRIDE + row_index % TOK_DEV
    values = tokens.astype(jnp.float32)
    scale = lax.rsqrt(lax.optimization_barrier(jnp.mean(values * values, axis=1, keepdims=True)) + 1e-06)
    normed = (values * scale * norm_gain[None, :]).astype(jnp.bfloat16)
    joined = jnp.dot(normed, qkv_weight, preferred_element_type=jnp.float32) + qkv_bias[None, :]
    qkv = rotate_heads(joined, 0, position, 1.0).astype(jnp.bfloat16)
    joined_grad = rotate_heads(qkv_grad.astype(jnp.float32), 0, position, -1.0)
    bias_grad = lax.optimization_barrier(jnp.sum(joined_grad, axis=0))
    joined_low = joined_grad.astype(jnp.bfloat16)
    normed_grad = lax.dot_general(joined_low, qkv_weight, (((1,), (1,)), ((), ())), preferred_element_type=jnp.float32)
    gain_grad = lax.optimization_barrier(jnp.sum(normed_grad * values * scale, axis=0))
    inner = lax.optimization_barrier(jnp.mean(norm_gain[None, :] * normed_grad * values, axis=1, keepdims=True))
    tokens_grad = scale * norm_gain[None, :] * normed_grad - values * scale * scale * scale * inner
    return (qkv, tokens_grad, gain_grad, bias_grad)
```

```python
import functools

import jax
import jax.numpy as jnp
import numpy as np
from jax import lax
from jax.experimental import pallas as pl
from jax.experimental.pallas import tpu as pltpu
from jax.sharding import PartitionSpec as P

HEAD_DIM = 128
SEQ_LEN = 32768
GROUP = 10
MESH = pl.DeviceIdType.MESH
CHUNK = 512
WCHUNK = 256
TILE_N = 256


def rope_tables(rows, tok_dev, stride):
    half = HEAD_DIM // 2
    row = np.arange(rows)
    place = (row // tok_dev * stride + row % tok_dev).astype(np.float32)
    inverse = np.exp(
        -np.log(np.float32(1000000.0))
        * (np.float32(2.0) * np.arange(half).astype(np.float32) / np.float32(HEAD_DIM))
    ).astype(np.float32)
    angle = (place[:, None] * inverse[None, :]).astype(np.float32)
    cosine, sine = np.cos(angle).astype(np.float32), np.sin(angle).astype(np.float32)

    def by_column(t):
        t = t.reshape(rows // (2 * tok_dev), 2, tok_dev, HEAD_DIM)
        return np.ascontiguousarray(np.swapaxes(t, 0, 1)).reshape(2, rows // 2, HEAD_DIM)

    return by_column(np.concatenate([cosine, cosine], 1)), by_column(np.concatenate([-sine, sine], 1))


def kernel(
    nz, ndp,
    tok_h, gain_h, w_h, bias_h, grad_h, cos_h, sin_h,
    qkv, tg, gg_ref, bg_ref,
    tok, gain, w, bias, grad, cos, sin,
    low, lowx, nx, held, part, run, acc, cx, qt, qx, ng, fin, gtot, gx, grecv, gres, bacc,
    in_sem, w_sem, wx_s, wx_r, nx_s, nx_r, low_s, low_r, bias_s, bias_r,
    ag_s, ag_r, rs_s, rs_r, fin_s, fin_r, c_s, c_r, q_s, q_r,
    gx_s, gx_r, g1_s, g1_r, g2_s, g2_r,
):
    f32, bf16 = jnp.float32, jnp.bfloat16
    dp, mp = lax.axis_index("dp"), lax.axis_index("mp")
    n = 2 * nz
    z, yl, core = mp // 2, lax.rem(mp, 2), lax.rem(dp, 2)
    rows, depth = tok.shape
    half = depth // 2
    col = nz * rows
    width = grad.shape[1]
    heads = width // HEAD_DIM
    chunks = half // CHUNK
    wchunks = half // WCHUNK
    quarter = half // 4
    slab = depth // n

    def at(start, size, unit):
        return pl.ds(pl.multiple_of(start, unit), size)

    up = {"mp": lax.rem(z + 1, nz) * 2 + yl}
    down = {"mp": lax.rem(z + nz - 1, nz) * 2 + yl}
    pair = {"mp": mp + 1 - 2 * yl}
    far = {"dp": lax.rem(dp + ndp // 2, ndp), "mp": mp + 1 - 2 * yl}
    twin = {"dp": dp + 1 - 2 * core}
    along = (up, down)

    barrier = pltpu.get_barrier_semaphore()
    for there in (up, down, pair, far, twin):
        pl.semaphore_signal(barrier, inc=1, device_id=there, device_id_type=MESH)

    loads = []
    for i, (src, dst) in enumerate((
        (tok_h, tok), (gain_h, gain.at[0]), (grad_h, grad), (cos_h, cos), (sin_h, sin),
        (bias_h, bias.at[0, pl.ds(0, width)]),
    )):
        c = pltpu.make_async_copy(src, dst, in_sem.at[i])
        c.start()
        loads.append(c)

    def w_load(k):
        return pltpu.make_async_copy(
            w_h.at[at(core * half + k * CHUNK, CHUNK, CHUNK), :],
            w.at[at(k * CHUNK, CHUNK, CHUNK), pl.ds(0, width)],
            w_sem.at[k],
        )

    @pl.loop(0, chunks)
    def _(k):
        w_load(k).start()

    def remote(src, dst, send, recv, there):
        return pltpu.make_async_remote_copy(
            src_ref=src, dst_ref=dst, send_sem=send, recv_sem=recv, device_id=there, device_id_type=MESH
        )

    def w_send(i, there):
        return remote(
            w_h.at[at(core * half + i * WCHUNK, WCHUNK, WCHUNK), :],
            w.at[at(i * WCHUNK, WCHUNK, WCHUNK), pl.ds(width, width)],
            wx_s.at[i], wx_r.at[i], there,
        )

    mine = at(core * col, col, col)
    other = at((1 - core) * col, col, col)
    home = at(core * col + z * rows, rows, rows)

    def nx_send(q):
        ks = pl.ds(q * quarter, quarter)
        return remote(nx.at[:, ks], held.at[home, ks], nx_s.at[q], nx_r.at[q], twin)

    def ag(way, j, e):
        d = lax.rem(core + e // 4, 2)
        b = lax.rem(z + (nz - j if way == 0 else j), nz)
        ref = held.at[at(d * col + b * rows, rows, rows), at(lax.rem(e, 4) * quarter, quarter, quarter)]
        return remote(ref, ref, ag_s.at[way, j, e], ag_r.at[way, j, e], along[way])

    loads[0].wait()
    loads[1].wait()
    total = jnp.zeros((rows, 1), f32)
    for q in range(8):
        v = tok[:, q * quarter:(q + 1) * quarter].astype(f32)
        total = total + jnp.sum(v * v, axis=1, keepdims=True)
    scale = lax.rsqrt(total / depth + 1e-06)

    def normed(ks):
        return (tok[:, ks].astype(f32) * scale * gain[:, ks]).astype(bf16)

    for q in range(4):
        held[home, q * quarter:(q + 1) * quarter] = normed(at(core * half + q * quarter, quarter, quarter))
    pl.semaphore_wait(barrier, 5)
    for q in range(4):
        for way in range(2):
            ag(way, 0, q).start()
    remote(
        bias_h, bias.at[0, pl.ds(width, width)], bias_s.at[0], bias_r.at[0], pair
    ).start()
    for q in range(4):
        nx[:, q * quarter:(q + 1) * quarter] = normed(at((1 - core) * half + q * quarter, quarter, quarter))
        nx_send(q).start()

    @pl.loop(0, wchunks)
    def _(i):
        @pl.when((i == 0) | (lax.rem(i, 2) == 1))
        def _():
            w_send(i, far).start()

    for l in loads[2:]:
        l.wait()
    bacc[...] = jnp.zeros_like(bacc)

    @pl.loop(0, nz)
    def _(b):
        for side, y in ((0, yl), (1, 1 - yl)):
            here = at((2 * b + y) * rows, rows, rows)
            there = at(b * rows, rows, rows)
            cs, sn = cos[y, there, :], sin[y, there, :]
            for h in range(heads):
                hs = slice(h * HEAD_DIM, (h + 1) * HEAD_DIM)
                x = grad[here, hs].astype(f32)
                turned = x * cs - pltpu.roll(x, HEAD_DIM // 2, 1) * sn
                plain = lax.rem(mp * heads + h, GROUP) == GROUP - 1
                x = jnp.where(plain, x, turned)
                bacc[:, hs] += jnp.sum(x.reshape(rows // 8, 8, HEAD_DIM), axis=0)
                if side == 0:
                    low[at(core * col + b * rows, rows, rows), hs] = x.astype(bf16)
                else:
                    lowx[there, hs] = x.astype(bf16)

    own_cols, pair_cols = pl.ds(0, width), pl.ds(width, width)
    low_pair = remote(lowx, low.at[mine, pair_cols], low_s.at[0], low_r.at[0], pair)
    low_twin = remote(low.at[mine, own_cols], low.at[mine, own_cols], low_s.at[1], low_r.at[1], twin)
    low_fwd = remote(low.at[mine, pair_cols], low.at[mine, pair_cols], low_s.at[2], low_r.at[2], twin)
    low_pair.start()
    low_twin.start()
    for q in range(4):
        nx_send(q).wait_recv()
        for way in range(2):
            ag(way, 0, 4 + q).start()

    @pl.loop(0, wchunks)
    def _(i):
        @pl.when((i > 0) & (lax.rem(i, 2) == 0))
        def _():
            w_send(i, pair).start()

    bg_ref[...] = jnp.sum(bacc[...], axis=0, keepdims=True)

    def cols(k):
        return at(k * CHUNK, CHUNK, CHUNK)

    def backward(k):
        w_send(2 * k, pair).wait_recv()
        w_send(2 * k + 1, pair).wait_recv()
        part[:, cols(k)] = lax.dot_general(
            low[...], w[cols(k), :], (((1,), (1,)), ((), ())), preferred_element_type=f32
        )

    def hops(way, k):
        return jnp.where(lax.rem(k, 2) == way, 4, 3)

    def rs(way, j, k):
        return remote(
            run.at[way, j, :, cols(k)], run.at[way, j + 1, :, cols(k)],
            rs_s.at[way, j, k], rs_r.at[way, j, k], along[way],
        )

    def rs_step(way, j, k):
        left = hops(way, k) - j
        t = lax.rem(z + (left if way == 0 else nz - left), nz)
        if j > 0:
            rs(way, j - 1, k).wait_recv()
        for d in range(2):
            ds = pl.ds(d * rows, rows)
            v = part[at(d * col + t * rows, rows, rows), cols(k)]
            if j > 0:
                v = v + run[way, j, ds, cols(k)].astype(f32)
            run[way, j, ds, cols(k)] = v.astype(bf16)
        rs(way, j, k).start()

    def fin_send(k):
        return remote(
            fin.at[:, cols(k)], ng.at[:, at(core * half + k * CHUNK, CHUNK, CHUNK)], fin_s.at[k], fin_r.at[k], twin
        )

    def rs_final(k):
        for way in range(2):
            rs(way, hops(way, k) - 1, k).wait_recv()
        for d, to in ((core, None), (1 - core, fin)):
            ds = at(d * rows, rows, rows)
            v = part[at(d * col + z * rows, rows, rows), cols(k)]
            for way in range(2):
                v = v + run[way, hops(way, k), ds, cols(k)].astype(f32)
            if to is None:
                ng[:, at(core * half + k * CHUNK, CHUNK, CHUNK)] = v
            else:
                fin[:, cols(k)] = v
        fin_send(k).start()

    def gain_share(k):
        full = at(core * half + k * CHUNK, CHUNK, CHUNK)
        for ds, to, ks in ((mine, gtot, full), (other, gx, cols(k))):
            share = jnp.sum(part[ds, cols(k)] * held[ds, cols(k)].astype(f32), axis=0, keepdims=True)
            to[:, ks] = share / gain[:, full]

    gx_send = remote(gx, gtot.at[:, at(core * half, half, half)], gx_s.at[0], gx_r.at[0], twin)

    def slab_of(i):
        return at(i * slab, slab, slab)

    def g1(k):
        to = lax.rem(mp + k, n)
        return remote(gtot.at[:, slab_of(to)], grecv.at[k - 1], g1_s.at[k - 1], g1_r.at[k - 1], {"mp": to})

    def g2(k):
        to = lax.rem(mp + k, n)
        return remote(
            gres.at[:, slab_of(mp)], gres.at[:, slab_of(mp)], g2_s.at[k - 1], g2_r.at[k - 1], {"mp": to}
        )

    def tile(t):
        return at(t * TILE_N, TILE_N, TILE_N)

    def c_send(t):
        return remote(acc.at[other, tile(t)], cx.at[:, tile(t)], c_s.at[t], c_r.at[t], twin)

    def forward(t):
        acc[:, tile(t)] = jnp.dot(held[...], w[:, tile(t)], preferred_element_type=f32)
        c_send(t).start()

    def q_send(h):
        return remote(
            qt.at[:, at(width + h * HEAD_DIM, HEAD_DIM, HEAD_DIM)], qx.at[:, at(h * HEAD_DIM, HEAD_DIM, HEAD_DIM)],
            q_s.at[h], q_r.at[h], pair,
        )

    def joined(t):
        c_send(t).wait_recv()
        for i in range(TILE_N // HEAD_DIM):
            h = t * (TILE_N // HEAD_DIM) + i
            hs = at(h * HEAD_DIM, HEAD_DIM, HEAD_DIM)
            x = acc[mine, hs] + cx[:, hs] + bias[:, hs]
            turned = x * cos[yl] + pltpu.roll(x, HEAD_DIM // 2, 1) * sin[yl]
            whole = jnp.where(h < heads, mp * heads + h, (mp + 1 - 2 * yl) * heads + h - heads)
            qt[:, hs] = jnp.where(lax.rem(whole, GROUP) == GROUP - 1, x, turned).astype(bf16)

            @pl.when(h >= heads)
            def _():
                q_send(h - heads).start()

    @pl.loop(0, 24)
    def _(i):
        j, e = 1 + i // 8, lax.rem(i, 8)
        for way in range(2):
            ag(way, j - 1, e).wait_recv()

            @pl.when((j < 3) | (lax.rem(e, 2) == way))
            def _():
                ag(way, j, e).start()

        @pl.when(i == 5)
        def _():
            low_pair.wait_recv()
            low_fwd.start()

        @pl.when(i == 7)
        def _():
            for k in range(chunks):
                w_load(k).wait()
            low_twin.wait_recv()
            low_fwd.wait_recv()

        @pl.when((i == 8) | (i == 12) | (i == 17) | (i == 22))
        def _():
            backward((i - 8) // 4)

    for k in range(2):
        for way in range(2):
            rs_step(way, 0, k)
    for e in range(8):
        ag(e % 2, 3, e).wait_recv()
    bias_wait = remote(bias_h, bias.at[0, pl.ds(width, width)], bias_s.at[0], bias_r.at[0], pair)
    bias_wait.wait_recv()
    for k in range(2):
        gain_share(k)

    @pl.loop(0, chunks + 3)
    def _(s):
        k3, k2, k1, k0 = s - 2, s - 1, s, s + 2

        for way in range(2):
            @pl.when((k3 >= 0) & (k3 < chunks) & (lax.rem(k3 + 2, 2) == way))
            def _():
                rs_step(way, 3, k3)

        for k, j in ((k2, 2), (k1, 1)):
            @pl.when((k >= 0) & (k < chunks))
            def _():
                for way in range(2):
                    rs_step(way, j, k)

        @pl.when((k0 >= 4) & (k0 < chunks))
        def _():
            backward(k0)

        @pl.when(k0 < chunks)
        def _():
            for way in range(2):
                rs_step(way, 0, k0)
            gain_share(k0)

        @pl.when(k0 == chunks - 1)
        def _():
            gx_send.start()

        @pl.when(s >= 3)
        def _():
            rs_final(s - 3)

        @pl.when((s == 2) | (s == 3) | ((s >= 6) & (s <= 8)))
        def _():
            joined(jnp.where(s < 4, s - 2, s - 4))

        @pl.when((s == 1) | (s == 2) | ((s >= 5) & (s <= 7)))
        def _():
            forward(jnp.where(s < 4, s - 1, s - 3))

        @pl.when(s == 6)
        def _():
            gx_send.wait_recv()
            for k in range(1, n):
                g1(k).start()

        @pl.when(s == 8)
        def _():
            share = gtot[:, slab_of(mp)]
            for k in range(1, n):
                g1(k).wait_recv()
                share = share + grecv[k - 1]
            gres[:, slab_of(mp)] = share
            for k in range(1, n):
                g2(k).start()

    for h in range(heads):
        q_send(h).wait_recv()
    for b in range(nz):
        there = pl.ds(b * rows, rows)
        qkv[at((2 * b + yl) * rows, rows, rows), :] = qt[there, pl.ds(0, width)]
        qkv[at((2 * b + 1 - yl) * rows, rows, rows), :] = qx[there, :]
    for k in range(1, n):
        g2(k).wait_recv()
    gg_ref[...] = gres[...]

    for k in range(chunks):
        fin_send(k).wait_recv()
    inner = jnp.zeros((rows, 1), f32)
    for q in range(8):
        ks = slice(q * quarter, (q + 1) * quarter)
        inner = inner + jnp.sum(ng[:, ks] * tok[:, ks].astype(f32) * gain[:, ks], axis=1, keepdims=True)
    weight = scale * scale * scale * (inner / depth)
    for q in range(8):
        ks = slice(q * quarter, (q + 1) * quarter)
        tg[:, ks] = scale * gain[:, ks] * ng[:, ks] - tok[:, ks].astype(f32) * weight

    bias_wait.wait_send()
    low_pair.wait_send()
    low_twin.wait_send()
    low_fwd.wait_send()
    gx_send.wait_send()
    for q in range(4):
        nx_send(q).wait_send()

    @pl.loop(0, wchunks)
    def _(i):
        w_send(i, pair).wait_send()

    @pl.loop(0, 4)
    def _(j):
        @pl.loop(0, 8)
        def _(e):
            for way in range(2):
                @pl.when((j < 3) | (lax.rem(e, 2) == way))
                def _():
                    ag(way, j, e).wait_send()
                    rs(way, j, e).wait_send()

    for k in range(chunks):
        fin_send(k).wait_send()
    for t in range(2 * width // TILE_N):
        c_send(t).wait_send()
    for h in range(heads):
        q_send(h).wait_send()
    for k in range(1, n):
        g1(k).wait_send()
        g2(k).wait_send()


def finish(qkv, tg, gg, bg, qkv_h, tg_h, gg_h, bg_h, sem):
    moves = ((qkv, qkv_h), (tg, tg_h), (gg.at[0], gg_h), (bg.at[0], bg_h))
    copies = [pltpu.make_async_copy(src, dst, sem.at[i]) for i, (src, dst) in enumerate(moves)]
    for c in copies:
        c.start()
    for c in copies:
        c.wait()


def shards(n, ndp, tokens, norm_gain, qkv_weight, qkv_bias, qkv_grad):
    rows, depth = tokens.shape
    every, width = qkv_grad.shape
    cosine, sine = rope_tables(every, rows, SEQ_LEN // n)
    bf16, f32 = jnp.bfloat16, jnp.float32
    half, col, nz = depth // 2, every // 2, n // 2
    chunks, wchunks, heads = half // CHUNK, half // WCHUNK, width // HEAD_DIM
    tiles = 2 * width // TILE_N
    dma = pltpu.SemaphoreType.DMA
    vm = pltpu.VMEM
    hbm = pl.BlockSpec(memory_space=pl.ANY)
    vmem = pl.BlockSpec(memory_space=pltpu.VMEM)
    results = pl.pallas_call(
        functools.partial(kernel, nz, ndp),
        out_shape=(
            vm((every, width), bf16),
            vm((rows, depth), f32),
            vm((1, depth), f32),
            vm((1, width), f32),
        ),
        in_specs=[hbm] * 7,
        out_specs=[vmem] * 4,
        scratch_shapes=[
            vm((rows, depth), bf16),
            vm((1, depth), f32),
            vm((half, 2 * width), bf16),
            vm((1, 2 * width), f32),
            vm((every, width), bf16),
            vm((2, col, HEAD_DIM), f32),
            vm((2, col, HEAD_DIM), f32),
            vm((every, 2 * width), bf16),
            vm((col, width), bf16),
            vm((rows, half), bf16),
            vm((every, half), bf16),
            vm((every, half), f32),
            vm((2, 5, 2 * rows, half), bf16),
            vm((every, 2 * width), f32),
            vm((col, 2 * width), f32),
            vm((col, 2 * width), bf16),
            vm((col, width), bf16),
            vm((rows, depth), f32),
            vm((rows, half), f32),
            vm((1, depth), f32),
            vm((1, half), f32),
            vm((n - 1, 1, depth // n), f32),
            vm((1, depth), f32),
            vm((8, width), f32),
            dma((6,)), dma((chunks,)),
            dma((wchunks,)), dma((wchunks,)),
            dma((4,)), dma((4,)),
            dma((3,)), dma((3,)),
            dma((1,)), dma((1,)),
            dma((2, 4, 8)), dma((2, 4, 8)),
            dma((2, 4, chunks)), dma((2, 4, chunks)),
            dma((chunks,)), dma((chunks,)),
            dma((tiles,)), dma((tiles,)),
            dma((heads,)), dma((heads,)),
            dma((1,)), dma((1,)),
            dma((n - 1,)), dma((n - 1,)),
            dma((n - 1,)), dma((n - 1,)),
        ],
        compiler_params=pltpu.CompilerParams(
            collective_id=0, has_side_effects=True, vmem_limit_bytes=60000000
        ),
        cost_estimate=pl.CostEstimate(
            flops=4 * every * depth * width, bytes_accessed=2 * depth * width, transcendentals=0
        ),
    )(
        tokens, norm_gain, qkv_weight, qkv_bias, qkv_grad,
        jnp.asarray(cosine), jnp.asarray(sine),
    )
    return pl.pallas_call(
        finish,
        out_shape=(
            jax.ShapeDtypeStruct((every, width), bf16),
            jax.ShapeDtypeStruct((rows, depth), f32),
            jax.ShapeDtypeStruct((depth,), f32),
            jax.ShapeDtypeStruct((width,), f32),
        ),
        in_specs=[vmem] * 4,
        out_specs=[hbm] * 4,
        scratch_shapes=[dma((4,))],
        compiler_params=pltpu.CompilerParams(vmem_limit_bytes=1 << 20),
    )(*results)


def solution(mesh):
    in_specs = (P(("dp", "mp"), None), P(), P(None, "mp"), P("mp"), P("dp", "mp"))
    out_specs = (P("dp", "mp"), P(("dp", "mp"), None), P("dp"), P(("dp", "mp")))
    body = functools.partial(shards, mesh.shape["mp"], mesh.shape["dp"])
    return jax.shard_map(body, mesh=mesh, in_specs=in_specs, out_specs=out_specs, check_vma=False)
```

```python
import functools

import jax
import jax.numpy as jnp
import numpy as np
from jax import lax
from jax.experimental import pallas as pl
from jax.experimental.pallas import tpu as pltpu
from jax.sharding import PartitionSpec as P

HEAD_DIM = 128
SEQ_LEN = 32768
GROUP = 10
MESH = pl.DeviceIdType.MESH
CHUNK = 512
WCHUNK = 256
TILE_N = 256


def rope_tables(rows, tok_dev, stride):
    half = HEAD_DIM // 2
    row = np.arange(rows)
    place = (row // tok_dev * stride + row % tok_dev).astype(np.float32)
    inverse = np.exp(
        -np.log(np.float32(1000000.0))
        * (np.float32(2.0) * np.arange(half).astype(np.float32) / np.float32(HEAD_DIM))
    ).astype(np.float32)
    angle = (place[:, None] * inverse[None, :]).astype(np.float32)
    cosine, sine = np.cos(angle).astype(np.float32), np.sin(angle).astype(np.float32)

    def by_column(t):
        t = t.reshape(rows // (2 * tok_dev), 2, tok_dev, HEAD_DIM)
        return np.ascontiguousarray(np.swapaxes(t, 0, 1)).reshape(2, rows // 2, HEAD_DIM)

    return np.stack([by_column(np.concatenate([cosine, cosine], 1)), by_column(np.concatenate([-sine, sine], 1))])


def kernel(
    nz, ndp,
    tok_h, gain_h, w_h, bias_h, grad_h, rope_h,
    qkv, tg, gg_ref, bg_ref,
    tok, gain, w, bias, grad, rope,
    low, lowx, nx, held, part, run, acc, cx, qt, qx, ng, fin, gtot, gx, grecv, gres, bacc,
    in_sem, send_sem, one_sem, low_r, wy_r, wx_r, ag_r, rs_r, c_r,
):
    f32, bf16 = jnp.float32, jnp.bfloat16
    dp, mp = lax.axis_index("dp"), lax.axis_index("mp")
    n = 2 * nz
    z, yl, core = mp // 2, lax.rem(mp, 2), lax.rem(dp, 2)
    nx_chips = ndp // 4
    row_of_x = dp // (2 * nx_chips) * (2 * nx_chips)
    x = lax.rem(dp // 2, nx_chips)
    odd = lax.rem(x, 2)
    rows, depth = tok.shape
    half = depth // 2
    col = nz * rows
    width = grad.shape[1]
    heads = width // HEAD_DIM
    chunks = half // CHUNK
    quarter = half // 4
    slab = depth // n

    def at(start, size, unit):
        return pl.ds(pl.multiple_of(start, unit), size)

    up = {"mp": lax.rem(z + 1, nz) * 2 + yl}
    down = {"mp": lax.rem(z + nz - 1, nz) * 2 + yl}
    pair = {"mp": mp + 1 - 2 * yl}
    far = {"dp": lax.rem(dp + ndp // 2, ndp), "mp": mp + 1 - 2 * yl}
    twin = {"dp": dp + 1 - 2 * core}
    east = {"dp": row_of_x + lax.rem(x + 1, nx_chips) * 2 + core}
    west = {"dp": row_of_x + lax.rem(x + nx_chips - 1, nx_chips) * 2 + core}
    along = (up, down)

    barrier = pltpu.get_barrier_semaphore()
    peers = (up, down, pair, far, twin, east, west)
    for there in peers:
        pl.semaphore_signal(barrier, inc=1, device_id=there, device_id_type=MESH)

    loads = []
    for i, (src, dst) in enumerate((
        (tok_h, tok), (gain_h, gain.at[0]), (grad_h, grad), (rope_h, rope),
        (bias_h, bias.at[0, pl.ds(0, width)]),
        (w_h.at[at(core * half, half, half), :], w.at[:, pl.ds(0, width)]),
    )):
        c = pltpu.make_async_copy(src, dst, in_sem.at[i])
        c.start()
        loads.append(c)

    def remote(src, dst, send, recv, there):
        return pltpu.make_async_remote_copy(
            src_ref=src, dst_ref=dst, send_sem=send_sem.at[send], recv_sem=recv,
            device_id=there, device_id_type=MESH,
        )

    own_cols, pair_cols = pl.ds(0, width), pl.ds(width, width)

    def w_send(a, there):
        i = 2 * a + odd
        return remote(
            w_h.at[at(core * half + i * WCHUNK, WCHUNK, WCHUNK), :],
            w.at[at(i * WCHUNK, WCHUNK, WCHUNK), pair_cols], 0, wy_r.at[a], there,
        )

    def w_pass(a):
        ref = w.at[at((2 * a + odd) * WCHUNK, WCHUNK, WCHUNK), pair_cols]
        return remote(ref, ref, 1, wx_r.at[a], east if a % 2 == 0 else west)

    def w_come(k):
        ref = w.at[at((2 * k + 1 - odd) * WCHUNK, WCHUNK, WCHUNK), pair_cols]
        return remote(ref, ref, 1, wx_r.at[k], east)

    mine = at(core * col, col, col)
    other = at((1 - core) * col, col, col)
    home = at(core * col + z * rows, rows, rows)
    nx_send = remote(nx, held.at[home, :], 2, one_sem.at[0], twin)

    def ag(way, j, e):
        d = lax.rem(core + e // 4, 2)
        b = lax.rem(z + (nz - j if way == 0 else j), nz)
        ref = held.at[at(d * col + b * rows, rows, rows), at(lax.rem(e, 4) * quarter, quarter, quarter)]
        place = j * 8 + jnp.where(j < 3, e, e // 2)
        return remote(ref, ref, 3, ag_r.at[way, place], along[way])

    loads[0].wait()
    loads[1].wait()
    total = jnp.zeros((rows, 1), f32)
    for q in range(8):
        v = tok[:, q * quarter:(q + 1) * quarter].astype(f32)
        total = total + jnp.sum(v * v, axis=1, keepdims=True)
    scale = lax.rsqrt(total / depth + 1e-06)

    def normed(ks):
        return (tok[:, ks].astype(f32) * scale * gain[:, ks]).astype(bf16)

    for q in range(4):
        held[home, q * quarter:(q + 1) * quarter] = normed(at(core * half + q * quarter, quarter, quarter))
    for q in range(4):
        nx[:, q * quarter:(q + 1) * quarter] = normed(at((1 - core) * half + q * quarter, quarter, quarter))
    pl.semaphore_wait(barrier, len(peers))
    for q in range(4):
        for way in range(2):
            ag(way, 0, q).start()
    nx_send.start()
    bias_send = remote(bias_h, bias.at[0, pair_cols], 4, one_sem.at[1], pair)
    bias_send.start()
    for a in (0, 1, 3, 5, 7):
        w_send(a, far).start()

    loads[2].wait()
    loads[3].wait()
    bacc[...] = jnp.zeros_like(bacc)

    @pl.loop(0, nz)
    def _(b):
        for side, y in ((0, yl), (1, 1 - yl)):
            here = at((2 * b + y) * rows, rows, rows)
            there = at(b * rows, rows, rows)
            cs, sn = rope[0, y, there, :], rope[1, y, there, :]
            for h in range(heads):
                hs = slice(h * HEAD_DIM, (h + 1) * HEAD_DIM)
                v = grad[here, hs].astype(f32)
                turned = v * cs - pltpu.roll(v, HEAD_DIM // 2, 1) * sn
                plain = lax.rem(mp * heads + h, GROUP) == GROUP - 1
                v = jnp.where(plain, v, turned)
                bacc[:, hs] += jnp.sum(v.reshape(rows // 8, 8, HEAD_DIM), axis=0)
                if side == 0:
                    low[at(core * col + b * rows, rows, rows), hs] = v.astype(bf16)
                else:
                    lowx[there, hs] = v.astype(bf16)

    low_pair = remote(lowx, low.at[mine, pair_cols], 5, low_r.at[0], pair)
    low_twin = remote(low.at[mine, own_cols], low.at[mine, own_cols], 5, low_r.at[1], twin)
    low_fwd = remote(low.at[mine, pair_cols], low.at[mine, pair_cols], 5, low_r.at[2], twin)
    low_pair.start()
    low_twin.start()
    for a in (2, 4, 6):
        w_send(a, pair).start()
    nx_send.wait_recv()
    for q in range(4):
        for way in range(2):
            ag(way, 0, 4 + q).start()
    bg_ref[...] = jnp.sum(bacc[...], axis=0, keepdims=True)

    def cols(k):
        return at(k * CHUNK, CHUNK, CHUNK)

    def backward(k):
        w_come(k).wait_recv()
        part[:, cols(k)] = lax.dot_general(
            low[...], w[cols(k), :], (((1,), (1,)), ((), ())), preferred_element_type=f32
        )

    def rs(way, j, k):
        place = j * 8 + jnp.where(j < 3, k, k // 2)
        return remote(
            run.at[way, j, :, cols(k)], run.at[way, j + 1, :, cols(k)], 6, rs_r.at[way, place], along[way]
        )

    def hops(way, k):
        return jnp.where(lax.rem(k, 2) == way, 4, 3)

    def rs_step(way, j, k, first):
        left = hops(way, k) - j
        t = lax.rem(z + (left if way == 0 else nz - left), nz)
        if not first:
            rs(way, j - 1, k).wait_recv()
        for d in range(2):
            ds = pl.ds(d * rows, rows)
            v = part[at(d * col + t * rows, rows, rows), cols(k)]
            if not first:
                v = v + run[way, j, ds, cols(k)].astype(f32)
            run[way, j, ds, cols(k)] = v.astype(bf16)
        rs(way, j, k).start()

    def fin_send(k):
        return remote(
            fin.at[:, cols(k)], ng.at[:, at(core * half + k * CHUNK, CHUNK, CHUNK)], 7, one_sem.at[2], twin
        )

    def rs_final(k):
        for way in range(2):
            rs(way, hops(way, k) - 1, k).wait_recv()
        for d, to in ((core, None), (1 - core, fin)):
            ds = at(d * rows, rows, rows)
            v = part[at(d * col + z * rows, rows, rows), cols(k)]
            for way in range(2):
                v = v + run[way, hops(way, k), ds, cols(k)].astype(f32)
            if to is None:
                ng[:, at(core * half + k * CHUNK, CHUNK, CHUNK)] = v
            else:
                fin[:, cols(k)] = v
        fin_send(k).start()

    def gain_share(k):
        full = at(core * half + k * CHUNK, CHUNK, CHUNK)
        for ds, to, ks in ((mine, gtot, full), (other, gx, cols(k))):
            share = jnp.sum(part[ds, cols(k)] * held[ds, cols(k)].astype(f32), axis=0, keepdims=True)
            to[:, ks] = share / gain[:, full]

    gx_send = remote(gx, gtot.at[:, at(core * half, half, half)], 8, one_sem.at[3], twin)

    def slab_of(i):
        return at(i * slab, slab, slab)

    def g1(k):
        to = lax.rem(mp + k, n)
        return remote(gtot.at[:, slab_of(to)], grecv.at[k - 1], 9, one_sem.at[4], {"mp": to})

    def g2(k):
        to = lax.rem(mp + k, n)
        return remote(gres.at[:, slab_of(mp)], gres.at[:, slab_of(mp)], 10, one_sem.at[5], {"mp": to})

    g1_all = remote(grecv, grecv, 9, one_sem.at[4], up)
    g2_all = remote(gres.at[:, pl.ds(0, (n - 1) * slab)], gres.at[:, pl.ds(0, (n - 1) * slab)], 10, one_sem.at[5], up)

    def tile(t):
        return at(t * TILE_N, TILE_N, TILE_N)

    def c_send(t):
        return remote(acc.at[other, tile(t)], cx.at[:, tile(t)], 11, c_r.at[t], twin)

    def forward(t):
        acc[:, tile(t)] = jnp.dot(held[...], w[:, tile(t)], preferred_element_type=f32)
        c_send(t).start()

    def q_send(h):
        return remote(
            qt.at[:, at(width + h * HEAD_DIM, HEAD_DIM, HEAD_DIM)], qx.at[:, at(h * HEAD_DIM, HEAD_DIM, HEAD_DIM)],
            12, one_sem.at[6], pair,
        )

    q_all = remote(qx, qx, 12, one_sem.at[6], pair)

    def joined(t):
        c_send(t).wait_recv()
        for i in range(TILE_N // HEAD_DIM):
            h = t * (TILE_N // HEAD_DIM) + i
            hs = at(h * HEAD_DIM, HEAD_DIM, HEAD_DIM)
            v = acc[mine, hs] + cx[:, hs] + bias[:, hs]
            turned = v * rope[0, yl] + pltpu.roll(v, HEAD_DIM // 2, 1) * rope[1, yl]
            whole = jnp.where(h < heads, mp * heads + h, (mp + 1 - 2 * yl) * heads + h - heads)
            qt[:, hs] = jnp.where(lax.rem(whole, GROUP) == GROUP - 1, v, turned).astype(bf16)

            @pl.when(h >= heads)
            def _():
                q_send(h - heads).start()

    passes = (3, 8, 10, 13, 15, 18, 20, 23)
    early = (11, 16, 18, 21, 23)

    @pl.loop(0, 24)
    def _(i):
        j, e = 1 + i // 8, lax.rem(i, 8)
        for way in range(2):
            ag(way, j - 1, e).wait_recv()

            @pl.when((j < 3) | (lax.rem(e, 2) == way))
            def _():
                ag(way, j, e).start()

        for a, step in enumerate(passes):
            @pl.when(i == step)
            def _():
                w_send(a, pair).wait_recv()
                w_pass(a).start()

        @pl.when(i == 6)
        def _():
            low_pair.wait_recv()
            low_fwd.start()

        @pl.when(i == 9)
        def _():
            loads[5].wait()
            low_twin.wait_recv()
            low_fwd.wait_recv()

        k, due = 0, i == early[0]
        for m in range(1, len(early)):
            k, due = jnp.where(i >= early[m], m, k), due | (i == early[m])

        @pl.when(due)
        def _():
            backward(k)

    @pl.loop(0, chunks)
    def _(k):
        @pl.when(k >= len(early))
        def _():
            backward(k)

        for way in range(2):
            rs_step(way, 0, k, True)

    for e in range(8):
        ag(e % 2, 3, e).wait_recv()
    loads[4].wait()
    bias_send.wait_recv()

    @pl.loop(0, chunks)
    def _(k):
        gain_share(k)

    gx_send.start()

    @pl.loop(0, 20)
    def _(m):
        j, q = 1 + m // 8, lax.rem(m, 8)
        for way in range(2):
            rs_step(way, j, jnp.where(j < 3, q, 2 * q + way), False)

        @pl.when((m >= 2) & (m < 7))
        def _():
            joined(lax.rem(m, 5))

        @pl.when(m < 5)
        def _():
            forward(lax.rem(m + 2, 5))

        @pl.when(m == 1)
        def _():
            gx_send.wait_recv()
            for k in range(1, n):
                g1(k).start()

        @pl.when(m == 9)
        def _():
            g1_all.wait_recv()
            share = gtot[:, slab_of(mp)]
            for k in range(1, n):
                share = share + grecv[k - 1]
            gres[:, slab_of(mp)] = share
            for k in range(1, n):
                g2(k).start()

        @pl.when(m == 16)
        def _():
            q_all.wait_recv()
            for b in range(nz):
                there = pl.ds(b * rows, rows)
                qkv[at((2 * b + yl) * rows, rows, rows), :] = qt[there, own_cols]
                qkv[at((2 * b + 1 - yl) * rows, rows, rows), :] = qx[there, :]

    @pl.loop(0, chunks)
    def _(k):
        rs_final(k)

    g2_all.wait_recv()
    gg_ref[...] = gres[...]
    remote(fin, fin, 7, one_sem.at[2], twin).wait_recv()
    inner = jnp.zeros((rows, 1), f32)
    for q in range(8):
        ks = slice(q * quarter, (q + 1) * quarter)
        inner = inner + jnp.sum(ng[:, ks] * tok[:, ks].astype(f32) * gain[:, ks], axis=1, keepdims=True)
    weight = scale * scale * scale * (inner / depth)
    for q in range(8):
        ks = slice(q * quarter, (q + 1) * quarter)
        tg[:, ks] = scale * gain[:, ks] * ng[:, ks] - tok[:, ks].astype(f32) * weight

    def sent(ref, send):
        remote(ref, ref, send, one_sem.at[0], twin).wait_send()

    sent(w_h.at[pl.ds(0, half // 2), :], 0)
    sent(w_h.at[pl.ds(0, half // 2), :], 1)
    sent(nx, 2)
    moved = held.at[pl.ds(0, 7 * 2 * rows), :]
    sent(moved, 3)
    bias_send.wait_send()
    sent(w_h.at[pl.ds(0, 3 * col), :], 5)
    sent(moved, 6)
    sent(fin, 7)
    sent(gx, 8)
    sent(grecv, 9)
    sent(grecv, 10)
    sent(cx, 11)
    sent(qx, 12)


def finish(qkv, tg, gg, bg, qkv_h, tg_h, gg_h, bg_h, sem):
    moves = ((qkv, qkv_h), (tg, tg_h), (gg.at[0], gg_h), (bg.at[0], bg_h))
    copies = [pltpu.make_async_copy(src, dst, sem.at[i]) for i, (src, dst) in enumerate(moves)]
    for c in copies:
        c.start()
    for c in copies:
        c.wait()


def shards(n, ndp, tokens, norm_gain, qkv_weight, qkv_bias, qkv_grad):
    rows, depth = tokens.shape
    every, width = qkv_grad.shape
    rope = rope_tables(every, rows, SEQ_LEN // n)
    bf16, f32 = jnp.bfloat16, jnp.float32
    half, col, nz = depth // 2, every // 2, n // 2
    chunks = half // CHUNK
    tiles = 2 * width // TILE_N
    dma = pltpu.SemaphoreType.DMA
    vm = pltpu.VMEM
    hbm = pl.BlockSpec(memory_space=pl.ANY)
    vmem = pl.BlockSpec(memory_space=pltpu.VMEM)
    results = pl.pallas_call(
        functools.partial(kernel, nz, ndp),
        out_shape=(
            vm((every, width), bf16),
            vm((rows, depth), f32),
            vm((1, depth), f32),
            vm((1, width), f32),
        ),
        in_specs=[hbm] * 6,
        out_specs=[vmem] * 4,
        scratch_shapes=[
            vm((rows, depth), bf16),
            vm((1, depth), f32),
            vm((half, 2 * width), bf16),
            vm((1, 2 * width), f32),
            vm((every, width), bf16),
            vm((2, 2, col, HEAD_DIM), f32),
            vm((every, 2 * width), bf16),
            vm((col, width), bf16),
            vm((rows, half), bf16),
            vm((every, half), bf16),
            vm((every, half), f32),
            vm((2, 5, 2 * rows, half), bf16),
            vm((every, 2 * width), f32),
            vm((col, 2 * width), f32),
            vm((col, 2 * width), bf16),
            vm((col, width), bf16),
            vm((rows, depth), f32),
            vm((rows, half), f32),
            vm((1, depth), f32),
            vm((1, half), f32),
            vm((n - 1, 1, depth // n), f32),
            vm((1, depth), f32),
            vm((8, width), f32),
            dma((6,)),
            dma((13,)),
            dma((7,)),
            dma((3,)),
            dma((chunks,)),
            dma((chunks,)),
            dma((2, 28)),
            dma((2, 28)),
            dma((tiles,)),
        ],
        compiler_params=pltpu.CompilerParams(
            collective_id=0, has_side_effects=True, vmem_limit_bytes=60000000
        ),
        cost_estimate=pl.CostEstimate(
            flops=4 * every * depth * width, bytes_accessed=2 * depth * width, transcendentals=0
        ),
    )(
        tokens, norm_gain, qkv_weight, qkv_bias, qkv_grad,
        jnp.asarray(rope),
    )
    return pl.pallas_call(
        finish,
        out_shape=(
            jax.ShapeDtypeStruct((every, width), bf16),
            jax.ShapeDtypeStruct((rows, depth), f32),
            jax.ShapeDtypeStruct((depth,), f32),
            jax.ShapeDtypeStruct((width,), f32),
        ),
        in_specs=[vmem] * 4,
        out_specs=[hbm] * 4,
        scratch_shapes=[dma((4,))],
        compiler_params=pltpu.CompilerParams(vmem_limit_bytes=1 << 20),
    )(*results)


def solution(mesh):
    in_specs = (P(("dp", "mp"), None), P(), P(None, "mp"), P("mp"), P("dp", "mp"))
    out_specs = (P("dp", "mp"), P(("dp", "mp"), None), P("dp"), P(("dp", "mp")))
    body = functools.partial(shards, mesh.shape["mp"], mesh.shape["dp"])
    return jax.shard_map(body, mesh=mesh, in_specs=in_specs, out_specs=out_specs, check_vma=False)
```

```python
import functools

import jax
import jax.numpy as jnp
import numpy as np
from jax import lax
from jax.experimental import pallas as pl
from jax.experimental.pallas import tpu as pltpu
from jax.sharding import PartitionSpec as P

HEAD_DIM = 128
SEQ_LEN = 32768
GROUP = 10
MESH = pl.DeviceIdType.MESH
CHUNK = 512
WCHUNK = 256
TILE_N = 256


def rope_tables(rows, tok_dev, stride):
    half = HEAD_DIM // 2
    row = np.arange(rows)
    place = (row // tok_dev * stride + row % tok_dev).astype(np.float32)
    inverse = np.exp(
        -np.log(np.float32(1000000.0))
        * (np.float32(2.0) * np.arange(half).astype(np.float32) / np.float32(HEAD_DIM))
    ).astype(np.float32)
    angle = (place[:, None] * inverse[None, :]).astype(np.float32)
    cosine, sine = np.cos(angle).astype(np.float32), np.sin(angle).astype(np.float32)

    def by_column(t):
        t = t.reshape(rows // (2 * tok_dev), 2, tok_dev, HEAD_DIM)
        return np.ascontiguousarray(np.swapaxes(t, 0, 1)).reshape(2, rows // 2, HEAD_DIM)

    return np.stack([by_column(np.concatenate([cosine, cosine], 1)), by_column(np.concatenate([-sine, sine], 1))])


def kernel(
    nz, ndp,
    tok_h, gain_h, w_h, bias_h, grad_h, rope_h,
    qkv, tg, gg_ref, bg_ref,
    tok, gain, w, bias, grad, rope,
    low, lowx, nx, held, part, run, rfin, acc, cx, qt, qx, ng, gtot, gx, gy, grecv, gres, bacc,
    in_sem, send_sem, one_sem, low_r, wy_r, wx_r, ag_r, rs_r, end_r, c_r,
):
    f32, bf16 = jnp.float32, jnp.bfloat16
    dp, mp = lax.axis_index("dp"), lax.axis_index("mp")
    z, yl, core = mp // 2, lax.rem(mp, 2), lax.rem(dp, 2)
    nx_chips = ndp // 4
    row_of_x = dp // (2 * nx_chips) * (2 * nx_chips)
    x = lax.rem(dp // 2, nx_chips)
    odd = lax.rem(x, 2)
    rows, depth = tok.shape
    half = depth // 2
    col = nz * rows
    width = grad.shape[1]
    heads = width // HEAD_DIM
    chunks = half // CHUNK
    quarter = half // 4
    slab = half // nz

    def at(start, size, unit):
        return pl.ds(pl.multiple_of(start, unit), size)

    up = {"mp": lax.rem(z + 1, nz) * 2 + yl}
    down = {"mp": lax.rem(z + nz - 1, nz) * 2 + yl}
    pair = {"mp": mp + 1 - 2 * yl}
    far = {"dp": lax.rem(dp + ndp // 2, ndp), "mp": mp + 1 - 2 * yl}
    twin = {"dp": dp + 1 - 2 * core}
    east = {"dp": row_of_x + lax.rem(x + 1, nx_chips) * 2 + core}
    west = {"dp": row_of_x + lax.rem(x + nx_chips - 1, nx_chips) * 2 + core}
    along = (up, down)

    barrier = pltpu.get_barrier_semaphore()
    peers = (up, down, pair, far, twin, east, west)
    for there in peers:
        pl.semaphore_signal(barrier, inc=1, device_id=there, device_id_type=MESH)

    loads = []
    for i, (src, dst) in enumerate((
        (tok_h, tok), (gain_h, gain.at[0]), (grad_h, grad), (rope_h, rope),
        (bias_h, bias.at[0, pl.ds(0, width)]),
        (w_h.at[at(core * half, half, half), :], w.at[:, pl.ds(0, width)]),
    )):
        c = pltpu.make_async_copy(src, dst, in_sem.at[i])
        c.start()
        loads.append(c)

    def remote(src, dst, send, recv, there):
        return pltpu.make_async_remote_copy(
            src_ref=src, dst_ref=dst, send_sem=send_sem.at[send], recv_sem=recv,
            device_id=there, device_id_type=MESH,
        )

    own_cols, pair_cols = pl.ds(0, width), pl.ds(width, width)

    def w_send(a, there):
        i = 2 * a + odd
        return remote(
            w_h.at[at(core * half + i * WCHUNK, WCHUNK, WCHUNK), :],
            w.at[at(i * WCHUNK, WCHUNK, WCHUNK), pair_cols], 0, wy_r.at[a], there,
        )

    def w_pass(a):
        ref = w.at[at((2 * a + odd) * WCHUNK, WCHUNK, WCHUNK), pair_cols]
        return remote(ref, ref, 1, wx_r.at[a], east if a % 2 == 0 else west)

    def w_come(k):
        ref = w.at[at((2 * k + 1 - odd) * WCHUNK, WCHUNK, WCHUNK), pair_cols]
        return remote(ref, ref, 1, wx_r.at[k], east)

    mine = at(core * col, col, col)
    other = at((1 - core) * col, col, col)
    home = at(core * col + z * rows, rows, rows)
    nx_send = remote(nx, held.at[home, :], 2, one_sem.at[0], twin)

    def ag(way, j, e):
        d = lax.rem(core + e // 4, 2)
        b = lax.rem(z + (nz - j if way == 0 else j), nz)
        ref = held.at[at(d * col + b * rows, rows, rows), at(lax.rem(e, 4) * quarter, quarter, quarter)]
        on = jnp.where(lax.rem(e, 2) == way, 16 + e // 2, 20)
        place = jnp.where(j < 2, j * 8 + e, jnp.where(j == 2, on, 20))
        return remote(ref, ref, 3, ag_r.at[way, place], along[way])

    loads[0].wait()
    loads[1].wait()
    total = jnp.zeros((rows, 1), f32)
    for q in range(8):
        v = tok[:, q * quarter:(q + 1) * quarter].astype(f32)
        total = total + jnp.sum(v * v, axis=1, keepdims=True)
    scale = lax.rsqrt(total / depth + 1e-06)

    def normed(ks):
        return (tok[:, ks].astype(f32) * scale * gain[:, ks]).astype(bf16)

    for q in range(4):
        held[home, q * quarter:(q + 1) * quarter] = normed(at(core * half + q * quarter, quarter, quarter))
    for q in range(4):
        nx[:, q * quarter:(q + 1) * quarter] = normed(at((1 - core) * half + q * quarter, quarter, quarter))
    pl.semaphore_wait(barrier, len(peers))
    for q in range(4):
        for way in range(2):
            ag(way, 0, q).start()
    nx_send.start()
    bias_send = remote(bias_h, bias.at[0, pair_cols], 4, one_sem.at[1], pair)
    bias_send.start()
    for a in (0, 1, 3, 5, 7):
        w_send(a, far).start()

    loads[2].wait()
    loads[3].wait()
    bacc[...] = jnp.zeros_like(bacc)

    @pl.loop(0, nz)
    def _(b):
        for side, y in ((0, yl), (1, 1 - yl)):
            here = at((2 * b + y) * rows, rows, rows)
            there = at(b * rows, rows, rows)
            cs, sn = rope[0, y, there, :], rope[1, y, there, :]
            for h in range(heads):
                hs = slice(h * HEAD_DIM, (h + 1) * HEAD_DIM)
                v = grad[here, hs].astype(f32)
                turned = v * cs - pltpu.roll(v, HEAD_DIM // 2, 1) * sn
                plain = lax.rem(mp * heads + h, GROUP) == GROUP - 1
                v = jnp.where(plain, v, turned)
                bacc[:, hs] += jnp.sum(v.reshape(rows // 8, 8, HEAD_DIM), axis=0)
                if side == 0:
                    low[at(core * col + b * rows, rows, rows), hs] = v.astype(bf16)
                else:
                    lowx[there, hs] = v.astype(bf16)

    low_pair = remote(lowx, low.at[mine, pair_cols], 5, low_r.at[0], pair)
    low_twin = remote(low.at[mine, own_cols], low.at[mine, own_cols], 5, low_r.at[1], twin)
    low_fwd = remote(low.at[mine, pair_cols], low.at[mine, pair_cols], 5, low_r.at[2], twin)
    low_pair.start()
    low_twin.start()
    for a in (2, 4, 6):
        w_send(a, pair).start()
    nx_send.wait_recv()
    for q in range(4):
        for way in range(2):
            ag(way, 0, 4 + q).start()
    bg_ref[...] = jnp.sum(bacc[...], axis=0, keepdims=True)

    def cols(k):
        return at(k * CHUNK, CHUNK, CHUNK)

    def backward(k):
        w_come(k).wait_recv()
        part[:, cols(k)] = lax.dot_general(
            low[...], w[cols(k), :], (((1,), (1,)), ((), ())), preferred_element_type=f32
        )

    def rs(way, j, k):
        place = j * 8 + jnp.where(j < 2, k, k // 2)
        return remote(
            run.at[way, j, :, cols(k)], run.at[way, j + 1, :, cols(k)], 6, rs_r.at[way, place], along[way]
        )

    def rs_end(way, j, k, d):
        return remote(
            run.at[way, j, pl.ds(d * rows, rows), cols(k)],
            rfin.at[way, :, at(core * half + k * CHUNK, CHUNK, CHUNK)],
            6, end_r.at[way, core, j - 2], dict(along[way], dp=dp - core + d),
        )

    def hops(way, k):
        return jnp.where(lax.rem(k, 2) == way, 4, 3)

    def rs_step(way, j, k, first):
        left = hops(way, k) - j
        t = lax.rem(z + (left if way == 0 else nz - left), nz)
        if not first:
            rs(way, j - 1, k).wait_recv()
        for d in range(2):
            ds = pl.ds(d * rows, rows)
            v = part[at(d * col + t * rows, rows, rows), cols(k)]
            if not first:
                v = v + run[way, j, ds, cols(k)].astype(f32)
            run[way, j, ds, cols(k)] = v.astype(bf16)
        if first:
            rs(way, j, k).start()
            return

        @pl.when(left > 1)
        def _():
            rs(way, j, k).start()

        @pl.when(left == 1)
        def _():
            for d in range(2):
                rs_end(way, j, k, d).start()

    own_half = at(core * half, half, half)
    swap = remote(
        part.at[at((1 - core) * col + z * rows, rows, rows), :], ng.at[:, own_half], 7, one_sem.at[2], twin
    )

    def ended(group):
        for way in range(2):
            for side in range(2):
                ref = rfin.at[way, :, pl.ds(0, half // 2)]
                remote(ref, ref, 6, end_r.at[way, side, group], up).wait_recv()

    def gain_share(k):
        full = at(core * half + k * CHUNK, CHUNK, CHUNK)
        for ds, to, ks in ((mine, gtot, full), (other, gx, cols(k))):
            share = jnp.sum(part[ds, cols(k)] * held[ds, cols(k)].astype(f32), axis=0, keepdims=True)
            to[:, ks] = share / gain[:, full]

    gx_send = remote(gx, gtot.at[:, own_half], 8, one_sem.at[3], twin)
    gy_send = remote(gtot.at[:, at((1 - yl) * half, half, half)], gy, 13, one_sem.at[7], pair)
    column_half = at(yl * half, half, half)
    g3_send = remote(gres.at[:, column_half], gres.at[:, column_half], 14, one_sem.at[8], pair)

    def slab_of(i):
        return at(yl * half + i * slab, slab, slab)

    def g1(k):
        to = lax.rem(z + k, nz)
        return remote(gtot.at[:, slab_of(to)], grecv.at[k - 1], 9, one_sem.at[4], {"mp": 2 * to + yl})

    def g2(k):
        to = lax.rem(z + k, nz)
        return remote(gres.at[:, slab_of(z)], gres.at[:, slab_of(z)], 10, one_sem.at[5], {"mp": 2 * to + yl})

    g1_all = remote(grecv, grecv, 9, one_sem.at[4], up)
    g2_ref = gres.at[:, pl.ds(0, (nz - 1) * slab)]
    g2_all = remote(g2_ref, g2_ref, 10, one_sem.at[5], up)

    def tile(t):
        return at(t * TILE_N, TILE_N, TILE_N)

    def c_send(t):
        return remote(acc.at[other, tile(t)], cx.at[:, tile(t)], 11, c_r.at[t], twin)

    def forward(t):
        acc[:, tile(t)] = jnp.dot(held[...], w[:, tile(t)], preferred_element_type=f32)
        c_send(t).start()

    def q_send(h):
        return remote(
            qt.at[:, at(width + h * HEAD_DIM, HEAD_DIM, HEAD_DIM)], qx.at[:, at(h * HEAD_DIM, HEAD_DIM, HEAD_DIM)],
            12, one_sem.at[6], pair,
        )

    q_all = remote(qx, qx, 12, one_sem.at[6], pair)

    def joined(t):
        c_send(t).wait_recv()
        for i in range(TILE_N // HEAD_DIM):
            h = t * (TILE_N // HEAD_DIM) + i
            hs = at(h * HEAD_DIM, HEAD_DIM, HEAD_DIM)
            v = acc[mine, hs] + cx[:, hs] + bias[:, hs]
            turned = v * rope[0, yl] + pltpu.roll(v, HEAD_DIM // 2, 1) * rope[1, yl]
            whole = jnp.where(h < heads, mp * heads + h, (mp + 1 - 2 * yl) * heads + h - heads)
            qt[:, hs] = jnp.where(lax.rem(whole, GROUP) == GROUP - 1, v, turned).astype(bf16)

            @pl.when(h >= heads)
            def _():
                q_send(h - heads).start()

    passes = (3, 8, 10, 13, 15, 18, 20, 23)
    early = (11, 16, 18, 21, 23)

    @pl.loop(0, 24)
    def _(i):
        j, e = 1 + i // 8, lax.rem(i, 8)
        for way in range(2):
            @pl.when((j < 3) | (lax.rem(e, 2) == way))
            def _():
                ag(way, j - 1, e).wait_recv()
                ag(way, j, e).start()

        for a, step in enumerate(passes):
            @pl.when(i == step)
            def _():
                w_send(a, pair).wait_recv()
                w_pass(a).start()

        @pl.when(i == 6)
        def _():
            low_pair.wait_recv()
            low_fwd.start()

        @pl.when(i == 9)
        def _():
            loads[5].wait()
            low_twin.wait_recv()
            low_fwd.wait_recv()

        k, due = 0, i == early[0]
        for m in range(1, len(early)):
            k, due = jnp.where(i >= early[m], m, k), due | (i == early[m])

        @pl.when(due)
        def _():
            backward(k)

    @pl.loop(0, chunks)
    def _(k):
        @pl.when(k >= len(early))
        def _():
            backward(k)

        for way in range(2):
            rs_step(way, 0, k, True)

    swap.start()
    for q in range(4):
        ks = pl.ds(q * quarter, quarter)
        ng[:, at(core * half + q * quarter, quarter, quarter)] = part[home, ks]
    for way in range(2):
        ref = held.at[pl.ds(0, 2 * rows), :]
        remote(ref, ref, 3, ag_r.at[way, 20], up).wait_recv()
    loads[4].wait()
    bias_send.wait_recv()

    @pl.loop(0, chunks)
    def _(k):
        gain_share(k)

    gx_send.start()

    @pl.loop(0, 20)
    def _(m):
        j, q = 1 + m // 8, lax.rem(m, 8)
        for way in range(2):
            rs_step(way, j, jnp.where(j < 3, q, 2 * q + way), False)

        @pl.when((m >= 2) & (m < 7))
        def _():
            joined(lax.rem(m, 5))

        @pl.when(m < 5)
        def _():
            forward(lax.rem(m + 2, 5))

        @pl.when(m == 1)
        def _():
            gx_send.wait_recv()
            gy_send.start()

        @pl.when(m == 4)
        def _():
            gy_send.wait_recv()
            gtot[:, column_half] += gy[...]
            for k in range(1, nz):
                g1(k).start()

        @pl.when(m == 13)
        def _():
            g1_all.wait_recv()
            share = gtot[:, slab_of(z)]
            for k in range(1, nz):
                share = share + grecv[k - 1]
            gres[:, slab_of(z)] = share
            for k in range(1, nz):
                g2(k).start()

        @pl.when(m == 16)
        def _():
            q_all.wait_recv()
            for b in range(nz):
                there = pl.ds(b * rows, rows)
                qkv[at((2 * b + yl) * rows, rows, rows), :] = qt[there, own_cols]
                qkv[at((2 * b + 1 - yl) * rows, rows, rows), :] = qx[there, :]

    g2_all.wait_recv()
    g3_send.start()
    swap.wait_recv()
    ended(0)
    for q in range(2 * chunks):
        ks = slice(q * CHUNK, (q + 1) * CHUNK)
        ng[:, ks] += rfin[1 - q % 2, :, ks].astype(f32)
    ended(1)
    inner = jnp.zeros((rows, 1), f32)
    for q in range(2 * chunks):
        ks = slice(q * CHUNK, (q + 1) * CHUNK)
        v = ng[:, ks] + rfin[q % 2, :, ks].astype(f32)
        ng[:, ks] = v
        inner = inner + jnp.sum(v * tok[:, ks].astype(f32) * gain[:, ks], axis=1, keepdims=True)
    weight = scale * scale * scale * (inner / depth)
    for q in range(8):
        ks = slice(q * quarter, (q + 1) * quarter)
        tg[:, ks] = scale * gain[:, ks] * ng[:, ks] - tok[:, ks].astype(f32) * weight

    g3_send.wait_recv()
    gg_ref[...] = gres[...]

    def sent(ref, send):
        remote(ref, ref, send, one_sem.at[0], twin).wait_send()

    sent(w_h.at[pl.ds(0, half // 2), :], 0)
    sent(w_h.at[pl.ds(0, half // 2), :], 1)
    sent(nx, 2)
    moved = held.at[pl.ds(0, 7 * 2 * rows), :]
    sent(moved, 3)
    bias_send.wait_send()
    sent(w_h.at[pl.ds(0, 3 * col), :], 5)
    sent(moved, 6)
    swap.wait_send()
    sent(gx, 8)
    sent(grecv, 9)
    sent(grecv, 10)
    sent(cx, 11)
    sent(qx, 12)
    gy_send.wait_send()
    g3_send.wait_send()


def finish(qkv, tg, gg, bg, qkv_h, tg_h, gg_h, bg_h, sem):
    moves = ((qkv, qkv_h), (tg, tg_h), (gg.at[0], gg_h), (bg.at[0], bg_h))
    copies = [pltpu.make_async_copy(src, dst, sem.at[i]) for i, (src, dst) in enumerate(moves)]
    for c in copies:
        c.start()
    for c in copies:
        c.wait()


def shards(n, ndp, tokens, norm_gain, qkv_weight, qkv_bias, qkv_grad):
    rows, depth = tokens.shape
    every, width = qkv_grad.shape
    rope = rope_tables(every, rows, SEQ_LEN // n)
    bf16, f32 = jnp.bfloat16, jnp.float32
    half, col, nz = depth // 2, every // 2, n // 2
    chunks = half // CHUNK
    tiles = 2 * width // TILE_N
    dma = pltpu.SemaphoreType.DMA
    vm = pltpu.VMEM
    hbm = pl.BlockSpec(memory_space=pl.ANY)
    vmem = pl.BlockSpec(memory_space=pltpu.VMEM)
    results = pl.pallas_call(
        functools.partial(kernel, nz, ndp),
        out_shape=(
            vm((every, width), bf16),
            vm((rows, depth), f32),
            vm((1, depth), f32),
            vm((1, width), f32),
        ),
        in_specs=[hbm] * 6,
        out_specs=[vmem] * 4,
        scratch_shapes=[
            vm((rows, depth), bf16),
            vm((1, depth), f32),
            vm((half, 2 * width), bf16),
            vm((1, 2 * width), f32),
            vm((every, width), bf16),
            vm((2, 2, col, HEAD_DIM), f32),
            vm((every, 2 * width), bf16),
            vm((col, width), bf16),
            vm((rows, half), bf16),
            vm((every, half), bf16),
            vm((every, half), f32),
            vm((2, 4, 2 * rows, half), bf16),
            vm((2, rows, depth), bf16),
            vm((every, 2 * width), f32),
            vm((col, 2 * width), f32),
            vm((col, 2 * width), bf16),
            vm((col, width), bf16),
            vm((rows, depth), f32),
            vm((1, depth), f32),
            vm((1, half), f32),
            vm((1, half), f32),
            vm((nz - 1, 1, depth // n), f32),
            vm((1, depth), f32),
            vm((8, width), f32),
            dma((6,)),
            dma((15,)),
            dma((9,)),
            dma((3,)),
            dma((chunks,)),
            dma((chunks,)),
            dma((2, 21)),
            dma((2, 20)),
            dma((2, 2, 2)),
            dma((tiles,)),
        ],
        compiler_params=pltpu.CompilerParams(
            collective_id=0, has_side_effects=True, vmem_limit_bytes=60000000
        ),
        cost_estimate=pl.CostEstimate(
            flops=4 * every * depth * width, bytes_accessed=2 * depth * width, transcendentals=0
        ),
    )(
        tokens, norm_gain, qkv_weight, qkv_bias, qkv_grad,
        jnp.asarray(rope),
    )
    return pl.pallas_call(
        finish,
        out_shape=(
            jax.ShapeDtypeStruct((every, width), bf16),
            jax.ShapeDtypeStruct((rows, depth), f32),
            jax.ShapeDtypeStruct((depth,), f32),
            jax.ShapeDtypeStruct((width,), f32),
        ),
        in_specs=[vmem] * 4,
        out_specs=[hbm] * 4,
        scratch_shapes=[dma((4,))],
        compiler_params=pltpu.CompilerParams(vmem_limit_bytes=1 << 20),
    )(*results)


def solution(mesh):
    in_specs = (P(("dp", "mp"), None), P(), P(None, "mp"), P("mp"), P("dp", "mp"))
    out_specs = (P("dp", "mp"), P(("dp", "mp"), None), P("dp"), P(("dp", "mp")))
    body = functools.partial(shards, mesh.shape["mp"], mesh.shape["dp"])
    return jax.shard_map(body, mesh=mesh, in_specs=in_specs, out_specs=out_specs, check_vma=False)
```

```python
import functools

import jax
import jax.numpy as jnp
import numpy as np
from jax import lax
from jax.experimental import pallas as pl
from jax.experimental.pallas import tpu as pltpu
from jax.sharding import PartitionSpec as P

HEAD_DIM = 128
SEQ_LEN = 32768
GROUP = 10
MESH = pl.DeviceIdType.MESH
CHUNK = 512
WCHUNK = 256
TILE_N = 256


def rope_tables(rows, tok_dev, stride):
    half = HEAD_DIM // 2
    row = np.arange(rows)
    place = (row // tok_dev * stride + row % tok_dev).astype(np.float32)
    inverse = np.exp(
        -np.log(np.float32(1000000.0))
        * (np.float32(2.0) * np.arange(half).astype(np.float32) / np.float32(HEAD_DIM))
    ).astype(np.float32)
    angle = (place[:, None] * inverse[None, :]).astype(np.float32)
    cosine, sine = np.cos(angle).astype(np.float32), np.sin(angle).astype(np.float32)

    def by_column(t):
        t = t.reshape(rows // (2 * tok_dev), 2, tok_dev, HEAD_DIM)
        return np.ascontiguousarray(np.swapaxes(t, 0, 1)).reshape(2, rows // 2, HEAD_DIM)

    return np.stack([by_column(np.concatenate([cosine, cosine], 1)), by_column(np.concatenate([-sine, sine], 1))])


def kernel(
    nz, ndp,
    tok_h, gain_h, w_h, bias_h, grad_h, rope_h,
    qkv, total_ng, tok, gain, factors, gg_ref, bg_ref,
    w, bias, grad, rope,
    low, lowx, nx, held, part, run, rfin, acc, cx, qt, qx, ng, gtot, gx, gy, grecv, gres, bacc,
    in_sem, send_sem, one_sem, low_r, wy_r, wx_r, ag_r, end_r, c_r,
):
    f32, bf16 = jnp.float32, jnp.bfloat16
    dp, mp = lax.axis_index("dp"), lax.axis_index("mp")
    z, yl, core = mp // 2, lax.rem(mp, 2), lax.rem(dp, 2)
    nx_chips = ndp // 4
    row_of_x = dp // (2 * nx_chips) * (2 * nx_chips)
    x = lax.rem(dp // 2, nx_chips)
    odd = lax.rem(x, 2)
    rows, depth = tok.shape
    half = depth // 2
    col = nz * rows
    width = grad.shape[1]
    heads = width // HEAD_DIM
    chunks = half // CHUNK
    quarter = half // 4
    slab = half // nz

    def at(start, size, unit):
        return pl.ds(pl.multiple_of(start, unit), size)

    up = {"mp": lax.rem(z + 1, nz) * 2 + yl}
    down = {"mp": lax.rem(z + nz - 1, nz) * 2 + yl}
    pair = {"mp": mp + 1 - 2 * yl}
    far = {"dp": lax.rem(dp + ndp // 2, ndp), "mp": mp + 1 - 2 * yl}
    twin = {"dp": dp + 1 - 2 * core}
    east = {"dp": row_of_x + lax.rem(x + 1, nx_chips) * 2 + core}
    west = {"dp": row_of_x + lax.rem(x + nx_chips - 1, nx_chips) * 2 + core}
    along = (up, down)

    barrier = pltpu.get_barrier_semaphore()
    peers = (up, down, pair, far, twin, east, west)
    for there in peers:
        pl.semaphore_signal(barrier, inc=1, device_id=there, device_id_type=MESH)

    loads = []
    for i, (src, dst) in enumerate((
        (tok_h, tok), (gain_h, gain.at[0]), (grad_h, grad), (rope_h, rope),
        (bias_h, bias.at[0, pl.ds(0, width)]),
        (w_h.at[at(core * half, half, half), :], w.at[:, pl.ds(0, width)]),
    )):
        c = pltpu.make_async_copy(src, dst, in_sem.at[i])
        c.start()
        loads.append(c)

    def remote(src, dst, send, recv, there):
        return pltpu.make_async_remote_copy(
            src_ref=src, dst_ref=dst, send_sem=send_sem.at[send], recv_sem=recv,
            device_id=there, device_id_type=MESH,
        )

    own_cols, pair_cols = pl.ds(0, width), pl.ds(width, width)

    def w_send(a, there):
        i = 2 * a + odd
        return remote(
            w_h.at[at(core * half + i * WCHUNK, WCHUNK, WCHUNK), :],
            w.at[at(i * WCHUNK, WCHUNK, WCHUNK), pair_cols], 0, wy_r.at[a], there,
        )

    def w_pass(a):
        ref = w.at[at((2 * a + odd) * WCHUNK, WCHUNK, WCHUNK), pair_cols]
        return remote(ref, ref, 1, wx_r.at[a], east if a % 2 == 0 else west)

    def w_last():
        i = 2 * chunks - 1 - odd
        return remote(
            w_h.at[at(core * half + i * WCHUNK, WCHUNK, WCHUNK), :],
            w.at[at(i * WCHUNK, WCHUNK, WCHUNK), pair_cols], 0, wx_r.at[chunks - 1], pair,
        )

    def w_come(k):
        ref = w.at[at((2 * k + 1 - odd) * WCHUNK, WCHUNK, WCHUNK), pair_cols]
        return remote(ref, ref, 1, wx_r.at[k], east)

    mine = at(core * col, col, col)
    other = at((1 - core) * col, col, col)
    home = at(core * col + z * rows, rows, rows)
    nx_send = remote(nx, held.at[home, :], 2, one_sem.at[0], twin)

    def ag(way, j, e):
        d = lax.rem(core + e // 4, 2)
        b = lax.rem(z + (nz - j if way == 0 else j), nz)
        ref = held.at[at(d * col + b * rows, rows, rows), at(lax.rem(e, 4) * quarter, quarter, quarter)]
        on = jnp.where(lax.rem(e, 2) == way, 16 + e // 2, 20)
        place = jnp.where(j < 2, j * 8 + e, jnp.where(j == 2, on, 20))
        return remote(ref, ref, 3, ag_r.at[way, place], along[way])

    loads[0].wait()
    loads[1].wait()
    total = jnp.zeros((rows, 1), f32)
    for q in range(8):
        v = tok[:, q * quarter:(q + 1) * quarter].astype(f32)
        total = total + jnp.sum(v * v, axis=1, keepdims=True)
    scale = lax.rsqrt(total / depth + 1e-06)

    def normed(ks):
        return (tok[:, ks].astype(f32) * scale * gain[:, ks]).astype(bf16)

    for q in range(4):
        held[home, q * quarter:(q + 1) * quarter] = normed(at(core * half + q * quarter, quarter, quarter))
    for q in range(4):
        nx[:, q * quarter:(q + 1) * quarter] = normed(at((1 - core) * half + q * quarter, quarter, quarter))
    pl.semaphore_wait(barrier, len(peers))
    for q in range(4):
        for way in range(2):
            ag(way, 0, q).start()
    nx_send.start()
    bias_send = remote(bias_h, bias.at[0, pair_cols], 4, one_sem.at[1], pair)
    bias_send.start()
    for a in (0, 1, 3, 5, 7):
        w_send(a, far).start()

    loads[2].wait()
    loads[3].wait()
    bacc[...] = jnp.zeros_like(bacc)

    @pl.loop(0, nz)
    def _(b):
        for side, y in ((0, yl), (1, 1 - yl)):
            here = at((2 * b + y) * rows, rows, rows)
            there = at(b * rows, rows, rows)
            cs, sn = rope[0, y, there, :], rope[1, y, there, :]
            for h in range(heads):
                hs = slice(h * HEAD_DIM, (h + 1) * HEAD_DIM)
                v = grad[here, hs].astype(f32)
                turned = v * cs - pltpu.roll(v, HEAD_DIM // 2, 1) * sn
                plain = lax.rem(mp * heads + h, GROUP) == GROUP - 1
                v = jnp.where(plain, v, turned)
                bacc[:, hs] += jnp.sum(v.reshape(rows // 8, 8, HEAD_DIM), axis=0)
                if side == 0:
                    low[at(core * col + b * rows, rows, rows), hs] = v.astype(bf16)
                else:
                    lowx[there, hs] = v.astype(bf16)

    low_pair = remote(lowx, low.at[mine, pair_cols], 5, low_r.at[0], pair)
    low_twin = remote(low.at[mine, own_cols], low.at[mine, own_cols], 5, low_r.at[1], twin)
    low_fwd = remote(low.at[mine, pair_cols], low.at[mine, pair_cols], 5, low_r.at[2], twin)
    low_pair.start()
    low_twin.start()
    for a in (2, 4, 6):
        w_send(a, pair).start()
    w_last().start()
    nx_send.wait_recv()
    for q in range(4):
        for way in range(2):
            ag(way, 0, 4 + q).start()
    bg_ref[...] = jnp.sum(bacc[...], axis=0, keepdims=True)

    def cols(k):
        return at(k * CHUNK, CHUNK, CHUNK)

    def backward(k):
        @pl.when(k == chunks - 1)
        def _():
            w_send(chunks - 1, far).wait_recv()

        w_come(k).wait_recv()
        part[:, cols(k)] = lax.dot_general(
            low[...], w[cols(k), :], (((1,), (1,)), ((), ())), preferred_element_type=f32
        )

    def rs(way, j, k):
        place = j * 8 + jnp.where(j < 2, k, k // 2)
        return remote(
            run.at[way, j, :, cols(k)], run.at[way, j + 1, :, cols(k)], 6, ag_r.at[way, place], along[way]
        )

    def rs_end(way, j, k, d):
        return remote(
            run.at[way, j, pl.ds(d * rows, rows), cols(k)],
            rfin.at[way, :, at(core * half + k * CHUNK, CHUNK, CHUNK)],
            6, end_r.at[way, core, j - 2], dict(along[way], dp=dp - core + d),
        )

    def hops(way, k):
        return jnp.where(lax.rem(k, 2) == way, 4, 3)

    def rs_step(way, j, k, first):
        left = hops(way, k) - j
        t = lax.rem(z + (left if way == 0 else nz - left), nz)
        if not first:
            rs(way, j - 1, k).wait_recv()
        for d in range(2):
            ds = pl.ds(d * rows, rows)
            v = part[at(d * col + t * rows, rows, rows), cols(k)]
            if not first:
                v = v + run[way, j, ds, cols(k)].astype(f32)
            run[way, j, ds, cols(k)] = v.astype(bf16)
        if first:
            rs(way, j, k).start()
            return

        @pl.when(left > 1)
        def _():
            rs(way, j, k).start()

        @pl.when(left == 1)
        def _():
            for d in range(2):
                rs_end(way, j, k, d).start()

    own_half = at(core * half, half, half)
    swap = remote(
        part.at[at((1 - core) * col + z * rows, rows, rows), :], ng.at[:, own_half], 7, one_sem.at[2], twin
    )

    def ended(group):
        for way in range(2):
            for side in range(2):
                ref = rfin.at[way, :, pl.ds(0, half // 2)]
                remote(ref, ref, 6, end_r.at[way, side, group], up).wait_recv()

    def gain_share(k):
        full = at(core * half + k * CHUNK, CHUNK, CHUNK)
        for ds, to, ks in ((mine, gtot, full), (other, gx, cols(k))):
            share = jnp.sum(part[ds, cols(k)] * held[ds, cols(k)].astype(f32), axis=0, keepdims=True)
            to[:, ks] = share / gain[:, full]

    gx_send = remote(gx, gtot.at[:, own_half], 8, one_sem.at[3], twin)
    gy_send = remote(gtot.at[:, at((1 - yl) * half, half, half)], gy, 13, one_sem.at[7], pair)
    column_half = at(yl * half, half, half)
    g3_send = remote(gres.at[:, column_half], gres.at[:, column_half], 14, one_sem.at[8], pair)

    def slab_of(i):
        return at(yl * half + i * slab, slab, slab)

    def g1(k):
        to = lax.rem(z + k, nz)
        return remote(gtot.at[:, slab_of(to)], grecv.at[k - 1], 9, one_sem.at[4], {"mp": 2 * to + yl})

    def g2(k):
        to = lax.rem(z + k, nz)
        return remote(gres.at[:, slab_of(z)], gres.at[:, slab_of(z)], 10, one_sem.at[5], {"mp": 2 * to + yl})

    g1_all = remote(grecv, grecv, 9, one_sem.at[4], up)
    g2_ref = gres.at[:, pl.ds(0, (nz - 1) * slab)]
    g2_all = remote(g2_ref, g2_ref, 10, one_sem.at[5], up)

    def tile(t):
        return at(t * TILE_N, TILE_N, TILE_N)

    def c_send(t):
        return remote(acc.at[other, tile(t)], cx.at[:, tile(t)], 11, c_r.at[t], twin)

    def forward(t):
        acc[:, tile(t)] = jnp.dot(held[...], w[:, tile(t)], preferred_element_type=f32)
        c_send(t).start()

    def q_send(h):
        return remote(
            qt.at[:, at(width + h * HEAD_DIM, HEAD_DIM, HEAD_DIM)], qx.at[:, at(h * HEAD_DIM, HEAD_DIM, HEAD_DIM)],
            12, one_sem.at[6], pair,
        )

    q_all = remote(qx, qx, 12, one_sem.at[6], pair)

    def joined(t):
        c_send(t).wait_recv()
        for i in range(TILE_N // HEAD_DIM):
            h = t * (TILE_N // HEAD_DIM) + i
            hs = at(h * HEAD_DIM, HEAD_DIM, HEAD_DIM)
            v = acc[mine, hs] + cx[:, hs] + bias[:, hs]
            turned = v * rope[0, yl] + pltpu.roll(v, HEAD_DIM // 2, 1) * rope[1, yl]
            whole = jnp.where(h < heads, mp * heads + h, (mp + 1 - 2 * yl) * heads + h - heads)
            qt[:, hs] = jnp.where(lax.rem(whole, GROUP) == GROUP - 1, v, turned).astype(bf16)

            @pl.when(h >= heads)
            def _():
                q_send(h - heads).start()

    passes = (4, 9, 11, 14, 16, 19, 21)
    early = (12, 17, 18, 22, 23)
    ahead = 4

    @pl.loop(0, 24)
    def _(i):
        j, e = 1 + i // 8, lax.rem(i, 8)
        for way in range(2):
            @pl.when((j < 3) | (lax.rem(e, 2) == way))
            def _():
                ag(way, j - 1, e).wait_recv()
                ag(way, j, e).start()

        @pl.when(i >= 24 - ahead)
        def _():
            for way in range(2):
                rs_step(way, 0, i - (24 - ahead), True)

        for a, step in enumerate(passes):
            @pl.when(i == step)
            def _():
                w_send(a, pair).wait_recv()
                w_pass(a).start()

        @pl.when(i == 6)
        def _():
            low_pair.wait_recv()
            low_fwd.start()

        @pl.when(i == 9)
        def _():
            loads[5].wait()
            low_twin.wait_recv()
            low_fwd.wait_recv()

        k, due = 0, i == early[0]
        for m in range(1, len(early)):
            k, due = jnp.where(i >= early[m], m, k), due | (i == early[m])

        @pl.when(due)
        def _():
            backward(k)

    @pl.loop(ahead, chunks)
    def _(m):
        k = jnp.where(m < chunks - 2, m, 2 * chunks - 3 - m)

        @pl.when(m >= len(early))
        def _():
            backward(k)

        for way in range(2):
            rs_step(way, 0, k, True)

    swap.start()
    for q in range(4):
        ks = pl.ds(q * quarter, quarter)
        ng[:, at(core * half + q * quarter, quarter, quarter)] = part[home, ks]
    for way in range(2):
        ref = held.at[pl.ds(0, 2 * rows), :]
        remote(ref, ref, 3, ag_r.at[way, 20], up).wait_recv()
    loads[4].wait()
    bias_send.wait_recv()

    @pl.loop(0, chunks)
    def _(k):
        gain_share(k)

    gx_send.start()

    @pl.loop(0, 20)
    def _(m):
        j, q = 1 + m // 8, lax.rem(m, 8)
        for way in range(2):
            rs_step(way, j, jnp.where(j < 3, q, 2 * q + way), False)

        @pl.when((m >= 2) & (m < 7))
        def _():
            joined(lax.rem(m, 5))

        @pl.when(m < 5)
        def _():
            forward(lax.rem(m + 2, 5))

        @pl.when(m == 1)
        def _():
            gx_send.wait_recv()
            gy_send.start()

        @pl.when(m == 4)
        def _():
            gy_send.wait_recv()
            gtot[:, column_half] += gy[...]
            for k in range(1, nz):
                g1(k).start()

        @pl.when(m == 13)
        def _():
            g1_all.wait_recv()
            share = gtot[:, slab_of(z)]
            for k in range(1, nz):
                share = share + grecv[k - 1]
            gres[:, slab_of(z)] = share
            for k in range(1, nz):
                g2(k).start()

        @pl.when(m == 16)
        def _():
            q_all.wait_recv()
            for b in range(nz):
                there = pl.ds(b * rows, rows)
                qkv[at((2 * b + yl) * rows, rows, rows), :] = qt[there, own_cols]
                qkv[at((2 * b + 1 - yl) * rows, rows, rows), :] = qx[there, :]

    g2_all.wait_recv()
    g3_send.start()
    swap.wait_recv()
    ended(0)
    for q in range(2 * chunks):
        ks = slice(q * CHUNK, (q + 1) * CHUNK)
        ng[:, ks] += rfin[1 - q % 2, :, ks].astype(f32)
    ended(1)
    inner = jnp.zeros((rows, 1), f32)
    for q in range(2 * chunks):
        ks = slice(q * CHUNK, (q + 1) * CHUNK)
        v = ng[:, ks] + rfin[q % 2, :, ks].astype(f32)
        total_ng[:, ks] = v
        inner = inner + jnp.sum(v * tok[:, ks].astype(f32) * gain[:, ks], axis=1, keepdims=True)
    factors[0] = jnp.broadcast_to(scale, factors.shape[1:])
    factors[1] = jnp.broadcast_to(scale * scale * scale * (inner / depth), factors.shape[1:])

    g3_send.wait_recv()
    gg_ref[...] = gres[...]

    def sent(ref, send):
        remote(ref, ref, send, one_sem.at[0], twin).wait_send()

    sent(w_h.at[pl.ds(0, (chunks + 1) * WCHUNK), :], 0)
    sent(w_h.at[pl.ds(0, (chunks - 1) * WCHUNK), :], 1)
    sent(nx, 2)
    moved = held.at[pl.ds(0, 7 * 2 * rows), :]
    sent(moved, 3)
    bias_send.wait_send()
    sent(w_h.at[pl.ds(0, 3 * col), :], 5)
    sent(moved, 6)
    swap.wait_send()
    sent(gx, 8)
    sent(grecv, 9)
    sent(grecv, 10)
    sent(cx, 11)
    sent(qx, 12)
    gy_send.wait_send()
    g3_send.wait_send()


def finish(qkv, ng, tok, gain, factors, gg, bg, qkv_h, tg_h, gg_h, bg_h, tg, sem):
    parts = sem.shape[0] - 3
    piece = tok.shape[1] // parts
    copies = [
        pltpu.make_async_copy(src, dst, sem.at[i])
        for i, (src, dst) in enumerate(((qkv, qkv_h), (gg.at[0], gg_h), (bg.at[0], bg_h)))
    ]
    for c in copies:
        c.start()
    scale, weight = factors[0, :, :1], factors[1, :, :1]
    for q in range(parts):
        ks = slice(q * piece, (q + 1) * piece)
        tg[:, ks] = scale * gain[:, ks] * ng[:, ks] - tok[:, ks].astype(jnp.float32) * weight
        c = pltpu.make_async_copy(tg.at[:, ks], tg_h.at[:, ks], sem.at[3 + q])
        c.start()
        copies.append(c)
    for c in copies:
        c.wait()


def shards(n, ndp, tokens, norm_gain, qkv_weight, qkv_bias, qkv_grad):
    rows, depth = tokens.shape
    every, width = qkv_grad.shape
    rope = rope_tables(every, rows, SEQ_LEN // n)
    bf16, f32 = jnp.bfloat16, jnp.float32
    half, col, nz = depth // 2, every // 2, n // 2
    chunks = half // CHUNK
    tiles = 2 * width // TILE_N
    dma = pltpu.SemaphoreType.DMA
    vm = pltpu.VMEM
    hbm = pl.BlockSpec(memory_space=pl.ANY)
    vmem = pl.BlockSpec(memory_space=pltpu.VMEM)
    results = pl.pallas_call(
        functools.partial(kernel, nz, ndp),
        out_shape=(
            vm((every, width), bf16),
            vm((rows, depth), f32),
            vm((rows, depth), bf16),
            vm((1, depth), f32),
            vm((2, rows, HEAD_DIM), f32),
            vm((1, depth), f32),
            vm((1, width), f32),
        ),
        in_specs=[hbm] * 6,
        out_specs=[vmem] * 7,
        scratch_shapes=[
            vm((half, 2 * width), bf16),
            vm((1, 2 * width), f32),
            vm((every, width), bf16),
            vm((2, 2, col, HEAD_DIM), f32),
            vm((every, 2 * width), bf16),
            vm((col, width), bf16),
            vm((rows, half), bf16),
            vm((every, half), bf16),
            vm((every, half), f32),
            vm((2, 4, 2 * rows, half), bf16),
            vm((2, rows, depth), bf16),
            vm((every, 2 * width), f32),
            vm((col, 2 * width), f32),
            vm((col, 2 * width), bf16),
            vm((col, width), bf16),
            vm((rows, depth), f32),
            vm((1, depth), f32),
            vm((1, half), f32),
            vm((1, half), f32),
            vm((nz - 1, 1, depth // n), f32),
            vm((1, depth), f32),
            vm((8, width), f32),
            dma((6,)),
            dma((15,)),
            dma((9,)),
            dma((3,)),
            dma((chunks,)),
            dma((chunks,)),
            dma((2, 21)),
            dma((2, 2, 2)),
            dma((tiles,)),
        ],
        compiler_params=pltpu.CompilerParams(
            collective_id=0, has_side_effects=True, vmem_limit_bytes=60000000
        ),
        cost_estimate=pl.CostEstimate(
            flops=4 * every * depth * width, bytes_accessed=2 * depth * width, transcendentals=0
        ),
    )(
        tokens, norm_gain, qkv_weight, qkv_bias, qkv_grad,
        jnp.asarray(rope),
    )
    return pl.pallas_call(
        finish,
        out_shape=(
            jax.ShapeDtypeStruct((every, width), bf16),
            jax.ShapeDtypeStruct((rows, depth), f32),
            jax.ShapeDtypeStruct((depth,), f32),
            jax.ShapeDtypeStruct((width,), f32),
        ),
        in_specs=[vmem] * 7,
        out_specs=[hbm] * 4,
        scratch_shapes=[vm((rows, depth), f32), dma((7,))],
        compiler_params=pltpu.CompilerParams(vmem_limit_bytes=1 << 21),
    )(*results)


def solution(mesh):
    in_specs = (P(("dp", "mp"), None), P(), P(None, "mp"), P("mp"), P("dp", "mp"))
    out_specs = (P("dp", "mp"), P(("dp", "mp"), None), P("dp"), P(("dp", "mp")))
    body = functools.partial(shards, mesh.shape["mp"], mesh.shape["dp"])
    return jax.shard_map(body, mesh=mesh, in_specs=in_specs, out_specs=out_specs, check_vma=False)
```

```python
import functools

import jax
import jax.numpy as jnp
import numpy as np
from jax import lax
from jax.experimental import pallas as pl
from jax.experimental.pallas import tpu as pltpu
from jax.sharding import PartitionSpec as P

HEAD_DIM = 128
SEQ_LEN = 32768
GROUP = 10
MESH = pl.DeviceIdType.MESH
CHUNK = 512
WCHUNK = 256
TILE_N = 256


def rope_tables(rows, tok_dev, stride):
    half = HEAD_DIM // 2
    row = np.arange(rows)
    place = (row // tok_dev * stride + row % tok_dev).astype(np.float32)
    inverse = np.exp(
        -np.log(np.float32(1000000.0))
        * (np.float32(2.0) * np.arange(half).astype(np.float32) / np.float32(HEAD_DIM))
    ).astype(np.float32)
    angle = (place[:, None] * inverse[None, :]).astype(np.float32)
    cosine, sine = np.cos(angle).astype(np.float32), np.sin(angle).astype(np.float32)

    def by_column(t):
        t = t.reshape(rows // (2 * tok_dev), 2, tok_dev, HEAD_DIM)
        return np.ascontiguousarray(np.swapaxes(t, 0, 1)).reshape(2, rows // 2, HEAD_DIM)

    return np.stack([by_column(np.concatenate([cosine, cosine], 1)), by_column(np.concatenate([-sine, sine], 1))])


def kernel(
    nz, ndp,
    tok_h, gain_h, w_h, bias_h, grad_h, rope_h,
    qkv, total_ng, tok, gain, factors, gg_ref, bg_ref,
    w, bias, grad, rope,
    low, lowx, nx, held, part, run, rfin, acc, cx, qt, qx, ng, gtot, gx, gy, gstage, gsend, grecv, gdone, gres, bacc,
    in_sem, send_sem, one_sem, low_r, wy_r, wx_r, ag_r, end_r, c_r,
):
    f32, bf16 = jnp.float32, jnp.bfloat16
    dp, mp = lax.axis_index("dp"), lax.axis_index("mp")
    z, yl, core = mp // 2, lax.rem(mp, 2), lax.rem(dp, 2)
    nx_chips = ndp // 4
    row_of_x = dp // (2 * nx_chips) * (2 * nx_chips)
    x = lax.rem(dp // 2, nx_chips)
    odd = lax.rem(x, 2)
    rows, depth = tok.shape
    half = depth // 2
    col = nz * rows
    width = grad.shape[1]
    heads = width // HEAD_DIM
    chunks = half // CHUNK
    quarter = half // 4
    slab = half // nz

    def at(start, size, unit):
        return pl.ds(pl.multiple_of(start, unit), size)

    up = {"mp": lax.rem(z + 1, nz) * 2 + yl}
    down = {"mp": lax.rem(z + nz - 1, nz) * 2 + yl}
    pair = {"mp": mp + 1 - 2 * yl}
    far = {"dp": lax.rem(dp + ndp // 2, ndp), "mp": mp + 1 - 2 * yl}
    twin = {"dp": dp + 1 - 2 * core}
    east = {"dp": row_of_x + lax.rem(x + 1, nx_chips) * 2 + core}
    west = {"dp": row_of_x + lax.rem(x + nx_chips - 1, nx_chips) * 2 + core}
    along = (up, down)

    barrier = pltpu.get_barrier_semaphore()
    peers = (up, down, pair, far, twin, east, west)
    for there in peers:
        pl.semaphore_signal(barrier, inc=1, device_id=there, device_id_type=MESH)

    loads = []
    for i, (src, dst) in enumerate((
        (tok_h, tok), (gain_h, gain.at[0]), (grad_h, grad), (rope_h, rope),
        (bias_h, bias.at[0, pl.ds(0, width)]),
        (w_h.at[at(core * half, half, half), :], w.at[:, pl.ds(0, width)]),
    )):
        c = pltpu.make_async_copy(src, dst, in_sem.at[i])
        c.start()
        loads.append(c)

    def remote(src, dst, send, recv, there):
        return pltpu.make_async_remote_copy(
            src_ref=src, dst_ref=dst, send_sem=send_sem.at[send], recv_sem=recv,
            device_id=there, device_id_type=MESH,
        )

    own_cols, pair_cols = pl.ds(0, width), pl.ds(width, width)

    def w_send(a, there):
        i = 2 * a + odd
        return remote(
            w_h.at[at(core * half + i * WCHUNK, WCHUNK, WCHUNK), :],
            w.at[at(i * WCHUNK, WCHUNK, WCHUNK), pair_cols], 0, wy_r.at[a], there,
        )

    def w_pass(a):
        ref = w.at[at((2 * a + odd) * WCHUNK, WCHUNK, WCHUNK), pair_cols]
        return remote(ref, ref, 1, wx_r.at[a], east if a % 2 == 0 else west)

    def w_last():
        i = 2 * chunks - 1 - odd
        return remote(
            w_h.at[at(core * half + i * WCHUNK, WCHUNK, WCHUNK), :],
            w.at[at(i * WCHUNK, WCHUNK, WCHUNK), pair_cols], 0, wx_r.at[chunks - 1], pair,
        )

    def w_come(k):
        ref = w.at[at((2 * k + 1 - odd) * WCHUNK, WCHUNK, WCHUNK), pair_cols]
        return remote(ref, ref, 1, wx_r.at[k], east)

    mine = at(core * col, col, col)
    other = at((1 - core) * col, col, col)
    home = at(core * col + z * rows, rows, rows)
    nx_send = remote(nx, held.at[home, :], 2, one_sem.at[0], twin)

    def ag(way, j, e):
        d = lax.rem(core + e // 4, 2)
        b = lax.rem(z + (nz - j if way == 0 else j), nz)
        ref = held.at[at(d * col + b * rows, rows, rows), at(lax.rem(e, 4) * quarter, quarter, quarter)]
        on = jnp.where(lax.rem(e, 2) == way, 16 + e // 2, 20)
        place = jnp.where(j < 2, j * 8 + e, jnp.where(j == 2, on, 20))
        return remote(ref, ref, 3, ag_r.at[way, place], along[way])

    loads[0].wait()
    loads[1].wait()
    total = jnp.zeros((rows, 1), f32)
    for q in range(8):
        v = tok[:, q * quarter:(q + 1) * quarter].astype(f32)
        total = total + jnp.sum(v * v, axis=1, keepdims=True)
    scale = lax.rsqrt(total / depth + 1e-06)

    def normed(ks):
        return (tok[:, ks].astype(f32) * scale * gain[:, ks]).astype(bf16)

    for q in range(4):
        held[home, q * quarter:(q + 1) * quarter] = normed(at(core * half + q * quarter, quarter, quarter))
    for q in range(4):
        nx[:, q * quarter:(q + 1) * quarter] = normed(at((1 - core) * half + q * quarter, quarter, quarter))
    pl.semaphore_wait(barrier, len(peers))
    for q in range(4):
        for way in range(2):
            ag(way, 0, q).start()
    nx_send.start()
    bias_send = remote(bias_h, bias.at[0, pair_cols], 4, one_sem.at[1], pair)
    bias_send.start()
    for a in (0, 1, 3, 5, 7):
        w_send(a, far).start()

    loads[2].wait()
    loads[3].wait()
    bacc[...] = jnp.zeros_like(bacc)

    @pl.loop(0, nz)
    def _(b):
        for side, y in ((0, yl), (1, 1 - yl)):
            here = at((2 * b + y) * rows, rows, rows)
            there = at(b * rows, rows, rows)
            cs, sn = rope[0, y, there, :], rope[1, y, there, :]
            for h in range(heads):
                hs = slice(h * HEAD_DIM, (h + 1) * HEAD_DIM)
                v = grad[here, hs].astype(f32)
                turned = v * cs - pltpu.roll(v, HEAD_DIM // 2, 1) * sn
                plain = lax.rem(mp * heads + h, GROUP) == GROUP - 1
                v = jnp.where(plain, v, turned)
                bacc[:, hs] += jnp.sum(v.reshape(rows // 8, 8, HEAD_DIM), axis=0)
                if side == 0:
                    low[at(core * col + b * rows, rows, rows), hs] = v.astype(bf16)
                else:
                    lowx[there, hs] = v.astype(bf16)

    low_pair = remote(lowx, low.at[mine, pair_cols], 5, low_r.at[0], pair)
    low_twin = remote(low.at[mine, own_cols], low.at[mine, own_cols], 5, low_r.at[1], twin)
    low_fwd = remote(low.at[mine, pair_cols], low.at[mine, pair_cols], 5, low_r.at[2], twin)
    low_pair.start()
    low_twin.start()
    for a in (2, 4, 6):
        w_send(a, pair).start()
    w_last().start()
    nx_send.wait_recv()
    for q in range(4):
        for way in range(2):
            ag(way, 0, 4 + q).start()
    bg_ref[...] = jnp.sum(bacc[...], axis=0, keepdims=True)

    def cols(k):
        return at(k * CHUNK, CHUNK, CHUNK)

    def backward(k):
        @pl.when(k == chunks - 1)
        def _():
            w_send(chunks - 1, far).wait_recv()

        w_come(k).wait_recv()
        part[:, cols(k)] = lax.dot_general(
            low[...], w[cols(k), :], (((1,), (1,)), ((), ())), preferred_element_type=f32
        )

    def rs(way, j, k):
        place = j * 8 + jnp.where(j < 2, k, k // 2)
        return remote(
            run.at[way, j, :, cols(k)], run.at[way, j + 1, :, cols(k)], 6, ag_r.at[way, place], along[way]
        )

    def rs_end(way, j, k, d):
        return remote(
            run.at[way, j, pl.ds(d * rows, rows), cols(k)],
            rfin.at[way, :, at(core * half + k * CHUNK, CHUNK, CHUNK)],
            6, end_r.at[way, core, jnp.where(j < 3, 0, jnp.where(k < chunks - 2, 1, 2))], dict(along[way], dp=dp - core + d),
        )

    def hops(way, k):
        return jnp.where(lax.rem(k, 2) == way, 4, 3)

    def rs_step(way, j, k, first):
        left = hops(way, k) - j
        t = lax.rem(z + (left if way == 0 else nz - left), nz)
        if not first:
            rs(way, j - 1, k).wait_recv()
        for d in range(2):
            ds = pl.ds(d * rows, rows)
            v = part[at(d * col + t * rows, rows, rows), cols(k)]
            if not first:
                v = v + run[way, j, ds, cols(k)].astype(f32)
            run[way, j, ds, cols(k)] = v.astype(bf16)
        if first:
            rs(way, j, k).start()
            return

        @pl.when(left > 1)
        def _():
            rs(way, j, k).start()

        @pl.when(left == 1)
        def _():
            for d in range(2):
                rs_end(way, j, k, d).start()

    own_half = at(core * half, half, half)
    swap = remote(
        part.at[at((1 - core) * col + z * rows, rows, rows), :], ng.at[:, own_half], 7, one_sem.at[2], twin
    )

    def ended(group):
        count = (chunks // 2, chunks // 2 - 1, 1)[group]
        for way in range(2):
            for side in range(2):
                ref = rfin.at[way, :, pl.ds(0, count * CHUNK)]
                remote(ref, ref, 6, end_r.at[way, side, group], up).wait_recv()

    def gain_share(k):
        full = at(core * half + k * CHUNK, CHUNK, CHUNK)
        for ds, to, ks in ((mine, gtot, full), (other, gx, cols(k))):
            share = jnp.sum(part[ds, cols(k)] * held[ds, cols(k)].astype(f32), axis=0, keepdims=True)
            to[:, ks] = share / gain[:, full]

    gx_send = remote(gx, gtot.at[:, own_half], 8, one_sem.at[3], twin)
    gy_send = remote(gtot.at[:, at((1 - yl) * half, half, half)], gy, 13, one_sem.at[7], pair)
    column_half = at(yl * half, half, half)
    g3_send = remote(gres.at[:, column_half], gres.at[:, column_half], 14, one_sem.at[8], pair)

    lines = slab // HEAD_DIM

    def line_of(zz, i):
        return at(yl * half + zz * slab + i * HEAD_DIM, HEAD_DIM, HEAD_DIM)

    def g1(k):
        to = lax.rem(z + k, nz)
        return remote(gsend.at[to], grecv.at[k - 1], 9, one_sem.at[4], {"mp": 2 * to + yl})

    def g2(k):
        to = lax.rem(z + k, nz)
        return remote(gdone.at[z], gdone.at[z], 10, one_sem.at[5], {"mp": 2 * to + yl})

    g1_all = remote(grecv, grecv, 9, one_sem.at[4], up)
    g2_all = remote(grecv, grecv, 10, one_sem.at[5], up)

    def tile(t):
        return at(t * TILE_N, TILE_N, TILE_N)

    def c_send(t):
        return remote(acc.at[other, tile(t)], cx.at[:, tile(t)], 11, c_r.at[t], twin)

    def forward(t):
        acc[:, tile(t)] = jnp.dot(held[...], w[:, tile(t)], preferred_element_type=f32)
        c_send(t).start()

    def q_send(h):
        return remote(
            qt.at[:, at(width + h * HEAD_DIM, HEAD_DIM, HEAD_DIM)], qx.at[:, at(h * HEAD_DIM, HEAD_DIM, HEAD_DIM)],
            12, one_sem.at[6], pair,
        )

    q_all = remote(qx, qx, 12, one_sem.at[6], pair)

    def joined(t):
        c_send(t).wait_recv()
        for i in range(TILE_N // HEAD_DIM):
            h = t * (TILE_N // HEAD_DIM) + i
            hs = at(h * HEAD_DIM, HEAD_DIM, HEAD_DIM)
            v = acc[mine, hs] + cx[:, hs] + bias[:, hs]
            turned = v * rope[0, yl] + pltpu.roll(v, HEAD_DIM // 2, 1) * rope[1, yl]
            whole = jnp.where(h < heads, mp * heads + h, (mp + 1 - 2 * yl) * heads + h - heads)
            qt[:, hs] = jnp.where(lax.rem(whole, GROUP) == GROUP - 1, v, turned).astype(bf16)

            @pl.when(h >= heads)
            def _():
                q_send(h - heads).start()

    passes = (4, 9, 11, 14, 16, 19, 21)
    early = (12, 17, 18, 22, 23)
    ahead = 4

    @pl.loop(0, 24)
    def _(i):
        j, e = 1 + i // 8, lax.rem(i, 8)
        for way in range(2):
            @pl.when((j < 3) | (lax.rem(e, 2) == way))
            def _():
                ag(way, j - 1, e).wait_recv()
                ag(way, j, e).start()

        @pl.when(i >= 24 - ahead)
        def _():
            for way in range(2):
                rs_step(way, 0, i - (24 - ahead), True)

        for a, step in enumerate(passes):
            @pl.when(i == step)
            def _():
                w_send(a, pair).wait_recv()
                w_pass(a).start()

        @pl.when(i == 6)
        def _():
            low_pair.wait_recv()
            low_fwd.start()

        @pl.when(i == 9)
        def _():
            loads[5].wait()
            low_twin.wait_recv()
            low_fwd.wait_recv()

        k, due = 0, i == early[0]
        for m in range(1, len(early)):
            k, due = jnp.where(i >= early[m], m, k), due | (i == early[m])

        @pl.when(due)
        def _():
            backward(k)

    @pl.loop(ahead, chunks)
    def _(m):
        k = jnp.where(m < chunks - 2, m, 2 * chunks - 3 - m)

        @pl.when(m >= len(early))
        def _():
            backward(k)

        for way in range(2):
            rs_step(way, 0, k, True)

    swap.start()
    for q in range(4):
        ks = pl.ds(q * quarter, quarter)
        ng[:, at(core * half + q * quarter, quarter, quarter)] = part[home, ks]
    for way in range(2):
        ref = held.at[pl.ds(0, 2 * rows), :]
        remote(ref, ref, 3, ag_r.at[way, 20], up).wait_recv()
    loads[4].wait()
    bias_send.wait_recv()

    @pl.loop(0, chunks)
    def _(k):
        gain_share(k)

    gx_send.start()

    @pl.loop(0, 20)
    def _(m):
        j, q = 1 + m // 8, lax.rem(m, 8)
        for way in range(2):
            rs_step(way, j, jnp.where(j < 3, q, 2 * q + way), False)

        @pl.when((m >= 2) & (m < 7))
        def _():
            joined(lax.rem(m, 5))

        @pl.when(m < 5)
        def _():
            forward(lax.rem(m + 2, 5))

        @pl.when(m == 1)
        def _():
            gx_send.wait_recv()
            gy_send.start()

        @pl.when(m == 4)
        def _():
            gy_send.wait_recv()
            gtot[:, column_half] += gy[...]
            for zz in range(nz):
                for i in range(lines):
                    gstage[zz, i:i + 1, :] = gtot[:, line_of(zz, i)]
            gsend[...] = gstage[...].astype(bf16)
            for k in range(1, nz):
                g1(k).start()

        @pl.when(m == 13)
        def _():
            g1_all.wait_recv()
            share = gstage[z]
            for k in range(1, nz):
                share = share + grecv[k - 1].astype(f32)
            gdone[z] = share.astype(bf16)
            for k in range(1, nz):
                g2(k).start()

        @pl.when(m == 16)
        def _():
            q_all.wait_recv()
            for b in range(nz):
                there = pl.ds(b * rows, rows)
                qkv[at((2 * b + yl) * rows, rows, rows), :] = qt[there, own_cols]
                qkv[at((2 * b + 1 - yl) * rows, rows, rows), :] = qx[there, :]

    g2_all.wait_recv()
    gstage[...] = gdone[...].astype(f32)
    for zz in range(nz):
        for i in range(lines):
            gres[:, line_of(zz, i)] = gstage[zz, i:i + 1, :]
    g3_send.start()
    swap.wait_recv()
    ended(0)
    for q in range(2 * chunks):
        ks = slice(q * CHUNK, (q + 1) * CHUNK)
        ng[:, ks] += rfin[1 - q % 2, :, ks].astype(f32)
    inner = jnp.zeros((rows, 1), f32)
    for group, ks_in in ((1, range(chunks - 2)), (2, range(chunks - 2, chunks))):
        ended(group)
        for side in range(2):
            for k in ks_in:
                q = side * chunks + k
                ks = slice(q * CHUNK, (q + 1) * CHUNK)
                v = ng[:, ks] + rfin[k % 2, :, ks].astype(f32)
                total_ng[:, ks] = v
                inner = inner + jnp.sum(v * tok[:, ks].astype(f32) * gain[:, ks], axis=1, keepdims=True)
    factors[0] = jnp.broadcast_to(scale, factors.shape[1:])
    factors[1] = jnp.broadcast_to(scale * scale * scale * (inner / depth), factors.shape[1:])

    g3_send.wait_recv()
    gg_ref[...] = gres[...]

    def sent(ref, send):
        remote(ref, ref, send, one_sem.at[0], twin).wait_send()

    sent(w_h.at[pl.ds(0, (chunks + 1) * WCHUNK), :], 0)
    sent(w_h.at[pl.ds(0, (chunks - 1) * WCHUNK), :], 1)
    sent(nx, 2)
    moved = held.at[pl.ds(0, 7 * 2 * rows), :]
    sent(moved, 3)
    bias_send.wait_send()
    sent(w_h.at[pl.ds(0, 3 * col), :], 5)
    sent(moved, 6)
    swap.wait_send()
    sent(gx, 8)
    sent(grecv, 9)
    sent(grecv, 10)
    sent(cx, 11)
    sent(qx, 12)
    gy_send.wait_send()
    g3_send.wait_send()


def finish(qkv, ng, tok, gain, factors, gg, bg, qkv_h, tg_h, gg_h, bg_h, tg, sem):
    parts = sem.shape[0] - 3
    piece = tok.shape[1] // parts
    copies = [
        pltpu.make_async_copy(src, dst, sem.at[i])
        for i, (src, dst) in enumerate(((qkv, qkv_h), (gg.at[0], gg_h), (bg.at[0], bg_h)))
    ]
    for c in copies:
        c.start()
    scale, weight = factors[0, :, :1], factors[1, :, :1]
    for q in range(parts):
        ks = slice(q * piece, (q + 1) * piece)
        tg[:, ks] = scale * gain[:, ks] * ng[:, ks] - tok[:, ks].astype(jnp.float32) * weight
        c = pltpu.make_async_copy(tg.at[:, ks], tg_h.at[:, ks], sem.at[3 + q])
        c.start()
        copies.append(c)
    for c in copies:
        c.wait()


def shards(n, ndp, tokens, norm_gain, qkv_weight, qkv_bias, qkv_grad):
    rows, depth = tokens.shape
    every, width = qkv_grad.shape
    rope = rope_tables(every, rows, SEQ_LEN // n)
    bf16, f32 = jnp.bfloat16, jnp.float32
    half, col, nz = depth // 2, every // 2, n // 2
    slab = half // nz
    chunks = half // CHUNK
    tiles = 2 * width // TILE_N
    dma = pltpu.SemaphoreType.DMA
    vm = pltpu.VMEM
    hbm = pl.BlockSpec(memory_space=pl.ANY)
    vmem = pl.BlockSpec(memory_space=pltpu.VMEM)
    results = pl.pallas_call(
        functools.partial(kernel, nz, ndp),
        out_shape=(
            vm((every, width), bf16),
            vm((rows, depth), f32),
            vm((rows, depth), bf16),
            vm((1, depth), f32),
            vm((2, rows, HEAD_DIM), f32),
            vm((1, depth), f32),
            vm((1, width), f32),
        ),
        in_specs=[hbm] * 6,
        out_specs=[vmem] * 7,
        scratch_shapes=[
            vm((half, 2 * width), bf16),
            vm((1, 2 * width), f32),
            vm((every, width), bf16),
            vm((2, 2, col, HEAD_DIM), f32),
            vm((every, 2 * width), bf16),
            vm((col, width), bf16),
            vm((rows, half), bf16),
            vm((every, half), bf16),
            vm((every, half), f32),
            vm((2, 4, 2 * rows, half), bf16),
            vm((2, rows, depth), bf16),
            vm((every, 2 * width), f32),
            vm((col, 2 * width), f32),
            vm((col, 2 * width), bf16),
            vm((col, width), bf16),
            vm((rows, depth), f32),
            vm((1, depth), f32),
            vm((1, half), f32),
            vm((1, half), f32),
            vm((nz, slab // HEAD_DIM, HEAD_DIM), f32),
            vm((nz, slab // HEAD_DIM, HEAD_DIM), bf16),
            vm((nz - 1, slab // HEAD_DIM, HEAD_DIM), bf16),
            vm((nz, slab // HEAD_DIM, HEAD_DIM), bf16),
            vm((1, depth), f32),
            vm((8, width), f32),
            dma((6,)),
            dma((15,)),
            dma((9,)),
            dma((3,)),
            dma((chunks,)),
            dma((chunks,)),
            dma((2, 21)),
            dma((2, 2, 3)),
            dma((tiles,)),
        ],
        compiler_params=pltpu.CompilerParams(
            collective_id=0, has_side_effects=True, vmem_limit_bytes=60000000
        ),
        cost_estimate=pl.CostEstimate(
            flops=4 * every * depth * width, bytes_accessed=2 * depth * width, transcendentals=0
        ),
    )(
        tokens, norm_gain, qkv_weight, qkv_bias, qkv_grad,
        jnp.asarray(rope),
    )
    return pl.pallas_call(
        finish,
        out_shape=(
            jax.ShapeDtypeStruct((every, width), bf16),
            jax.ShapeDtypeStruct((rows, depth), f32),
            jax.ShapeDtypeStruct((depth,), f32),
            jax.ShapeDtypeStruct((width,), f32),
        ),
        in_specs=[vmem] * 7,
        out_specs=[hbm] * 4,
        scratch_shapes=[vm((rows, depth), f32), dma((7,))],
        compiler_params=pltpu.CompilerParams(vmem_limit_bytes=1 << 21),
    )(*results)


def solution(mesh):
    in_specs = (P(("dp", "mp"), None), P(), P(None, "mp"), P("mp"), P("dp", "mp"))
    out_specs = (P("dp", "mp"), P(("dp", "mp"), None), P("dp"), P(("dp", "mp")))
    body = functools.partial(shards, mesh.shape["mp"], mesh.shape["dp"])
    return jax.shard_map(body, mesh=mesh, in_specs=in_specs, out_specs=out_specs, check_vma=False)
```

```python
import functools

import jax
import jax.numpy as jnp
import numpy as np
from jax import lax
from jax.experimental import pallas as pl
from jax.experimental.pallas import tpu as pltpu
from jax.sharding import PartitionSpec as P

HEAD_DIM = 128
SEQ_LEN = 32768
GROUP = 10
MESH = pl.DeviceIdType.MESH
CHUNK = 512
WCHUNK = 256
TILE_N = 256


def rope_tables(rows, tok_dev, stride):
    half = HEAD_DIM // 2
    row = np.arange(rows)
    place = (row // tok_dev * stride + row % tok_dev).astype(np.float32)
    inverse = np.exp(
        -np.log(np.float32(1000000.0))
        * (np.float32(2.0) * np.arange(half).astype(np.float32) / np.float32(HEAD_DIM))
    ).astype(np.float32)
    angle = (place[:, None] * inverse[None, :]).astype(np.float32)
    cosine, sine = np.cos(angle).astype(np.float32), np.sin(angle).astype(np.float32)

    def by_column(t):
        t = t.reshape(rows // (2 * tok_dev), 2, tok_dev, HEAD_DIM)
        return np.ascontiguousarray(np.swapaxes(t, 0, 1)).reshape(2, rows // 2, HEAD_DIM)

    return np.stack([by_column(np.concatenate([cosine, cosine], 1)), by_column(np.concatenate([-sine, sine], 1))])


def kernel(
    nz, ndp,
    tok_h, gain_h, w_h, bias_h, grad_h, rope_h,
    qkv, total_ng, tok, gain, factors, gg_ref, bg_ref,
    w, bias, grad, rope,
    low, lowx, nx, held, part, run, rfin, acc, cx, qt, qx, ng, gtot, gx, gy, gstage, gsend, grecv, gdone, gres, bacc,
    in_sem, send_sem, one_sem, low_r, wy_r, wx_r, ag_r, end_r, turn_r, c_r,
):
    f32, bf16 = jnp.float32, jnp.bfloat16
    dp, mp = lax.axis_index("dp"), lax.axis_index("mp")
    z, yl, core = mp // 2, lax.rem(mp, 2), lax.rem(dp, 2)
    nx_chips = ndp // 4
    row_of_x = dp // (2 * nx_chips) * (2 * nx_chips)
    x = lax.rem(dp // 2, nx_chips)
    odd = lax.rem(x, 2)
    rows, depth = tok.shape
    half = depth // 2
    col = nz * rows
    width = grad.shape[1]
    heads = width // HEAD_DIM
    chunks = half // CHUNK
    quarter = half // 4
    slab = half // nz

    def at(start, size, unit):
        return pl.ds(pl.multiple_of(start, unit), size)

    up = {"mp": lax.rem(z + 1, nz) * 2 + yl}
    down = {"mp": lax.rem(z + nz - 1, nz) * 2 + yl}
    pair = {"mp": mp + 1 - 2 * yl}
    far = {"dp": lax.rem(dp + ndp // 2, ndp), "mp": mp + 1 - 2 * yl}
    twin = {"dp": dp + 1 - 2 * core}
    east = {"dp": row_of_x + lax.rem(x + 1, nx_chips) * 2 + core}
    west = {"dp": row_of_x + lax.rem(x + nx_chips - 1, nx_chips) * 2 + core}
    along = (up, down)

    barrier = pltpu.get_barrier_semaphore()
    peers = (up, down, pair, far, twin, east, west)
    for there in peers:
        pl.semaphore_signal(barrier, inc=1, device_id=there, device_id_type=MESH)

    loads = []
    for i, (src, dst) in enumerate((
        (tok_h, tok), (gain_h, gain.at[0]), (grad_h, grad), (rope_h, rope),
        (bias_h, bias.at[0, pl.ds(0, width)]),
        (w_h.at[at(core * half, half, half), :], w.at[:, pl.ds(0, width)]),
    )):
        c = pltpu.make_async_copy(src, dst, in_sem.at[i])
        c.start()
        loads.append(c)

    def remote(src, dst, send, recv, there):
        return pltpu.make_async_remote_copy(
            src_ref=src, dst_ref=dst, send_sem=send_sem.at[send], recv_sem=recv,
            device_id=there, device_id_type=MESH,
        )

    own_cols, pair_cols = pl.ds(0, width), pl.ds(width, width)

    def w_send(a, there):
        i = 2 * a + odd
        return remote(
            w_h.at[at(core * half + i * WCHUNK, WCHUNK, WCHUNK), :],
            w.at[at(i * WCHUNK, WCHUNK, WCHUNK), pair_cols], 0, wy_r.at[a], there,
        )

    def w_pass(a):
        ref = w.at[at((2 * a + odd) * WCHUNK, WCHUNK, WCHUNK), pair_cols]
        return remote(ref, ref, 1, wx_r.at[a], east if a % 2 == 0 else west)

    def w_last():
        i = 2 * chunks - 1 - odd
        return remote(
            w_h.at[at(core * half + i * WCHUNK, WCHUNK, WCHUNK), :],
            w.at[at(i * WCHUNK, WCHUNK, WCHUNK), pair_cols], 0, wx_r.at[chunks - 1], pair,
        )

    def w_come(k):
        ref = w.at[at((2 * k + 1 - odd) * WCHUNK, WCHUNK, WCHUNK), pair_cols]
        return remote(ref, ref, 1, wx_r.at[k], east)

    mine = at(core * col, col, col)
    other = at((1 - core) * col, col, col)
    home = at(core * col + z * rows, rows, rows)
    nx_send = remote(nx, held.at[home, :], 2, one_sem.at[0], twin)

    def ag(way, j, e):
        d = lax.rem(core + e // 4, 2)
        b = lax.rem(z + (nz - j if way == 0 else j), nz)
        ref = held.at[at(d * col + b * rows, rows, rows), at(lax.rem(e, 4) * quarter, quarter, quarter)]
        on = jnp.where(lax.rem(e, 2) == way, 16 + e // 2, 20)
        place = jnp.where(j < 2, j * 8 + e, jnp.where(j == 2, on, 20))
        return remote(ref, ref, 3, ag_r.at[way, place], along[way])

    loads[0].wait()
    loads[1].wait()
    total = jnp.zeros((rows, 1), f32)
    for q in range(8):
        v = tok[:, q * quarter:(q + 1) * quarter].astype(f32)
        total = total + jnp.sum(v * v, axis=1, keepdims=True)
    scale = lax.rsqrt(total / depth + 1e-06)

    def normed(ks):
        return (tok[:, ks].astype(f32) * scale * gain[:, ks]).astype(bf16)

    for q in range(4):
        held[home, q * quarter:(q + 1) * quarter] = normed(at(core * half + q * quarter, quarter, quarter))
    for q in range(4):
        nx[:, q * quarter:(q + 1) * quarter] = normed(at((1 - core) * half + q * quarter, quarter, quarter))
    pl.semaphore_wait(barrier, len(peers))
    for q in range(4):
        for way in range(2):
            ag(way, 0, q).start()
    nx_send.start()
    bias_send = remote(bias_h, bias.at[0, pair_cols], 4, one_sem.at[1], pair)
    bias_send.start()
    for a in (0, 1, 3, 5, 7):
        w_send(a, far).start()

    loads[2].wait()
    loads[3].wait()
    bacc[...] = jnp.zeros_like(bacc)

    @pl.loop(0, nz)
    def _(b):
        for side, y in ((0, yl), (1, 1 - yl)):
            here = at((2 * b + y) * rows, rows, rows)
            there = at(b * rows, rows, rows)
            cs, sn = rope[0, y, there, :], rope[1, y, there, :]
            for h in range(heads):
                hs = slice(h * HEAD_DIM, (h + 1) * HEAD_DIM)
                v = grad[here, hs].astype(f32)
                turned = v * cs - pltpu.roll(v, HEAD_DIM // 2, 1) * sn
                plain = lax.rem(mp * heads + h, GROUP) == GROUP - 1
                v = jnp.where(plain, v, turned)
                bacc[:, hs] += jnp.sum(v.reshape(rows // 8, 8, HEAD_DIM), axis=0)
                if side == 0:
                    low[at(core * col + b * rows, rows, rows), hs] = v.astype(bf16)
                else:
                    lowx[there, hs] = v.astype(bf16)

    low_pair = remote(lowx, low.at[mine, pair_cols], 5, low_r.at[0], pair)
    low_twin = remote(low.at[mine, own_cols], low.at[mine, own_cols], 5, low_r.at[1], twin)
    low_fwd = remote(low.at[mine, pair_cols], low.at[mine, pair_cols], 5, low_r.at[2], twin)
    low_pair.start()
    low_twin.start()
    for a in (2, 4, 6):
        w_send(a, pair).start()
    w_last().start()
    nx_send.wait_recv()
    for q in range(4):
        for way in range(2):
            ag(way, 0, 4 + q).start()
    bg_ref[...] = jnp.sum(bacc[...], axis=0, keepdims=True)

    def cols(k):
        return at(k * CHUNK, CHUNK, CHUNK)

    def backward(k):
        @pl.when(k == chunks - 1)
        def _():
            w_send(chunks - 1, far).wait_recv()

        w_come(k).wait_recv()
        part[:, cols(k)] = lax.dot_general(
            low[...], w[cols(k), :], (((1,), (1,)), ((), ())), preferred_element_type=f32
        )

    def rs(way, j, k):
        place = j * 8 + jnp.where(j < 2, k, k // 2)
        return remote(
            run.at[way, j, :, cols(k)], run.at[way, j + 1, :, cols(k)], 6, ag_r.at[way, place], along[way]
        )

    def rs_end(way, j, k, d):
        return remote(
            run.at[way, j, pl.ds(d * rows, rows), cols(k)],
            rfin.at[way, :, at(core * half + k * CHUNK, CHUNK, CHUNK)],
            6, end_r.at[way, core, jnp.where(j < 3, 0, jnp.where(k < chunks - 2, 1, 2))], dict(along[way], dp=dp - core + d),
        )

    def hops(way, k):
        return jnp.where(lax.rem(k, 2) == way, 4, 3)

    turning = (nz - 1, 1)

    def turned(way):
        return remote(
            run.at[way, 0, :, cols(way)], run.at[1 - way, 0, :, cols(way)], 6, turn_r.at[way], along[1 - way]
        )

    def rs_term(way, j, k, more):
        left = hops(way, k) - j
        t = lax.rem(z + (left if way == 0 else nz - left), nz)
        for d in range(2):
            ds = pl.ds(d * rows, rows)
            v = part[at(d * col + t * rows, rows, rows), cols(k)]
            if more:
                v = v + run[way, j, ds, cols(k)].astype(f32)
            run[way, j, ds, cols(k)] = v.astype(bf16)

    def rs_turn(way):
        @pl.when(z == turning[way])
        def _():
            rs_term(way, 0, way, False)
            turned(way).start()

    def rs_first(way, k):
        joins = (k == 1 - way) & (z == (2, nz - 2)[way])

        @pl.when((k != way) | (z != turning[way]))
        def _():
            @pl.when(joins)
            def _():
                turned(1 - way).wait_recv()
                rs_term(way, 0, k, True)

            @pl.when(jnp.logical_not(joins))
            def _():
                rs_term(way, 0, k, False)

            rs(way, 0, k).start()

    def rs_step(way, j, k):
        left = hops(way, k) - j
        starts = (j == 1) & (k == way) & (z == 0)

        @pl.when(starts)
        def _():
            rs_term(way, j, k, False)

        @pl.when(jnp.logical_not(starts))
        def _():
            rs(way, j - 1, k).wait_recv()
            rs_term(way, j, k, True)

        @pl.when(left > 1)
        def _():
            rs(way, j, k).start()

        @pl.when(left == 1)
        def _():
            for d in range(2):
                rs_end(way, j, k, d).start()

    own_half = at(core * half, half, half)
    swap = remote(
        part.at[at((1 - core) * col + z * rows, rows, rows), :], ng.at[:, own_half], 7, one_sem.at[2], twin
    )

    def ended(group):
        count = (chunks // 2, chunks // 2 - 1, 1)[group]
        for way in range(2):
            for side in range(2):
                ref = rfin.at[way, :, pl.ds(0, count * CHUNK)]
                remote(ref, ref, 6, end_r.at[way, side, group], up).wait_recv()

    def gain_share(k):
        full = at(core * half + k * CHUNK, CHUNK, CHUNK)
        for ds, to, ks in ((mine, gtot, full), (other, gx, cols(k))):
            share = jnp.sum(part[ds, cols(k)] * held[ds, cols(k)].astype(f32), axis=0, keepdims=True)
            to[:, ks] = share / gain[:, full]

    gx_send = remote(gx, gtot.at[:, own_half], 8, one_sem.at[3], twin)
    gy_send = remote(gtot.at[:, at((1 - yl) * half, half, half)], gy, 13, one_sem.at[7], pair)
    column_half = at(yl * half, half, half)
    g3_send = remote(gres.at[:, column_half], gres.at[:, column_half], 14, one_sem.at[8], pair)

    lines = slab // HEAD_DIM

    def line_of(zz, i):
        return at(yl * half + zz * slab + i * HEAD_DIM, HEAD_DIM, HEAD_DIM)

    def g1(k):
        to = lax.rem(z + k, nz)
        return remote(gsend.at[to], grecv.at[k - 1], 9, one_sem.at[4], {"mp": 2 * to + yl})

    def g2(k):
        to = lax.rem(z + k, nz)
        return remote(gdone.at[z], gdone.at[z], 10, one_sem.at[5], {"mp": 2 * to + yl})

    g1_all = remote(grecv, grecv, 9, one_sem.at[4], up)
    g2_all = remote(grecv, grecv, 10, one_sem.at[5], up)

    def tile(t):
        return at(t * TILE_N, TILE_N, TILE_N)

    def c_send(t):
        return remote(acc.at[other, tile(t)], cx.at[:, tile(t)], 11, c_r.at[t], twin)

    def forward(t):
        acc[:, tile(t)] = jnp.dot(held[...], w[:, tile(t)], preferred_element_type=f32)
        c_send(t).start()

    def q_send(h):
        return remote(
            qt.at[:, at(width + h * HEAD_DIM, HEAD_DIM, HEAD_DIM)], qx.at[:, at(h * HEAD_DIM, HEAD_DIM, HEAD_DIM)],
            12, one_sem.at[6], pair,
        )

    q_all = remote(qx, qx, 12, one_sem.at[6], pair)

    def joined(t):
        c_send(t).wait_recv()
        for i in range(TILE_N // HEAD_DIM):
            h = t * (TILE_N // HEAD_DIM) + i
            hs = at(h * HEAD_DIM, HEAD_DIM, HEAD_DIM)
            v = acc[mine, hs] + cx[:, hs] + bias[:, hs]
            turned = v * rope[0, yl] + pltpu.roll(v, HEAD_DIM // 2, 1) * rope[1, yl]
            whole = jnp.where(h < heads, mp * heads + h, (mp + 1 - 2 * yl) * heads + h - heads)
            qt[:, hs] = jnp.where(lax.rem(whole, GROUP) == GROUP - 1, v, turned).astype(bf16)

            @pl.when(h >= heads)
            def _():
                q_send(h - heads).start()

    passes = (4, 9, 11, 14, 16, 19, 21)
    early = (12, 17, 18, 22, 23)
    ahead = 3

    @pl.loop(0, 24)
    def _(i):
        j, e = 1 + i // 8, lax.rem(i, 8)
        for way in range(2):
            @pl.when((j < 3) | (lax.rem(e, 2) == way))
            def _():
                ag(way, j - 1, e).wait_recv()
                ag(way, j, e).start()

        @pl.when(i >= 24 - ahead)
        def _():
            k = i - (24 - ahead)
            for way in range(2):
                rs_first(way, jnp.where(k < 1, k, k + 1))

        @pl.when(i == 13)
        def _():
            rs_turn(0)

        @pl.when(i == 18)
        def _():
            rs_turn(1)

        for a, step in enumerate(passes):
            @pl.when(i == step)
            def _():
                w_send(a, pair).wait_recv()
                w_pass(a).start()

        @pl.when(i == 6)
        def _():
            low_pair.wait_recv()
            low_fwd.start()

        @pl.when(i == 9)
        def _():
            loads[5].wait()
            low_twin.wait_recv()
            low_fwd.wait_recv()

        k, due = 0, i == early[0]
        for m in range(1, len(early)):
            k, due = jnp.where(i >= early[m], m, k), due | (i == early[m])

        @pl.when(due)
        def _():
            backward(k)

    @pl.loop(ahead, chunks)
    def _(m):
        k = jnp.where(m == ahead, 1, jnp.where(m < chunks - 2, m, 2 * chunks - 3 - m))

        @pl.when(m >= len(early))
        def _():
            backward(k)

        for way in range(2):
            rs_first(way, k)

    swap.start()
    for q in range(4):
        ks = pl.ds(q * quarter, quarter)
        ng[:, at(core * half + q * quarter, quarter, quarter)] = part[home, ks]
    for way in range(2):
        ref = held.at[pl.ds(0, 2 * rows), :]
        remote(ref, ref, 3, ag_r.at[way, 20], up).wait_recv()
    loads[4].wait()
    bias_send.wait_recv()

    @pl.loop(0, chunks)
    def _(k):
        gain_share(k)

    gx_send.start()

    @pl.loop(0, 20)
    def _(m):
        j, q = 1 + m // 8, lax.rem(m, 8)
        for way in range(2):
            rs_step(way, j, jnp.where(j < 3, q, 2 * q + way))

        @pl.when((m >= 2) & (m < 7))
        def _():
            joined(lax.rem(m, 5))

        @pl.when(m < 5)
        def _():
            forward(lax.rem(m + 2, 5))

        @pl.when(m == 1)
        def _():
            gx_send.wait_recv()
            gy_send.start()

        @pl.when(m == 4)
        def _():
            gy_send.wait_recv()
            gtot[:, column_half] += gy[...]
            for zz in range(nz):
                for i in range(lines):
                    gstage[zz, i:i + 1, :] = gtot[:, line_of(zz, i)]
            gsend[...] = gstage[...].astype(bf16)
            for k in range(1, nz):
                g1(k).start()

        @pl.when(m == 13)
        def _():
            g1_all.wait_recv()
            share = gstage[z]
            for k in range(1, nz):
                share = share + grecv[k - 1].astype(f32)
            gdone[z] = share.astype(bf16)
            for k in range(1, nz):
                g2(k).start()

        @pl.when(m == 16)
        def _():
            q_all.wait_recv()
            for b in range(nz):
                there = pl.ds(b * rows, rows)
                qkv[at((2 * b + yl) * rows, rows, rows), :] = qt[there, own_cols]
                qkv[at((2 * b + 1 - yl) * rows, rows, rows), :] = qx[there, :]

    g2_all.wait_recv()
    gstage[...] = gdone[...].astype(f32)
    for zz in range(nz):
        for i in range(lines):
            gres[:, line_of(zz, i)] = gstage[zz, i:i + 1, :]
    g3_send.start()
    swap.wait_recv()
    ended(0)
    for q in range(2 * chunks):
        ks = slice(q * CHUNK, (q + 1) * CHUNK)
        ng[:, ks] += rfin[1 - q % 2, :, ks].astype(f32)
    inner = jnp.zeros((rows, 1), f32)
    for group, ks_in in ((1, range(chunks - 2)), (2, range(chunks - 2, chunks))):
        ended(group)
        for side in range(2):
            for k in ks_in:
                q = side * chunks + k
                ks = slice(q * CHUNK, (q + 1) * CHUNK)
                v = ng[:, ks] + rfin[k % 2, :, ks].astype(f32)
                total_ng[:, ks] = v
                inner = inner + jnp.sum(v * tok[:, ks].astype(f32) * gain[:, ks], axis=1, keepdims=True)
    factors[0] = jnp.broadcast_to(scale, factors.shape[1:])
    factors[1] = jnp.broadcast_to(scale * scale * scale * (inner / depth), factors.shape[1:])

    g3_send.wait_recv()
    gg_ref[...] = gres[...]

    def sent(ref, send):
        remote(ref, ref, send, one_sem.at[0], twin).wait_send()

    sent(w_h.at[pl.ds(0, (chunks + 1) * WCHUNK), :], 0)
    sent(w_h.at[pl.ds(0, (chunks - 1) * WCHUNK), :], 1)
    sent(nx, 2)
    moved = held.at[pl.ds(0, 7 * 2 * rows), :]
    sent(moved, 3)
    bias_send.wait_send()
    sent(w_h.at[pl.ds(0, 3 * col), :], 5)
    sent(moved, 6)
    swap.wait_send()
    sent(gx, 8)
    sent(grecv, 9)
    sent(grecv, 10)
    sent(cx, 11)
    sent(qx, 12)
    gy_send.wait_send()
    g3_send.wait_send()


def finish(qkv, ng, tok, gain, factors, gg, bg, qkv_h, tg_h, gg_h, bg_h, tg, sem):
    parts = sem.shape[0] - 3
    piece = tok.shape[1] // parts
    copies = [
        pltpu.make_async_copy(src, dst, sem.at[i])
        for i, (src, dst) in enumerate(((qkv, qkv_h), (gg.at[0], gg_h), (bg.at[0], bg_h)))
    ]
    for c in copies:
        c.start()
    scale, weight = factors[0, :, :1], factors[1, :, :1]
    for q in range(parts):
        ks = slice(q * piece, (q + 1) * piece)
        tg[:, ks] = scale * gain[:, ks] * ng[:, ks] - tok[:, ks].astype(jnp.float32) * weight
        c = pltpu.make_async_copy(tg.at[:, ks], tg_h.at[:, ks], sem.at[3 + q])
        c.start()
        copies.append(c)
    for c in copies:
        c.wait()


def shards(n, ndp, tokens, norm_gain, qkv_weight, qkv_bias, qkv_grad):
    rows, depth = tokens.shape
    every, width = qkv_grad.shape
    rope = rope_tables(every, rows, SEQ_LEN // n)
    bf16, f32 = jnp.bfloat16, jnp.float32
    half, col, nz = depth // 2, every // 2, n // 2
    slab = half // nz
    chunks = half // CHUNK
    tiles = 2 * width // TILE_N
    dma = pltpu.SemaphoreType.DMA
    vm = pltpu.VMEM
    hbm = pl.BlockSpec(memory_space=pl.ANY)
    vmem = pl.BlockSpec(memory_space=pltpu.VMEM)
    results = pl.pallas_call(
        functools.partial(kernel, nz, ndp),
        out_shape=(
            vm((every, width), bf16),
            vm((rows, depth), f32),
            vm((rows, depth), bf16),
            vm((1, depth), f32),
            vm((2, rows, HEAD_DIM), f32),
            vm((1, depth), f32),
            vm((1, width), f32),
        ),
        in_specs=[hbm] * 6,
        out_specs=[vmem] * 7,
        scratch_shapes=[
            vm((half, 2 * width), bf16),
            vm((1, 2 * width), f32),
            vm((every, width), bf16),
            vm((2, 2, col, HEAD_DIM), f32),
            vm((every, 2 * width), bf16),
            vm((col, width), bf16),
            vm((rows, half), bf16),
            vm((every, half), bf16),
            vm((every, half), f32),
            vm((2, 4, 2 * rows, half), bf16),
            vm((2, rows, depth), bf16),
            vm((every, 2 * width), f32),
            vm((col, 2 * width), f32),
            vm((col, 2 * width), bf16),
            vm((col, width), bf16),
            vm((rows, depth), f32),
            vm((1, depth), f32),
            vm((1, half), f32),
            vm((1, half), f32),
            vm((nz, slab // HEAD_DIM, HEAD_DIM), f32),
            vm((nz, slab // HEAD_DIM, HEAD_DIM), bf16),
            vm((nz - 1, slab // HEAD_DIM, HEAD_DIM), bf16),
            vm((nz, slab // HEAD_DIM, HEAD_DIM), bf16),
            vm((1, depth), f32),
            vm((8, width), f32),
            dma((6,)),
            dma((15,)),
            dma((9,)),
            dma((3,)),
            dma((chunks,)),
            dma((chunks,)),
            dma((2, 21)),
            dma((2, 2, 3)),
            dma((2,)),
            dma((tiles,)),
        ],
        compiler_params=pltpu.CompilerParams(
            collective_id=0, has_side_effects=True, vmem_limit_bytes=60000000
        ),
        cost_estimate=pl.CostEstimate(
            flops=4 * every * depth * width, bytes_accessed=2 * depth * width, transcendentals=0
        ),
    )(
        tokens, norm_gain, qkv_weight, qkv_bias, qkv_grad,
        jnp.asarray(rope),
    )
    return pl.pallas_call(
        finish,
        out_shape=(
            jax.ShapeDtypeStruct((every, width), bf16),
            jax.ShapeDtypeStruct((rows, depth), f32),
            jax.ShapeDtypeStruct((depth,), f32),
            jax.ShapeDtypeStruct((width,), f32),
        ),
        in_specs=[vmem] * 7,
        out_specs=[hbm] * 4,
        scratch_shapes=[vm((rows, depth), f32), dma((7,))],
        compiler_params=pltpu.CompilerParams(vmem_limit_bytes=1 << 21),
    )(*results)


def solution(mesh):
    in_specs = (P(("dp", "mp"), None), P(), P(None, "mp"), P("mp"), P("dp", "mp"))
    out_specs = (P("dp", "mp"), P(("dp", "mp"), None), P("dp"), P(("dp", "mp")))
    body = functools.partial(shards, mesh.shape["mp"], mesh.shape["dp"])
    return jax.shard_map(body, mesh=mesh, in_specs=in_specs, out_specs=out_specs, check_vma=False)
```

```python
import functools

import jax
import jax.numpy as jnp
import numpy as np
from jax import lax
from jax.experimental import pallas as pl
from jax.experimental.pallas import tpu as pltpu
from jax.sharding import PartitionSpec as P

HEAD_DIM = 128
SEQ_LEN = 32768
GROUP = 10
MESH = pl.DeviceIdType.MESH
CHUNK = 512
WCHUNK = 256
TILE_N = 256
TURNED = 2


def rope_tables(rows, tok_dev, stride):
    half = HEAD_DIM // 2
    row = np.arange(rows)
    place = (row // tok_dev * stride + row % tok_dev).astype(np.float32)
    inverse = np.exp(
        -np.log(np.float32(1000000.0))
        * (np.float32(2.0) * np.arange(half).astype(np.float32) / np.float32(HEAD_DIM))
    ).astype(np.float32)
    angle = (place[:, None] * inverse[None, :]).astype(np.float32)
    cosine, sine = np.cos(angle).astype(np.float32), np.sin(angle).astype(np.float32)

    def by_column(t):
        t = t.reshape(rows // (2 * tok_dev), 2, tok_dev, HEAD_DIM)
        return np.ascontiguousarray(np.swapaxes(t, 0, 1)).reshape(2, rows // 2, HEAD_DIM)

    return np.stack([by_column(np.concatenate([cosine, cosine], 1)), by_column(np.concatenate([-sine, sine], 1))])


def kernel(
    nz, ndp,
    tok_h, gain_h, w_h, bias_h, grad_h, rope_h,
    qkv, total_ng, tok, gain, factors, gg_ref, bg_ref,
    w, bias, grad, rope,
    low, lowx, nx, held, part, run, rfin, acc, cx, qt, qx, ng, gtot, gx, gy, gstage, gsend, grecv, gdone, gres, bacc,
    in_sem, send_sem, one_sem, low_r, wy_r, wx_r, ag_r, end_r, turn_r, c_r,
):
    f32, bf16 = jnp.float32, jnp.bfloat16
    dp, mp = lax.axis_index("dp"), lax.axis_index("mp")
    z, yl, core = mp // 2, lax.rem(mp, 2), lax.rem(dp, 2)
    nx_chips = ndp // 4
    row_of_x = dp // (2 * nx_chips) * (2 * nx_chips)
    x = lax.rem(dp // 2, nx_chips)
    odd = lax.rem(x, 2)
    rows, depth = tok.shape
    half = depth // 2
    col = nz * rows
    width = grad.shape[1]
    heads = width // HEAD_DIM
    chunks = half // CHUNK
    quarter = half // 4
    slab = half // nz

    def at(start, size, unit):
        return pl.ds(pl.multiple_of(start, unit), size)

    up = {"mp": lax.rem(z + 1, nz) * 2 + yl}
    down = {"mp": lax.rem(z + nz - 1, nz) * 2 + yl}
    pair = {"mp": mp + 1 - 2 * yl}
    far = {"dp": lax.rem(dp + ndp // 2, ndp), "mp": mp + 1 - 2 * yl}
    twin = {"dp": dp + 1 - 2 * core}
    east = {"dp": row_of_x + lax.rem(x + 1, nx_chips) * 2 + core}
    west = {"dp": row_of_x + lax.rem(x + nx_chips - 1, nx_chips) * 2 + core}
    along = (up, down)

    barrier = pltpu.get_barrier_semaphore()
    peers = (up, down, pair, far, twin, east, west)
    for there in peers:
        pl.semaphore_signal(barrier, inc=1, device_id=there, device_id_type=MESH)

    loads = []
    for i, (src, dst) in enumerate((
        (tok_h, tok), (gain_h, gain.at[0]), (grad_h, grad), (rope_h, rope),
        (bias_h, bias.at[0, pl.ds(0, width)]),
        (w_h.at[at(core * half, half, half), :], w.at[:, pl.ds(0, width)]),
    )):
        c = pltpu.make_async_copy(src, dst, in_sem.at[i])
        c.start()
        loads.append(c)

    def remote(src, dst, send, recv, there):
        return pltpu.make_async_remote_copy(
            src_ref=src, dst_ref=dst, send_sem=send_sem.at[send], recv_sem=recv,
            device_id=there, device_id_type=MESH,
        )

    own_cols, pair_cols = pl.ds(0, width), pl.ds(width, width)

    def w_send(a, there):
        i = 2 * a + odd
        return remote(
            w_h.at[at(core * half + i * WCHUNK, WCHUNK, WCHUNK), :],
            w.at[at(i * WCHUNK, WCHUNK, WCHUNK), pair_cols], 0, wy_r.at[a], there,
        )

    def w_pass(a):
        ref = w.at[at((2 * a + odd) * WCHUNK, WCHUNK, WCHUNK), pair_cols]
        return remote(ref, ref, 1, wx_r.at[a], east if a % 2 == 0 else west)

    def w_last():
        i = 2 * chunks - 1 - odd
        return remote(
            w_h.at[at(core * half + i * WCHUNK, WCHUNK, WCHUNK), :],
            w.at[at(i * WCHUNK, WCHUNK, WCHUNK), pair_cols], 0, wx_r.at[chunks - 1], pair,
        )

    def w_come(k):
        ref = w.at[at((2 * k + 1 - odd) * WCHUNK, WCHUNK, WCHUNK), pair_cols]
        return remote(ref, ref, 1, wx_r.at[k], east)

    mine = at(core * col, col, col)
    other = at((1 - core) * col, col, col)
    home = at(core * col + z * rows, rows, rows)
    nx_send = remote(nx, held.at[home, :], 2, one_sem.at[0], twin)

    def ag(way, j, e):
        d = lax.rem(core + e // 4, 2)
        b = lax.rem(z + (nz - j if way == 0 else j), nz)
        ref = held.at[at(d * col + b * rows, rows, rows), at(lax.rem(e, 4) * quarter, quarter, quarter)]
        on = jnp.where(lax.rem(e, 2) == way, 16 + e // 2, 20)
        place = jnp.where(j < 2, j * 8 + e, jnp.where(j == 2, on, 20))
        return remote(ref, ref, 3, ag_r.at[way, place], along[way])

    loads[0].wait()
    loads[1].wait()
    total = jnp.zeros((rows, 1), f32)
    for q in range(8):
        v = tok[:, q * quarter:(q + 1) * quarter].astype(f32)
        total = total + jnp.sum(v * v, axis=1, keepdims=True)
    scale = lax.rsqrt(total / depth + 1e-06)

    def normed(ks):
        return (tok[:, ks].astype(f32) * scale * gain[:, ks]).astype(bf16)

    for q in range(4):
        held[home, q * quarter:(q + 1) * quarter] = normed(at(core * half + q * quarter, quarter, quarter))
    for q in range(4):
        nx[:, q * quarter:(q + 1) * quarter] = normed(at((1 - core) * half + q * quarter, quarter, quarter))
    pl.semaphore_wait(barrier, len(peers))
    for q in range(4):
        for way in range(2):
            ag(way, 0, q).start()
    nx_send.start()
    bias_send = remote(bias_h, bias.at[0, pair_cols], 4, one_sem.at[1], pair)
    bias_send.start()
    for a in (0, 1, 3, 5, 7):
        w_send(a, far).start()

    loads[2].wait()
    loads[3].wait()
    bacc[...] = jnp.zeros_like(bacc)

    @pl.loop(0, nz)
    def _(b):
        for side, y in ((0, yl), (1, 1 - yl)):
            here = at((2 * b + y) * rows, rows, rows)
            there = at(b * rows, rows, rows)
            cs, sn = rope[0, y, there, :], rope[1, y, there, :]
            for h in range(heads):
                hs = slice(h * HEAD_DIM, (h + 1) * HEAD_DIM)
                v = grad[here, hs].astype(f32)
                turned = v * cs - pltpu.roll(v, HEAD_DIM // 2, 1) * sn
                plain = lax.rem(mp * heads + h, GROUP) == GROUP - 1
                v = jnp.where(plain, v, turned)
                bacc[:, hs] += jnp.sum(v.reshape(rows // 8, 8, HEAD_DIM), axis=0)
                if side == 0:
                    low[at(core * col + b * rows, rows, rows), hs] = v.astype(bf16)
                else:
                    lowx[there, hs] = v.astype(bf16)

    low_pair = remote(lowx, low.at[mine, pair_cols], 5, low_r.at[0], pair)
    low_twin = remote(low.at[mine, own_cols], low.at[mine, own_cols], 5, low_r.at[1], twin)
    low_fwd = remote(low.at[mine, pair_cols], low.at[mine, pair_cols], 5, low_r.at[2], twin)
    low_pair.start()
    low_twin.start()
    for a in (2, 4, 6):
        w_send(a, pair).start()
    w_last().start()
    nx_send.wait_recv()
    for q in range(4):
        for way in range(2):
            ag(way, 0, 4 + q).start()
    bg_ref[...] = jnp.sum(bacc[...], axis=0, keepdims=True)

    def cols(k):
        return at(k * CHUNK, CHUNK, CHUNK)

    def backward(k):
        @pl.when(k == chunks - 1)
        def _():
            w_send(chunks - 1, far).wait_recv()

        w_come(k).wait_recv()
        part[:, cols(k)] = lax.dot_general(
            low[...], w[cols(k), :], (((1,), (1,)), ((), ())), preferred_element_type=f32
        )

    def rs(way, j, k):
        place = j * 8 + jnp.where(j < 2, k, k // 2)
        return remote(
            run.at[way, j, :, cols(k)], run.at[way, j + 1, :, cols(k)], 6, ag_r.at[way, place], along[way]
        )

    def rs_end(way, j, k, d):
        return remote(
            run.at[way, j, pl.ds(d * rows, rows), cols(k)],
            rfin.at[way, :, at(core * half + k * CHUNK, CHUNK, CHUNK)],
            6, end_r.at[way, core, jnp.where(j < 3, 0, jnp.where(k < chunks - 2, 1, 2))], dict(along[way], dp=dp - core + d),
        )

    def hops(way, k):
        return jnp.where(lax.rem(k, 2) == way, 4, 3)

    turning = (nz - 1, 1)

    def turned(way, k):
        return remote(
            run.at[way, 0, :, cols(k)], run.at[1 - way, 0, :, cols(k)], 6, turn_r.at[way, k], along[1 - way]
        )

    def rs_term(way, j, k, more):
        left = hops(way, k) - j
        t = lax.rem(z + (left if way == 0 else nz - left), nz)
        for d in range(2):
            ds = pl.ds(d * rows, rows)
            v = part[at(d * col + t * rows, rows, rows), cols(k)]
            if more:
                v = v + run[way, j, ds, cols(k)].astype(f32)
            run[way, j, ds, cols(k)] = v.astype(bf16)

    def rs_turn(k):
        for way in range(2):
            @pl.when(z == turning[way])
            def _():
                rs_term(way, 0, k, False)
                turned(way, k).start()

    def rs_first(way, k):
        joins = (k < TURNED) & (z == (2, nz - 2)[way])

        @pl.when((k >= TURNED) | (z != turning[way]))
        def _():
            @pl.when(joins)
            def _():
                turned(1 - way, jnp.where(k < TURNED, k, 0)).wait_recv()
                rs_term(way, 0, k, True)

            @pl.when(jnp.logical_not(joins))
            def _():
                rs_term(way, 0, k, False)

            rs(way, 0, k).start()

    def rs_step(way, j, k):
        left = hops(way, k) - j
        starts = (j == 1) & (k < TURNED) & (z == 0)

        @pl.when(starts)
        def _():
            rs_term(way, j, k, False)

        @pl.when(jnp.logical_not(starts))
        def _():
            rs(way, j - 1, k).wait_recv()
            rs_term(way, j, k, True)

        @pl.when(left > 1)
        def _():
            rs(way, j, k).start()

        @pl.when(left == 1)
        def _():
            for d in range(2):
                rs_end(way, j, k, d).start()

    own_half = at(core * half, half, half)
    swap = remote(
        part.at[at((1 - core) * col + z * rows, rows, rows), :], ng.at[:, own_half], 7, one_sem.at[2], twin
    )

    def ended(group):
        count = (chunks // 2, chunks // 2 - 1, 1)[group]
        for way in range(2):
            for side in range(2):
                ref = rfin.at[way, :, pl.ds(0, count * CHUNK)]
                remote(ref, ref, 6, end_r.at[way, side, group], up).wait_recv()

    def gain_share(k):
        full = at(core * half + k * CHUNK, CHUNK, CHUNK)
        for ds, to, ks in ((mine, gtot, full), (other, gx, cols(k))):
            share = jnp.sum(part[ds, cols(k)] * held[ds, cols(k)].astype(f32), axis=0, keepdims=True)
            to[:, ks] = share / gain[:, full]

    gx_send = remote(gx, gtot.at[:, own_half], 8, one_sem.at[3], twin)
    gy_send = remote(gtot.at[:, at((1 - yl) * half, half, half)], gy, 13, one_sem.at[7], pair)
    column_half = at(yl * half, half, half)
    g3_send = remote(gres.at[:, column_half], gres.at[:, column_half], 14, one_sem.at[8], pair)

    lines = slab // HEAD_DIM

    def line_of(zz, i):
        return at(yl * half + zz * slab + i * HEAD_DIM, HEAD_DIM, HEAD_DIM)

    def g1(k):
        to = lax.rem(z + k, nz)
        return remote(gsend.at[to], grecv.at[k - 1], 9, one_sem.at[4], {"mp": 2 * to + yl})

    def g2(k):
        to = lax.rem(z + k, nz)
        return remote(gdone.at[z], gdone.at[z], 10, one_sem.at[5], {"mp": 2 * to + yl})

    g1_all = remote(grecv, grecv, 9, one_sem.at[4], up)
    g2_all = remote(grecv, grecv, 10, one_sem.at[5], up)

    def tile(t):
        return at(t * TILE_N, TILE_N, TILE_N)

    def c_send(t):
        return remote(acc.at[other, tile(t)], cx.at[:, tile(t)], 11, c_r.at[t], twin)

    def forward(t):
        acc[:, tile(t)] = jnp.dot(held[...], w[:, tile(t)], preferred_element_type=f32)
        c_send(t).start()

    def q_send(h):
        return remote(
            qt.at[:, at(width + h * HEAD_DIM, HEAD_DIM, HEAD_DIM)], qx.at[:, at(h * HEAD_DIM, HEAD_DIM, HEAD_DIM)],
            12, one_sem.at[6], pair,
        )

    q_all = remote(qx, qx, 12, one_sem.at[6], pair)

    def joined(t):
        c_send(t).wait_recv()
        for i in range(TILE_N // HEAD_DIM):
            h = t * (TILE_N // HEAD_DIM) + i
            hs = at(h * HEAD_DIM, HEAD_DIM, HEAD_DIM)
            v = acc[mine, hs] + cx[:, hs] + bias[:, hs]
            turned = v * rope[0, yl] + pltpu.roll(v, HEAD_DIM // 2, 1) * rope[1, yl]
            whole = jnp.where(h < heads, mp * heads + h, (mp + 1 - 2 * yl) * heads + h - heads)
            qt[:, hs] = jnp.where(lax.rem(whole, GROUP) == GROUP - 1, v, turned).astype(bf16)

            @pl.when(h >= heads)
            def _():
                q_send(h - heads).start()

    passes = (4, 9, 11, 14, 16, 19, 21)
    early = (12, 17, 18, 22, 23)
    ahead = 3

    @pl.loop(0, 24)
    def _(i):
        j, e = 1 + i // 8, lax.rem(i, 8)
        for way in range(2):
            @pl.when((j < 3) | (lax.rem(e, 2) == way))
            def _():
                ag(way, j - 1, e).wait_recv()
                ag(way, j, e).start()

        @pl.when(i >= 24 - ahead)
        def _():
            k = i - (24 - ahead)
            for way in range(2):
                rs_first(way, jnp.where(k < 1, k, k + 1))

        @pl.when(i == 13)
        def _():
            rs_turn(0)

        @pl.when(i == 18)
        def _():
            rs_turn(1)

        for a, step in enumerate(passes):
            @pl.when(i == step)
            def _():
                w_send(a, pair).wait_recv()
                w_pass(a).start()

        @pl.when(i == 6)
        def _():
            low_pair.wait_recv()
            low_fwd.start()

        @pl.when(i == 9)
        def _():
            loads[5].wait()
            low_twin.wait_recv()
            low_fwd.wait_recv()

        k, due = 0, i == early[0]
        for m in range(1, len(early)):
            k, due = jnp.where(i >= early[m], m, k), due | (i == early[m])

        @pl.when(due)
        def _():
            backward(k)

    @pl.loop(ahead, chunks)
    def _(m):
        k = jnp.where(m == ahead, 1, jnp.where(m < chunks - 2, m, 2 * chunks - 3 - m))

        @pl.when(m >= len(early))
        def _():
            backward(k)

        for way in range(2):
            rs_first(way, k)

    swap.start()
    for q in range(4):
        ks = pl.ds(q * quarter, quarter)
        ng[:, at(core * half + q * quarter, quarter, quarter)] = part[home, ks]
    for way in range(2):
        ref = held.at[pl.ds(0, 2 * rows), :]
        remote(ref, ref, 3, ag_r.at[way, 20], up).wait_recv()
    loads[4].wait()
    bias_send.wait_recv()

    @pl.loop(0, chunks)
    def _(k):
        gain_share(k)

    gx_send.start()

    @pl.loop(0, 20)
    def _(m):
        j, q = 1 + m // 8, lax.rem(m, 8)
        for way in range(2):
            rs_step(way, j, jnp.where(j < 3, q, 2 * q + way))

        @pl.when((m >= 2) & (m < 7))
        def _():
            joined(lax.rem(m, 5))

        @pl.when(m < 5)
        def _():
            forward(lax.rem(m + 2, 5))

        @pl.when(m == 1)
        def _():
            gx_send.wait_recv()
            gy_send.start()

        @pl.when(m == 4)
        def _():
            gy_send.wait_recv()
            gtot[:, column_half] += gy[...]
            for zz in range(nz):
                for i in range(lines):
                    gstage[zz, i:i + 1, :] = gtot[:, line_of(zz, i)]
            gsend[...] = gstage[...].astype(bf16)
            for k in range(1, nz):
                g1(k).start()

        @pl.when(m == 13)
        def _():
            g1_all.wait_recv()
            share = gstage[z]
            for k in range(1, nz):
                share = share + grecv[k - 1].astype(f32)
            gdone[z] = share.astype(bf16)
            for k in range(1, nz):
                g2(k).start()

        @pl.when(m == 16)
        def _():
            q_all.wait_recv()
            for b in range(nz):
                there = pl.ds(b * rows, rows)
                qkv[at((2 * b + yl) * rows, rows, rows), :] = qt[there, own_cols]
                qkv[at((2 * b + 1 - yl) * rows, rows, rows), :] = qx[there, :]

    g2_all.wait_recv()
    gstage[...] = gdone[...].astype(f32)
    for zz in range(nz):
        for i in range(lines):
            gres[:, line_of(zz, i)] = gstage[zz, i:i + 1, :]
    g3_send.start()
    swap.wait_recv()
    ended(0)
    for q in range(2 * chunks):
        ks = slice(q * CHUNK, (q + 1) * CHUNK)
        ng[:, ks] += rfin[1 - q % 2, :, ks].astype(f32)
    inner = jnp.zeros((rows, 1), f32)
    for group, ks_in in ((1, range(chunks - 2)), (2, range(chunks - 2, chunks))):
        ended(group)
        for side in range(2):
            for k in ks_in:
                q = side * chunks + k
                ks = slice(q * CHUNK, (q + 1) * CHUNK)
                v = ng[:, ks] + rfin[k % 2, :, ks].astype(f32)
                total_ng[:, ks] = v
                inner = inner + jnp.sum(v * tok[:, ks].astype(f32) * gain[:, ks], axis=1, keepdims=True)
    factors[0] = jnp.broadcast_to(scale, factors.shape[1:])
    factors[1] = jnp.broadcast_to(scale * scale * scale * (inner / depth), factors.shape[1:])

    g3_send.wait_recv()
    gg_ref[...] = gres[...]

    def sent(ref, send):
        remote(ref, ref, send, one_sem.at[0], twin).wait_send()

    sent(w_h.at[pl.ds(0, (chunks + 1) * WCHUNK), :], 0)
    sent(w_h.at[pl.ds(0, (chunks - 1) * WCHUNK), :], 1)
    sent(nx, 2)
    moved = held.at[pl.ds(0, 7 * 2 * rows), :]
    sent(moved, 3)
    bias_send.wait_send()
    sent(w_h.at[pl.ds(0, 3 * col), :], 5)
    sent(moved, 6)
    swap.wait_send()
    sent(gx, 8)
    sent(grecv, 9)
    sent(grecv, 10)
    sent(cx, 11)
    sent(qx, 12)
    gy_send.wait_send()
    g3_send.wait_send()


def finish(qkv, ng, tok, gain, factors, gg, bg, qkv_h, tg_h, gg_h, bg_h, tg, sem):
    parts = sem.shape[0] - 3
    piece = tok.shape[1] // parts
    copies = [
        pltpu.make_async_copy(src, dst, sem.at[i])
        for i, (src, dst) in enumerate(((qkv, qkv_h), (gg.at[0], gg_h), (bg.at[0], bg_h)))
    ]
    for c in copies:
        c.start()
    scale, weight = factors[0, :, :1], factors[1, :, :1]
    for q in range(parts):
        ks = slice(q * piece, (q + 1) * piece)
        tg[:, ks] = scale * gain[:, ks] * ng[:, ks] - tok[:, ks].astype(jnp.float32) * weight
        c = pltpu.make_async_copy(tg.at[:, ks], tg_h.at[:, ks], sem.at[3 + q])
        c.start()
        copies.append(c)
    for c in copies:
        c.wait()


def shards(n, ndp, tokens, norm_gain, qkv_weight, qkv_bias, qkv_grad):
    rows, depth = tokens.shape
    every, width = qkv_grad.shape
    rope = rope_tables(every, rows, SEQ_LEN // n)
    bf16, f32 = jnp.bfloat16, jnp.float32
    half, col, nz = depth // 2, every // 2, n // 2
    slab = half // nz
    chunks = half // CHUNK
    tiles = 2 * width // TILE_N
    dma = pltpu.SemaphoreType.DMA
    vm = pltpu.VMEM
    hbm = pl.BlockSpec(memory_space=pl.ANY)
    vmem = pl.BlockSpec(memory_space=pltpu.VMEM)
    results = pl.pallas_call(
        functools.partial(kernel, nz, ndp),
        out_shape=(
            vm((every, width), bf16),
            vm((rows, depth), f32),
            vm((rows, depth), bf16),
            vm((1, depth), f32),
            vm((2, rows, HEAD_DIM), f32),
            vm((1, depth), f32),
            vm((1, width), f32),
        ),
        in_specs=[hbm] * 6,
        out_specs=[vmem] * 7,
        scratch_shapes=[
            vm((half, 2 * width), bf16),
            vm((1, 2 * width), f32),
            vm((every, width), bf16),
            vm((2, 2, col, HEAD_DIM), f32),
            vm((every, 2 * width), bf16),
            vm((col, width), bf16),
            vm((rows, half), bf16),
            vm((every, half), bf16),
            vm((every, half), f32),
            vm((2, 4, 2 * rows, half), bf16),
            vm((2, rows, depth), bf16),
            vm((every, 2 * width), f32),
            vm((col, 2 * width), f32),
            vm((col, 2 * width), bf16),
            vm((col, width), bf16),
            vm((rows, depth), f32),
            vm((1, depth), f32),
            vm((1, half), f32),
            vm((1, half), f32),
            vm((nz, slab // HEAD_DIM, HEAD_DIM), f32),
            vm((nz, slab // HEAD_DIM, HEAD_DIM), bf16),
            vm((nz - 1, slab // HEAD_DIM, HEAD_DIM), bf16),
            vm((nz, slab // HEAD_DIM, HEAD_DIM), bf16),
            vm((1, depth), f32),
            vm((8, width), f32),
            dma((6,)),
            dma((15,)),
            dma((9,)),
            dma((3,)),
            dma((chunks,)),
            dma((chunks,)),
            dma((2, 21)),
            dma((2, 2, 3)),
            dma((2, TURNED)),
            dma((tiles,)),
        ],
        compiler_params=pltpu.CompilerParams(
            collective_id=0, has_side_effects=True, vmem_limit_bytes=60000000
        ),
        cost_estimate=pl.CostEstimate(
            flops=4 * every * depth * width, bytes_accessed=2 * depth * width, transcendentals=0
        ),
    )(
        tokens, norm_gain, qkv_weight, qkv_bias, qkv_grad,
        jnp.asarray(rope),
    )
    return pl.pallas_call(
        finish,
        out_shape=(
            jax.ShapeDtypeStruct((every, width), bf16),
            jax.ShapeDtypeStruct((rows, depth), f32),
            jax.ShapeDtypeStruct((depth,), f32),
            jax.ShapeDtypeStruct((width,), f32),
        ),
        in_specs=[vmem] * 7,
        out_specs=[hbm] * 4,
        scratch_shapes=[vm((rows, depth), f32), dma((7,))],
        compiler_params=pltpu.CompilerParams(vmem_limit_bytes=1 << 21),
    )(*results)


def solution(mesh):
    in_specs = (P(("dp", "mp"), None), P(), P(None, "mp"), P("mp"), P("dp", "mp"))
    out_specs = (P("dp", "mp"), P(("dp", "mp"), None), P("dp"), P(("dp", "mp")))
    body = functools.partial(shards, mesh.shape["mp"], mesh.shape["dp"])
    return jax.shard_map(body, mesh=mesh, in_specs=in_specs, out_specs=out_specs, check_vma=False)
```

```python
import functools

import jax
import jax.numpy as jnp
import numpy as np
from jax import lax
from jax.experimental import pallas as pl
from jax.experimental.pallas import tpu as pltpu
from jax.sharding import PartitionSpec as P

HEAD_DIM = 128
SEQ_LEN = 32768
GROUP = 10
MESH = pl.DeviceIdType.MESH
CHUNK = 512
WCHUNK = 256
TILE_N = 256
TURNED = 2


def rope_tables(rows, tok_dev, stride):
    half = HEAD_DIM // 2
    row = np.arange(rows)
    place = (row // tok_dev * stride + row % tok_dev).astype(np.float32)
    inverse = np.exp(
        -np.log(np.float32(1000000.0))
        * (np.float32(2.0) * np.arange(half).astype(np.float32) / np.float32(HEAD_DIM))
    ).astype(np.float32)
    angle = (place[:, None] * inverse[None, :]).astype(np.float32)
    cosine, sine = np.cos(angle).astype(np.float32), np.sin(angle).astype(np.float32)

    def by_column(t):
        t = t.reshape(rows // (2 * tok_dev), 2, tok_dev, HEAD_DIM)
        return np.ascontiguousarray(np.swapaxes(t, 0, 1)).reshape(2, rows // 2, HEAD_DIM)

    return np.stack([by_column(np.concatenate([cosine, cosine], 1)), by_column(np.concatenate([-sine, sine], 1))])


def kernel(
    nz, ndp,
    tok_h, gain_h, w_h, bias_h, grad_h, rope_h,
    qkv, total_ng, tok, gain, factors, gg_ref, bg_ref,
    w, bias, grad, rope,
    low, lowx, nx, held, part, run, rfin, acc, cx, qt, qx, ng, gtot, gx, gy, gstage, gsend, grecv, gdone, gres, bacc,
    in_sem, send_sem, one_sem, low_r, wy_r, wx_r, ag_r, end_r, turn_r, c_r,
):
    f32, bf16 = jnp.float32, jnp.bfloat16
    dp, mp = lax.axis_index("dp"), lax.axis_index("mp")
    z, yl, core = mp // 2, lax.rem(mp, 2), lax.rem(dp, 2)
    nx_chips = ndp // 4
    row_of_x = dp // (2 * nx_chips) * (2 * nx_chips)
    x = lax.rem(dp // 2, nx_chips)
    odd = lax.rem(x, 2)
    rows, depth = tok.shape
    half = depth // 2
    col = nz * rows
    width = grad.shape[1]
    heads = width // HEAD_DIM
    chunks = half // CHUNK
    quarter = half // 4
    slab = half // nz

    def at(start, size, unit):
        return pl.ds(pl.multiple_of(start, unit), size)

    up = {"mp": lax.rem(z + 1, nz) * 2 + yl}
    down = {"mp": lax.rem(z + nz - 1, nz) * 2 + yl}
    pair = {"mp": mp + 1 - 2 * yl}
    far = {"dp": lax.rem(dp + ndp // 2, ndp), "mp": mp + 1 - 2 * yl}
    twin = {"dp": dp + 1 - 2 * core}
    east = {"dp": row_of_x + lax.rem(x + 1, nx_chips) * 2 + core}
    west = {"dp": row_of_x + lax.rem(x + nx_chips - 1, nx_chips) * 2 + core}
    along = (up, down)

    loads = [
        pltpu.make_async_copy(src, dst, in_sem.at[i])
        for i, (src, dst) in enumerate((
            (tok_h, tok), (gain_h, gain.at[0]), (grad_h, grad), (rope_h, rope),
            (bias_h, bias.at[0, pl.ds(0, width)]),
            (w_h.at[at(core * half, half, half), :], w.at[:, pl.ds(0, width)]),
        ))
    ]
    loads[0].start()
    loads[1].start()

    barrier = pltpu.get_barrier_semaphore()
    peers = (up, down, pair, far, twin, east, west)
    for there in peers:
        pl.semaphore_signal(barrier, inc=1, device_id=there, device_id_type=MESH)

    def remote(src, dst, send, recv, there):
        return pltpu.make_async_remote_copy(
            src_ref=src, dst_ref=dst, send_sem=send_sem.at[send], recv_sem=recv,
            device_id=there, device_id_type=MESH,
        )

    own_cols, pair_cols = pl.ds(0, width), pl.ds(width, width)

    def w_send(a, there):
        i = 2 * a + odd
        return remote(
            w_h.at[at(core * half + i * WCHUNK, WCHUNK, WCHUNK), :],
            w.at[at(i * WCHUNK, WCHUNK, WCHUNK), pair_cols], 0, wy_r.at[a], there,
        )

    def w_pass(a):
        ref = w.at[at((2 * a + odd) * WCHUNK, WCHUNK, WCHUNK), pair_cols]
        return remote(ref, ref, 0, wx_r.at[a], east if a % 2 == 0 else west)

    def w_last():
        i = 2 * chunks - 1 - odd
        return remote(
            w_h.at[at(core * half + i * WCHUNK, WCHUNK, WCHUNK), :],
            w.at[at(i * WCHUNK, WCHUNK, WCHUNK), pair_cols], 0, wx_r.at[chunks - 1], pair,
        )

    def w_come(k):
        ref = w.at[at((2 * k + 1 - odd) * WCHUNK, WCHUNK, WCHUNK), pair_cols]
        return remote(ref, ref, 0, wx_r.at[k], east)

    mine = at(core * col, col, col)
    other = at((1 - core) * col, col, col)
    home = at(core * col + z * rows, rows, rows)
    nx_send = remote(nx, held.at[home, :], 1, one_sem.at[0], twin)

    def ag(way, j, e):
        d = lax.rem(core + e // 4, 2)
        b = lax.rem(z + (nz - j if way == 0 else j), nz)
        ref = held.at[at(d * col + b * rows, rows, rows), at(lax.rem(e, 4) * quarter, quarter, quarter)]
        on = jnp.where(lax.rem(e, 2) == way, 16 + e // 2, 20)
        place = jnp.where(j < 2, j * 8 + e, jnp.where(j == 2, on, 20))
        return remote(ref, ref, 1, ag_r.at[way, place], along[way])

    loads[0].wait()
    loads[1].wait()
    for l in loads[2:]:
        l.start()
    total = jnp.zeros((rows, 1), f32)
    for q in range(8):
        v = tok[:, q * quarter:(q + 1) * quarter].astype(f32)
        total = total + jnp.sum(v * v, axis=1, keepdims=True)
    scale = lax.rsqrt(total / depth + 1e-06)

    def normed(ks):
        return (tok[:, ks].astype(f32) * scale * gain[:, ks]).astype(bf16)

    for q in range(4):
        held[home, q * quarter:(q + 1) * quarter] = normed(at(core * half + q * quarter, quarter, quarter))
    pl.semaphore_wait(barrier, len(peers))
    for q in range(4):
        for way in range(2):
            ag(way, 0, q).start()
    for q in range(4):
        nx[:, q * quarter:(q + 1) * quarter] = normed(at((1 - core) * half + q * quarter, quarter, quarter))
    nx_send.start()
    bias_send = remote(bias_h, bias.at[0, pair_cols], 4, one_sem.at[1], pair)
    bias_send.start()
    for a in (0, 1, 3, 5, 7):
        w_send(a, far).start()

    loads[2].wait()
    loads[3].wait()
    bacc[...] = jnp.zeros_like(bacc)

    @pl.loop(0, nz)
    def _(b):
        for side, y in ((0, yl), (1, 1 - yl)):
            here = at((2 * b + y) * rows, rows, rows)
            there = at(b * rows, rows, rows)
            cs, sn = rope[0, y, there, :], rope[1, y, there, :]
            for h in range(heads):
                hs = slice(h * HEAD_DIM, (h + 1) * HEAD_DIM)
                v = grad[here, hs].astype(f32)
                turned = v * cs - pltpu.roll(v, HEAD_DIM // 2, 1) * sn
                plain = lax.rem(mp * heads + h, GROUP) == GROUP - 1
                v = jnp.where(plain, v, turned)
                bacc[:, hs] += jnp.sum(v.reshape(rows // 8, 8, HEAD_DIM), axis=0)
                if side == 0:
                    low[at(core * col + b * rows, rows, rows), hs] = v.astype(bf16)
                else:
                    lowx[there, hs] = v.astype(bf16)

    low_pair = remote(lowx, low.at[mine, pair_cols], 0, low_r.at[0], pair)
    low_twin = remote(low.at[mine, own_cols], low.at[mine, own_cols], 0, low_r.at[1], twin)
    low_fwd = remote(low.at[mine, pair_cols], low.at[mine, pair_cols], 0, low_r.at[2], twin)
    low_pair.start()
    low_twin.start()
    for a in (2, 4, 6):
        w_send(a, pair).start()
    w_last().start()
    nx_send.wait_recv()
    for q in range(4):
        for way in range(2):
            ag(way, 0, 4 + q).start()
    bg_ref[...] = jnp.sum(bacc[...], axis=0, keepdims=True)

    def cols(k):
        return at(k * CHUNK, CHUNK, CHUNK)

    def backward(k):
        @pl.when(k == chunks - 1)
        def _():
            w_send(chunks - 1, far).wait_recv()

        w_come(k).wait_recv()
        part[:, cols(k)] = lax.dot_general(
            low[...], w[cols(k), :], (((1,), (1,)), ((), ())), preferred_element_type=f32
        )

    def rs(way, j, k):
        place = j * 8 + jnp.where(j < 2, k, k // 2)
        return remote(
            run.at[way, j, :, cols(k)], run.at[way, j + 1, :, cols(k)], 1, ag_r.at[way, place], along[way]
        )

    def rs_end(way, j, k, d):
        return remote(
            run.at[way, j, pl.ds(d * rows, rows), cols(k)],
            rfin.at[way, :, at(core * half + k * CHUNK, CHUNK, CHUNK)],
            1, end_r.at[way, core, jnp.where(j < 3, 0, jnp.where(k < chunks - 2, 1, 2))], dict(along[way], dp=dp - core + d),
        )

    def hops(way, k):
        return jnp.where(lax.rem(k, 2) == way, 4, 3)

    turning = (nz - 1, 1)

    def turned(way, k):
        return remote(
            run.at[way, 0, :, cols(k)], run.at[1 - way, 0, :, cols(k)], 1, turn_r.at[way, k], along[1 - way]
        )

    def rs_term(way, j, k, more):
        left = hops(way, k) - j
        t = lax.rem(z + (left if way == 0 else nz - left), nz)
        for d in range(2):
            ds = pl.ds(d * rows, rows)
            v = part[at(d * col + t * rows, rows, rows), cols(k)]
            if more:
                v = v + run[way, j, ds, cols(k)].astype(f32)
            run[way, j, ds, cols(k)] = v.astype(bf16)

    def rs_turn(k):
        for way in range(2):
            @pl.when(z == turning[way])
            def _():
                rs_term(way, 0, k, False)
                turned(way, k).start()

    def rs_first(way, k):
        joins = (k < TURNED) & (z == (2, nz - 2)[way])

        @pl.when((k >= TURNED) | (z != turning[way]))
        def _():
            @pl.when(joins)
            def _():
                turned(1 - way, jnp.where(k < TURNED, k, 0)).wait_recv()
                rs_term(way, 0, k, True)

            @pl.when(jnp.logical_not(joins))
            def _():
                rs_term(way, 0, k, False)

            rs(way, 0, k).start()

    def rs_step(way, j, k):
        left = hops(way, k) - j
        starts = (j == 1) & (k < TURNED) & (z == 0)

        @pl.when(starts)
        def _():
            rs_term(way, j, k, False)

        @pl.when(jnp.logical_not(starts))
        def _():
            rs(way, j - 1, k).wait_recv()
            rs_term(way, j, k, True)

        @pl.when(left > 1)
        def _():
            rs(way, j, k).start()

        @pl.when(left == 1)
        def _():
            for d in range(2):
                rs_end(way, j, k, d).start()

    own_half = at(core * half, half, half)
    swap = remote(
        part.at[at((1 - core) * col + z * rows, rows, rows), :], ng.at[:, own_half], 1, one_sem.at[2], twin
    )

    def ended(group):
        count = (chunks // 2, chunks // 2 - 1, 1)[group]
        for way in range(2):
            for side in range(2):
                ref = rfin.at[way, :, pl.ds(0, count * CHUNK)]
                remote(ref, ref, 1, end_r.at[way, side, group], up).wait_recv()

    def gain_share(k):
        full = at(core * half + k * CHUNK, CHUNK, CHUNK)
        for ds, to, ks in ((mine, gtot, full), (other, gx, cols(k))):
            share = jnp.sum(part[ds, cols(k)] * held[ds, cols(k)].astype(f32), axis=0, keepdims=True)
            to[:, ks] = share / gain[:, full]

    gx_send = remote(gx, gtot.at[:, own_half], 3, one_sem.at[3], twin)
    gy_send = remote(gtot.at[:, at((1 - yl) * half, half, half)], gy, 3, one_sem.at[7], pair)
    column_half = at(yl * half, half, half)
    g3_send = remote(gres.at[:, column_half], gres.at[:, column_half], 7, one_sem.at[8], pair)

    lines = slab // HEAD_DIM

    def line_of(zz, i):
        return at(yl * half + zz * slab + i * HEAD_DIM, HEAD_DIM, HEAD_DIM)

    def g1(k):
        to = lax.rem(z + k, nz)
        return remote(gsend.at[to], grecv.at[k - 1], 5, one_sem.at[4], {"mp": 2 * to + yl})

    def g2(k):
        to = lax.rem(z + k, nz)
        return remote(gdone.at[z], gdone.at[z], 6, one_sem.at[5], {"mp": 2 * to + yl})

    g1_all = remote(grecv, grecv, 5, one_sem.at[4], up)
    g2_all = remote(grecv, grecv, 6, one_sem.at[5], up)

    def tile(t):
        return at(t * TILE_N, TILE_N, TILE_N)

    def c_send(t):
        return remote(acc.at[other, tile(t)], cx.at[:, tile(t)], 2, c_r.at[t], twin)

    def forward(t):
        acc[:, tile(t)] = jnp.dot(held[...], w[:, tile(t)], preferred_element_type=f32)
        c_send(t).start()

    def q_send(h):
        return remote(
            qt.at[:, at(width + h * HEAD_DIM, HEAD_DIM, HEAD_DIM)], qx.at[:, at(h * HEAD_DIM, HEAD_DIM, HEAD_DIM)],
            2, one_sem.at[6], pair,
        )

    q_all = remote(qx, qx, 2, one_sem.at[6], pair)

    def joined(t):
        c_send(t).wait_recv()
        for i in range(TILE_N // HEAD_DIM):
            h = t * (TILE_N // HEAD_DIM) + i
            hs = at(h * HEAD_DIM, HEAD_DIM, HEAD_DIM)
            v = acc[mine, hs] + cx[:, hs] + bias[:, hs]
            turned = v * rope[0, yl] + pltpu.roll(v, HEAD_DIM // 2, 1) * rope[1, yl]
            whole = jnp.where(h < heads, mp * heads + h, (mp + 1 - 2 * yl) * heads + h - heads)
            qt[:, hs] = jnp.where(lax.rem(whole, GROUP) == GROUP - 1, v, turned).astype(bf16)

            @pl.when(h >= heads)
            def _():
                q_send(h - heads).start()

    passes = (4, 9, 11, 14, 16, 19, 21)
    early = (12, 17, 18, 22, 23)
    ahead = 3

    @pl.loop(0, 24)
    def _(i):
        j, e = 1 + i // 8, lax.rem(i, 8)
        for way in range(2):
            @pl.when((j < 3) | (lax.rem(e, 2) == way))
            def _():
                ag(way, j - 1, e).wait_recv()
                ag(way, j, e).start()

        @pl.when(i >= 24 - ahead)
        def _():
            k = i - (24 - ahead)
            for way in range(2):
                rs_first(way, jnp.where(k < 1, k, k + 1))

        @pl.when(i == 13)
        def _():
            rs_turn(0)

        @pl.when(i == 18)
        def _():
            rs_turn(1)

        for a, step in enumerate(passes):
            @pl.when(i == step)
            def _():
                w_send(a, pair).wait_recv()
                w_pass(a).start()

        @pl.when(i == 6)
        def _():
            low_pair.wait_recv()
            low_fwd.start()

        @pl.when(i == 9)
        def _():
            loads[5].wait()
            low_twin.wait_recv()
            low_fwd.wait_recv()

        k, due = 0, i == early[0]
        for m in range(1, len(early)):
            k, due = jnp.where(i >= early[m], m, k), due | (i == early[m])

        @pl.when(due)
        def _():
            backward(k)

    @pl.loop(ahead, chunks)
    def _(m):
        k = jnp.where(m == ahead, 1, jnp.where(m < chunks - 2, m, 2 * chunks - 3 - m))

        @pl.when(m >= len(early))
        def _():
            backward(k)

        for way in range(2):
            rs_first(way, k)

    swap.start()
    for q in range(4):
        ks = pl.ds(q * quarter, quarter)
        ng[:, at(core * half + q * quarter, quarter, quarter)] = part[home, ks]
    for way in range(2):
        ref = held.at[pl.ds(0, 2 * rows), :]
        remote(ref, ref, 1, ag_r.at[way, 20], up).wait_recv()
    loads[4].wait()
    bias_send.wait_recv()

    @pl.loop(0, chunks)
    def _(k):
        gain_share(k)

    gx_send.start()

    @pl.loop(0, 20)
    def _(m):
        j, q = 1 + m // 8, lax.rem(m, 8)
        for way in range(2):
            rs_step(way, j, jnp.where(j < 3, q, 2 * q + way))

        @pl.when((m >= 2) & (m < 7))
        def _():
            joined(lax.rem(m, 5))

        @pl.when(m < 5)
        def _():
            forward(lax.rem(m + 2, 5))

        @pl.when(m == 1)
        def _():
            gx_send.wait_recv()
            gy_send.start()

        @pl.when(m == 4)
        def _():
            gy_send.wait_recv()
            gtot[:, column_half] += gy[...]
            for zz in range(nz):
                for i in range(lines):
                    gstage[zz, i:i + 1, :] = gtot[:, line_of(zz, i)]
            gsend[...] = gstage[...].astype(bf16)
            for k in range(1, nz):
                g1(k).start()

        @pl.when(m == 13)
        def _():
            g1_all.wait_recv()
            share = gstage[z]
            for k in range(1, nz):
                share = share + grecv[k - 1].astype(f32)
            gdone[z] = share.astype(bf16)
            for k in range(1, nz):
                g2(k).start()

        @pl.when(m == 16)
        def _():
            q_all.wait_recv()
            for b in range(nz):
                there = pl.ds(b * rows, rows)
                qkv[at((2 * b + yl) * rows, rows, rows), :] = qt[there, own_cols]
                qkv[at((2 * b + 1 - yl) * rows, rows, rows), :] = qx[there, :]

    g2_all.wait_recv()
    gstage[...] = gdone[...].astype(f32)
    for zz in range(nz):
        for i in range(lines):
            gres[:, line_of(zz, i)] = gstage[zz, i:i + 1, :]
    g3_send.start()
    swap.wait_recv()
    ended(0)
    for q in range(2 * chunks):
        ks = slice(q * CHUNK, (q + 1) * CHUNK)
        ng[:, ks] += rfin[1 - q % 2, :, ks].astype(f32)
    inner = jnp.zeros((rows, 1), f32)
    for group, ks_in in ((1, range(chunks - 2)), (2, range(chunks - 2, chunks))):
        ended(group)
        for side in range(2):
            for k in ks_in:
                q = side * chunks + k
                ks = slice(q * CHUNK, (q + 1) * CHUNK)
                v = ng[:, ks] + rfin[k % 2, :, ks].astype(f32)
                total_ng[:, ks] = v
                inner = inner + jnp.sum(v * tok[:, ks].astype(f32) * gain[:, ks], axis=1, keepdims=True)
    factors[0] = jnp.broadcast_to(scale, factors.shape[1:])
    factors[1] = jnp.broadcast_to(scale * scale * scale * (inner / depth), factors.shape[1:])

    g3_send.wait_recv()
    gg_ref[...] = gres[...]

    def sent(ref, send):
        remote(ref, ref, send, one_sem.at[0], twin).wait_send()

    sent(w_h.at[pl.ds(0, 2 * chunks * WCHUNK + 3 * col), :], 0)
    sent(part.at[pl.ds(0, (2 * 7 + 1) * rows + rows // 2), :], 1)
    sent(acc.at[pl.ds(0, col + col // 4), :], 2)
    sent(gtot, 3)
    bias_send.wait_send()
    sent(grecv, 5)
    sent(grecv, 6)
    g3_send.wait_send()


def finish(qkv, ng, tok, gain, factors, gg, bg, qkv_h, tg_h, gg_h, bg_h, tg, sem):
    parts = sem.shape[0] - 3
    piece = tok.shape[1] // parts
    copies = [
        pltpu.make_async_copy(src, dst, sem.at[i])
        for i, (src, dst) in enumerate(((qkv, qkv_h), (gg.at[0], gg_h), (bg.at[0], bg_h)))
    ]
    for c in copies:
        c.start()
    scale, weight = factors[0, :, :1], factors[1, :, :1]
    for q in range(parts):
        ks = slice(q * piece, (q + 1) * piece)
        tg[:, ks] = scale * gain[:, ks] * ng[:, ks] - tok[:, ks].astype(jnp.float32) * weight
        c = pltpu.make_async_copy(tg.at[:, ks], tg_h.at[:, ks], sem.at[3 + q])
        c.start()
        copies.append(c)
    for c in copies:
        c.wait()


def shards(n, ndp, tokens, norm_gain, qkv_weight, qkv_bias, qkv_grad):
    rows, depth = tokens.shape
    every, width = qkv_grad.shape
    rope = rope_tables(every, rows, SEQ_LEN // n)
    bf16, f32 = jnp.bfloat16, jnp.float32
    half, col, nz = depth // 2, every // 2, n // 2
    slab = half // nz
    chunks = half // CHUNK
    tiles = 2 * width // TILE_N
    dma = pltpu.SemaphoreType.DMA
    vm = pltpu.VMEM
    hbm = pl.BlockSpec(memory_space=pl.ANY)
    vmem = pl.BlockSpec(memory_space=pltpu.VMEM)
    results = pl.pallas_call(
        functools.partial(kernel, nz, ndp),
        out_shape=(
            vm((every, width), bf16),
            vm((rows, depth), f32),
            vm((rows, depth), bf16),
            vm((1, depth), f32),
            vm((2, rows, HEAD_DIM), f32),
            vm((1, depth), f32),
            vm((1, width), f32),
        ),
        in_specs=[hbm] * 6,
        out_specs=[vmem] * 7,
        scratch_shapes=[
            vm((half, 2 * width), bf16),
            vm((1, 2 * width), f32),
            vm((every, width), bf16),
            vm((2, 2, col, HEAD_DIM), f32),
            vm((every, 2 * width), bf16),
            vm((col, width), bf16),
            vm((rows, half), bf16),
            vm((every, half), bf16),
            vm((every, half), f32),
            vm((2, 4, 2 * rows, half), bf16),
            vm((2, rows, depth), bf16),
            vm((every, 2 * width), f32),
            vm((col, 2 * width), f32),
            vm((col, 2 * width), bf16),
            vm((col, width), bf16),
            vm((rows, depth), f32),
            vm((1, depth), f32),
            vm((1, half), f32),
            vm((1, half), f32),
            vm((nz, slab // HEAD_DIM, HEAD_DIM), f32),
            vm((nz, slab // HEAD_DIM, HEAD_DIM), bf16),
            vm((nz - 1, slab // HEAD_DIM, HEAD_DIM), bf16),
            vm((nz, slab // HEAD_DIM, HEAD_DIM), bf16),
            vm((1, depth), f32),
            vm((8, width), f32),
            dma((6,)),
            dma((8,)),
            dma((9,)),
            dma((3,)),
            dma((chunks,)),
            dma((chunks,)),
            dma((2, 21)),
            dma((2, 2, 3)),
            dma((2, TURNED)),
            dma((tiles,)),
        ],
        compiler_params=pltpu.CompilerParams(
            collective_id=0, has_side_effects=True, vmem_limit_bytes=60000000
        ),
        cost_estimate=pl.CostEstimate(
            flops=4 * every * depth * width, bytes_accessed=2 * depth * width, transcendentals=0
        ),
    )(
        tokens, norm_gain, qkv_weight, qkv_bias, qkv_grad,
        jnp.asarray(rope),
    )
    return pl.pallas_call(
        finish,
        out_shape=(
            jax.ShapeDtypeStruct((every, width), bf16),
            jax.ShapeDtypeStruct((rows, depth), f32),
            jax.ShapeDtypeStruct((depth,), f32),
            jax.ShapeDtypeStruct((width,), f32),
        ),
        in_specs=[vmem] * 7,
        out_specs=[hbm] * 4,
        scratch_shapes=[vm((rows, depth), f32), dma((7,))],
        compiler_params=pltpu.CompilerParams(vmem_limit_bytes=1 << 21),
    )(*results)


def solution(mesh):
    in_specs = (P(("dp", "mp"), None), P(), P(None, "mp"), P("mp"), P("dp", "mp"))
    out_specs = (P("dp", "mp"), P(("dp", "mp"), None), P("dp"), P(("dp", "mp")))
    body = functools.partial(shards, mesh.shape["mp"], mesh.shape["dp"])
    return jax.shard_map(body, mesh=mesh, in_specs=in_specs, out_specs=out_specs, check_vma=False)
```

```python
import functools

import jax
import jax.numpy as jnp
import numpy as np
from jax import lax
from jax.experimental import pallas as pl
from jax.experimental.pallas import tpu as pltpu
from jax.sharding import PartitionSpec as P

HEAD_DIM = 128
SEQ_LEN = 32768
GROUP = 10
MESH = pl.DeviceIdType.MESH
CHUNK = 512
WCHUNK = 256
TILE_N = 256
TURNED = 2


def rope_tables(rows, tok_dev, stride):
    half = HEAD_DIM // 2
    row = np.arange(rows)
    place = (row // tok_dev * stride + row % tok_dev).astype(np.float32)
    inverse = np.exp(
        -np.log(np.float32(1000000.0))
        * (np.float32(2.0) * np.arange(half).astype(np.float32) / np.float32(HEAD_DIM))
    ).astype(np.float32)
    angle = (place[:, None] * inverse[None, :]).astype(np.float32)
    cosine, sine = np.cos(angle).astype(np.float32), np.sin(angle).astype(np.float32)

    def by_column(t):
        t = t.reshape(rows // (2 * tok_dev), 2, tok_dev, HEAD_DIM)
        return np.ascontiguousarray(np.swapaxes(t, 0, 1)).reshape(2, rows // 2, HEAD_DIM)

    return np.stack([by_column(np.concatenate([cosine, cosine], 1)), by_column(np.concatenate([-sine, sine], 1))])


def kernel(
    nz, ndp,
    tok_h, gain_h, w_h, bias_h, grad_h, rope_h,
    qkv, total_ng, tok, gain, factors, gg_ref, bg_ref,
    w, bias, grad, rope,
    low, lowx, nx, held, part, run, rfin, acc, cx, qt, qx, ng, gtot, gx, gy, gstage, gsend, grecv, gdone, gres, bacc,
    in_sem, send_sem, one_sem, low_r, wy_r, wx_r, ag_r, end_r, turn_r, c_r,
):
    f32, bf16 = jnp.float32, jnp.bfloat16
    dp, mp = lax.axis_index("dp"), lax.axis_index("mp")
    z, yl, core = mp // 2, lax.rem(mp, 2), lax.rem(dp, 2)
    nx_chips = ndp // 4
    row_of_x = dp // (2 * nx_chips) * (2 * nx_chips)
    x = lax.rem(dp // 2, nx_chips)
    odd = lax.rem(x, 2)
    rows, depth = tok.shape
    half = depth // 2
    col = nz * rows
    width = grad.shape[1]
    heads = width // HEAD_DIM
    chunks = half // CHUNK
    quarter = half // 4
    slab = half // nz

    def at(start, size, unit):
        return pl.ds(pl.multiple_of(start, unit), size)

    up = {"mp": lax.rem(z + 1, nz) * 2 + yl}
    down = {"mp": lax.rem(z + nz - 1, nz) * 2 + yl}
    pair = {"mp": mp + 1 - 2 * yl}
    far = {"dp": lax.rem(dp + ndp // 2, ndp), "mp": mp + 1 - 2 * yl}
    twin = {"dp": dp + 1 - 2 * core}
    east = {"dp": row_of_x + lax.rem(x + 1, nx_chips) * 2 + core}
    west = {"dp": row_of_x + lax.rem(x + nx_chips - 1, nx_chips) * 2 + core}
    along = (up, down)

    loads = [
        pltpu.make_async_copy(src, dst, in_sem.at[i])
        for i, (src, dst) in enumerate((
            (tok_h, tok), (gain_h, gain.at[0]), (grad_h, grad), (rope_h, rope),
            (bias_h, bias.at[0, pl.ds(0, width)]),
            (w_h.at[at(core * half, half, half), :], w.at[:, pl.ds(0, width)]),
        ))
    ]
    loads[0].start()
    loads[1].start()

    barrier = pltpu.get_barrier_semaphore()
    peers = (up, down, pair, far, twin, east, west)
    for there in peers:
        pl.semaphore_signal(barrier, inc=1, device_id=there, device_id_type=MESH)

    def remote(src, dst, send, recv, there):
        return pltpu.make_async_remote_copy(
            src_ref=src, dst_ref=dst, send_sem=send_sem.at[send], recv_sem=recv,
            device_id=there, device_id_type=MESH,
        )

    own_cols, pair_cols = pl.ds(0, width), pl.ds(width, width)

    def w_send(a, there):
        i = 2 * a + odd
        return remote(
            w_h.at[at(core * half + i * WCHUNK, WCHUNK, WCHUNK), :],
            w.at[at(i * WCHUNK, WCHUNK, WCHUNK), pair_cols], 0, wy_r.at[a], there,
        )

    def w_pass(a):
        ref = w.at[at((2 * a + odd) * WCHUNK, WCHUNK, WCHUNK), pair_cols]
        return remote(ref, ref, 0, wx_r.at[a], east if a % 2 == 0 else west)

    def w_last():
        i = 2 * chunks - 1 - odd
        return remote(
            w_h.at[at(core * half + i * WCHUNK, WCHUNK, WCHUNK), :],
            w.at[at(i * WCHUNK, WCHUNK, WCHUNK), pair_cols], 0, wx_r.at[chunks - 1], pair,
        )

    def w_come(k):
        ref = w.at[at((2 * k + 1 - odd) * WCHUNK, WCHUNK, WCHUNK), pair_cols]
        return remote(ref, ref, 0, wx_r.at[k], east)

    mine = at(core * col, col, col)
    other = at((1 - core) * col, col, col)
    home = at(core * col + z * rows, rows, rows)
    nx_send = remote(nx, held.at[home, :], 1, one_sem.at[0], twin)

    def ag(way, j, e):
        d = lax.rem(core + e // 4, 2)
        b = lax.rem(z + (nz - j if way == 0 else j), nz)
        ref = held.at[at(d * col + b * rows, rows, rows), at(lax.rem(e, 4) * quarter, quarter, quarter)]
        on = jnp.where(lax.rem(e, 2) == way, 16 + e // 2, 20)
        place = jnp.where(j < 2, j * 8 + e, jnp.where(j == 2, on, 20))
        return remote(ref, ref, 1, ag_r.at[way, place], along[way])

    loads[0].wait()
    loads[1].wait()
    for l in loads[2:]:
        l.start()
    total = jnp.zeros((rows, 1), f32)
    for q in range(8):
        v = tok[:, q * quarter:(q + 1) * quarter].astype(f32)
        total = total + jnp.sum(v * v, axis=1, keepdims=True)
    scale = lax.rsqrt(total / depth + 1e-06)

    def normed(ks):
        return (tok[:, ks].astype(f32) * scale * gain[:, ks]).astype(bf16)

    for q in range(4):
        held[home, q * quarter:(q + 1) * quarter] = normed(at(core * half + q * quarter, quarter, quarter))
    pl.semaphore_wait(barrier, len(peers))
    for q in range(4):
        for way in range(2):
            ag(way, 0, q).start()
    for q in range(4):
        nx[:, q * quarter:(q + 1) * quarter] = normed(at((1 - core) * half + q * quarter, quarter, quarter))
    nx_send.start()
    bias_send = remote(bias_h, bias.at[0, pair_cols], 4, one_sem.at[1], pair)
    bias_send.start()
    for a in (0, 1, 3, 5, 7):
        w_send(a, far).start()

    loads[2].wait()
    loads[3].wait()
    bacc[...] = jnp.zeros_like(bacc)

    @pl.loop(0, nz)
    def _(b):
        for side, y in ((0, yl), (1, 1 - yl)):
            here = at((2 * b + y) * rows, rows, rows)
            there = at(b * rows, rows, rows)
            cs, sn = rope[0, y, there, :], rope[1, y, there, :]
            for h in range(heads):
                hs = slice(h * HEAD_DIM, (h + 1) * HEAD_DIM)
                v = grad[here, hs].astype(f32)
                turned = v * cs - pltpu.roll(v, HEAD_DIM // 2, 1) * sn
                plain = lax.rem(mp * heads + h, GROUP) == GROUP - 1
                v = jnp.where(plain, v, turned)
                bacc[:, hs] += jnp.sum(v.reshape(rows // 8, 8, HEAD_DIM), axis=0)
                if side == 0:
                    low[at(core * col + b * rows, rows, rows), hs] = v.astype(bf16)
                else:
                    lowx[there, hs] = v.astype(bf16)

    low_pair = remote(lowx, low.at[mine, pair_cols], 0, low_r.at[0], pair)
    low_twin = remote(low.at[mine, own_cols], low.at[mine, own_cols], 0, low_r.at[1], twin)
    low_fwd = remote(low.at[mine, pair_cols], low.at[mine, pair_cols], 0, low_r.at[1], twin)
    low_pair.start()
    low_twin.start()
    for a in (2, 4, 6):
        w_send(a, pair).start()
    w_last().start()
    nx_send.wait_recv()
    for q in range(4):
        for way in range(2):
            ag(way, 0, 4 + q).start()
    bg_ref[...] = jnp.sum(bacc[...], axis=0, keepdims=True)

    def cols(k):
        return at(k * CHUNK, CHUNK, CHUNK)

    def backward(k):
        @pl.when(k == chunks - 1)
        def _():
            w_send(chunks - 1, far).wait_recv()

        w_come(k).wait_recv()
        part[:, cols(k)] = lax.dot_general(
            low[...], w[cols(k), :], (((1,), (1,)), ((), ())), preferred_element_type=f32
        )

    def rs(way, j, k):
        place = j * 8 + jnp.where(j < 2, k, k // 2)
        return remote(
            run.at[way, j, :, cols(k)], run.at[way, j + 1, :, cols(k)], 1, ag_r.at[way, place], along[way]
        )

    def rs_end(way, j, k, d):
        return remote(
            run.at[way, j, pl.ds(d * rows, rows), cols(k)],
            rfin.at[way, :, at(core * half + k * CHUNK, CHUNK, CHUNK)],
            1, end_r.at[jnp.where(j < 3, 0, jnp.where(k < chunks - 2, 1, 2))], dict(along[way], dp=dp - core + d),
        )

    def hops(way, k):
        return jnp.where(lax.rem(k, 2) == way, 4, 3)

    turning = (nz - 1, 1)

    def turned(way, k):
        return remote(
            run.at[way, 0, :, cols(k)], run.at[1 - way, 0, :, cols(k)], 1, turn_r.at[way, k], along[1 - way]
        )

    def rs_term(way, j, k, more):
        left = hops(way, k) - j
        t = lax.rem(z + (left if way == 0 else nz - left), nz)
        for d in range(2):
            ds = pl.ds(d * rows, rows)
            v = part[at(d * col + t * rows, rows, rows), cols(k)]
            if more:
                v = v + run[way, j, ds, cols(k)].astype(f32)
            run[way, j, ds, cols(k)] = v.astype(bf16)

    def rs_turn(k):
        for way in range(2):
            @pl.when(z == turning[way])
            def _():
                rs_term(way, 0, k, False)
                turned(way, k).start()

    def rs_first(way, k):
        joins = (k < TURNED) & (z == (2, nz - 2)[way])

        @pl.when((k >= TURNED) | (z != turning[way]))
        def _():
            @pl.when(joins)
            def _():
                turned(1 - way, jnp.where(k < TURNED, k, 0)).wait_recv()
                rs_term(way, 0, k, True)

            @pl.when(jnp.logical_not(joins))
            def _():
                rs_term(way, 0, k, False)

            rs(way, 0, k).start()

    def rs_step(way, j, k):
        left = hops(way, k) - j
        starts = (j == 1) & (k < TURNED) & (z == 0)

        @pl.when(starts)
        def _():
            rs_term(way, j, k, False)

        @pl.when(jnp.logical_not(starts))
        def _():
            rs(way, j - 1, k).wait_recv()
            rs_term(way, j, k, True)

        @pl.when(left > 1)
        def _():
            rs(way, j, k).start()

        @pl.when(left == 1)
        def _():
            for d in range(2):
                rs_end(way, j, k, d).start()

    own_half = at(core * half, half, half)
    swap = remote(
        part.at[at((1 - core) * col + z * rows, rows, rows), :], ng.at[:, own_half], 1, one_sem.at[2], twin
    )

    def ended(group):
        count = (chunks // 2, chunks // 2 - 1, 1)[group]
        ref = rfin.at[0, :, pl.ds(0, 4 * count * CHUNK)]
        remote(ref, ref, 1, end_r.at[group], up).wait_recv()

    def gain_share(k):
        full = at(core * half + k * CHUNK, CHUNK, CHUNK)
        for ds, to, ks in ((mine, gtot, full), (other, gx, cols(k))):
            share = jnp.sum(part[ds, cols(k)] * held[ds, cols(k)].astype(f32), axis=0, keepdims=True)
            to[:, ks] = share / gain[:, full]

    gx_send = remote(gx, gtot.at[:, own_half], 3, one_sem.at[3], twin)
    gy_send = remote(gtot.at[:, at((1 - yl) * half, half, half)], gy, 3, one_sem.at[7], pair)
    column_half = at(yl * half, half, half)
    g3_send = remote(gres.at[:, column_half], gres.at[:, column_half], 7, one_sem.at[8], pair)

    lines = slab // HEAD_DIM

    def line_of(zz, i):
        return at(yl * half + zz * slab + i * HEAD_DIM, HEAD_DIM, HEAD_DIM)

    def g1(k):
        to = lax.rem(z + k, nz)
        return remote(gsend.at[to], grecv.at[k - 1], 5, one_sem.at[4], {"mp": 2 * to + yl})

    def g2(k):
        to = lax.rem(z + k, nz)
        return remote(gdone.at[z], gdone.at[z], 6, one_sem.at[5], {"mp": 2 * to + yl})

    g1_all = remote(grecv, grecv, 5, one_sem.at[4], up)
    g2_all = remote(grecv, grecv, 6, one_sem.at[5], up)

    def tile(t):
        return at(t * TILE_N, TILE_N, TILE_N)

    def c_send(t):
        return remote(acc.at[other, tile(t)], cx.at[:, tile(t)], 2, c_r.at[0], twin)

    def forward(t):
        acc[:, tile(t)] = jnp.dot(held[...], w[:, tile(t)], preferred_element_type=f32)
        c_send(t).start()

    def q_send(h):
        return remote(
            qt.at[:, at(width + h * HEAD_DIM, HEAD_DIM, HEAD_DIM)], qx.at[:, at(h * HEAD_DIM, HEAD_DIM, HEAD_DIM)],
            2, one_sem.at[6], pair,
        )

    q_all = remote(qx, qx, 2, one_sem.at[6], pair)

    c_all = remote(cx, cx, 2, c_r.at[0], twin)

    def joined(t):
        for i in range(TILE_N // HEAD_DIM):
            h = t * (TILE_N // HEAD_DIM) + i
            hs = at(h * HEAD_DIM, HEAD_DIM, HEAD_DIM)
            v = acc[mine, hs] + cx[:, hs] + bias[:, hs]
            turned = v * rope[0, yl] + pltpu.roll(v, HEAD_DIM // 2, 1) * rope[1, yl]
            whole = jnp.where(h < heads, mp * heads + h, (mp + 1 - 2 * yl) * heads + h - heads)
            qt[:, hs] = jnp.where(lax.rem(whole, GROUP) == GROUP - 1, v, turned).astype(bf16)

            @pl.when(h >= heads)
            def _():
                q_send(h - heads).start()

    passes = (4, 9, 11, 14, 16, 19, 21)
    early = (12, 17, 18, 22, 23)
    ahead = 3

    @pl.loop(0, 24)
    def _(i):
        j, e = 1 + i // 8, lax.rem(i, 8)
        for way in range(2):
            @pl.when((j < 3) | (lax.rem(e, 2) == way))
            def _():
                ag(way, j - 1, e).wait_recv()
                ag(way, j, e).start()

        @pl.when(i >= 24 - ahead)
        def _():
            k = i - (24 - ahead)
            for way in range(2):
                rs_first(way, jnp.where(k < 1, k, k + 1))

        @pl.when(i == 13)
        def _():
            rs_turn(0)

        @pl.when(i == 18)
        def _():
            rs_turn(1)

        for a, step in enumerate(passes):
            @pl.when(i == step)
            def _():
                w_send(a, pair).wait_recv()
                w_pass(a).start()

        @pl.when(i == 6)
        def _():
            low_pair.wait_recv()
            low_fwd.start()

        @pl.when(i == 9)
        def _():
            loads[5].wait()
            remote(grad, grad, 0, low_r.at[1], twin).wait_recv()

        k, due = 0, i == early[0]
        for m in range(1, len(early)):
            k, due = jnp.where(i >= early[m], m, k), due | (i == early[m])

        @pl.when(due)
        def _():
            backward(k)

    @pl.loop(ahead, chunks)
    def _(m):
        k = jnp.where(m == ahead, 1, jnp.where(m < chunks - 2, m, 2 * chunks - 3 - m))

        @pl.when(m >= len(early))
        def _():
            backward(k)

        for way in range(2):
            rs_first(way, k)

    swap.start()
    for q in range(4):
        ks = pl.ds(q * quarter, quarter)
        ng[:, at(core * half + q * quarter, quarter, quarter)] = part[home, ks]
    for way in range(2):
        ref = held.at[pl.ds(0, 2 * rows), :]
        remote(ref, ref, 1, ag_r.at[way, 20], up).wait_recv()
    loads[4].wait()
    bias_send.wait_recv()

    @pl.loop(0, chunks)
    def _(k):
        gain_share(k)

    gx_send.start()

    @pl.loop(0, 20)
    def _(m):
        j, q = 1 + m // 8, lax.rem(m, 8)
        for way in range(2):
            rs_step(way, j, jnp.where(j < 3, q, 2 * q + way))

        @pl.when(m == 7)
        def _():
            c_all.wait_recv()

        @pl.when((m >= 7) & (m < 12))
        def _():
            joined(lax.rem(m, 5))

        @pl.when(m < 5)
        def _():
            forward(lax.rem(m + 2, 5))

        @pl.when(m == 1)
        def _():
            gx_send.wait_recv()
            gy_send.start()

        @pl.when(m == 4)
        def _():
            gy_send.wait_recv()
            gtot[:, column_half] += gy[...]
            for zz in range(nz):
                for i in range(lines):
                    gstage[zz, i:i + 1, :] = gtot[:, line_of(zz, i)]
            gsend[...] = gstage[...].astype(bf16)
            for k in range(1, nz):
                g1(k).start()

        @pl.when(m == 13)
        def _():
            g1_all.wait_recv()
            share = gstage[z]
            for k in range(1, nz):
                share = share + grecv[k - 1].astype(f32)
            gdone[z] = share.astype(bf16)
            for k in range(1, nz):
                g2(k).start()

        @pl.when(m == 16)
        def _():
            q_all.wait_recv()
            for b in range(nz):
                there = pl.ds(b * rows, rows)
                qkv[at((2 * b + yl) * rows, rows, rows), :] = qt[there, own_cols]
                qkv[at((2 * b + 1 - yl) * rows, rows, rows), :] = qx[there, :]

    g2_all.wait_recv()
    gstage[...] = gdone[...].astype(f32)
    for zz in range(nz):
        for i in range(lines):
            gres[:, line_of(zz, i)] = gstage[zz, i:i + 1, :]
    g3_send.start()
    swap.wait_recv()
    ended(0)
    for q in range(2 * chunks):
        ks = slice(q * CHUNK, (q + 1) * CHUNK)
        ng[:, ks] += rfin[1 - q % 2, :, ks].astype(f32)
    inner = jnp.zeros((rows, 1), f32)
    for group, ks_in in ((1, range(chunks - 2)), (2, range(chunks - 2, chunks))):
        ended(group)
        for side in range(2):
            for k in ks_in:
                q = side * chunks + k
                ks = slice(q * CHUNK, (q + 1) * CHUNK)
                v = ng[:, ks] + rfin[k % 2, :, ks].astype(f32)
                total_ng[:, ks] = v
                inner = inner + jnp.sum(v * tok[:, ks].astype(f32) * gain[:, ks], axis=1, keepdims=True)
    factors[0] = jnp.broadcast_to(scale, factors.shape[1:])
    factors[1] = jnp.broadcast_to(scale * scale * scale * (inner / depth), factors.shape[1:])

    g3_send.wait_recv()
    gg_ref[...] = gres[...]

    def sent(ref, send):
        remote(ref, ref, send, one_sem.at[0], twin).wait_send()

    sent(w_h.at[pl.ds(0, 2 * chunks * WCHUNK + 3 * col), :], 0)
    sent(part.at[pl.ds(0, (2 * 7 + 1) * rows + rows // 2), :], 1)
    sent(acc.at[pl.ds(0, col + col // 4), :], 2)
    sent(gtot, 3)
    bias_send.wait_send()
    sent(grecv, 5)
    sent(grecv, 6)
    g3_send.wait_send()


def finish(qkv, ng, tok, gain, factors, gg, bg, qkv_h, tg_h, gg_h, bg_h, tg, sem):
    parts = sem.shape[0] - 3
    piece = tok.shape[1] // parts
    copies = [
        pltpu.make_async_copy(src, dst, sem.at[i])
        for i, (src, dst) in enumerate(((qkv, qkv_h), (gg.at[0], gg_h), (bg.at[0], bg_h)))
    ]
    for c in copies:
        c.start()
    scale, weight = factors[0, :, :1], factors[1, :, :1]
    for q in range(parts):
        ks = slice(q * piece, (q + 1) * piece)
        tg[:, ks] = scale * gain[:, ks] * ng[:, ks] - tok[:, ks].astype(jnp.float32) * weight
        c = pltpu.make_async_copy(tg.at[:, ks], tg_h.at[:, ks], sem.at[3 + q])
        c.start()
        copies.append(c)
    for c in copies:
        c.wait()


def shards(n, ndp, tokens, norm_gain, qkv_weight, qkv_bias, qkv_grad):
    rows, depth = tokens.shape
    every, width = qkv_grad.shape
    rope = rope_tables(every, rows, SEQ_LEN // n)
    bf16, f32 = jnp.bfloat16, jnp.float32
    half, col, nz = depth // 2, every // 2, n // 2
    slab = half // nz
    chunks = half // CHUNK
    dma = pltpu.SemaphoreType.DMA
    vm = pltpu.VMEM
    hbm = pl.BlockSpec(memory_space=pl.ANY)
    vmem = pl.BlockSpec(memory_space=pltpu.VMEM)
    results = pl.pallas_call(
        functools.partial(kernel, nz, ndp),
        out_shape=(
            vm((every, width), bf16),
            vm((rows, depth), f32),
            vm((rows, depth), bf16),
            vm((1, depth), f32),
            vm((2, rows, HEAD_DIM), f32),
            vm((1, depth), f32),
            vm((1, width), f32),
        ),
        in_specs=[hbm] * 6,
        out_specs=[vmem] * 7,
        scratch_shapes=[
            vm((half, 2 * width), bf16),
            vm((1, 2 * width), f32),
            vm((every, width), bf16),
            vm((2, 2, col, HEAD_DIM), f32),
            vm((every, 2 * width), bf16),
            vm((col, width), bf16),
            vm((rows, half), bf16),
            vm((every, half), bf16),
            vm((every, half), f32),
            vm((2, 4, 2 * rows, half), bf16),
            vm((2, rows, depth), bf16),
            vm((every, 2 * width), f32),
            vm((col, 2 * width), f32),
            vm((col, 2 * width), bf16),
            vm((col, width), bf16),
            vm((rows, depth), f32),
            vm((1, depth), f32),
            vm((1, half), f32),
            vm((1, half), f32),
            vm((nz, slab // HEAD_DIM, HEAD_DIM), f32),
            vm((nz, slab // HEAD_DIM, HEAD_DIM), bf16),
            vm((nz - 1, slab // HEAD_DIM, HEAD_DIM), bf16),
            vm((nz, slab // HEAD_DIM, HEAD_DIM), bf16),
            vm((1, depth), f32),
            vm((8, width), f32),
            dma((6,)),
            dma((8,)),
            dma((9,)),
            dma((2,)),
            dma((chunks,)),
            dma((chunks,)),
            dma((2, 21)),
            dma((3,)),
            dma((2, TURNED)),
            dma((1,)),
        ],
        compiler_params=pltpu.CompilerParams(
            collective_id=0, has_side_effects=True, vmem_limit_bytes=60000000
        ),
        cost_estimate=pl.CostEstimate(
            flops=4 * every * depth * width, bytes_accessed=2 * depth * width, transcendentals=0
        ),
    )(
        tokens, norm_gain, qkv_weight, qkv_bias, qkv_grad,
        jnp.asarray(rope),
    )
    return pl.pallas_call(
        finish,
        out_shape=(
            jax.ShapeDtypeStruct((every, width), bf16),
            jax.ShapeDtypeStruct((rows, depth), f32),
            jax.ShapeDtypeStruct((depth,), f32),
            jax.ShapeDtypeStruct((width,), f32),
        ),
        in_specs=[vmem] * 7,
        out_specs=[hbm] * 4,
        scratch_shapes=[vm((rows, depth), f32), dma((7,))],
        compiler_params=pltpu.CompilerParams(vmem_limit_bytes=1 << 21),
    )(*results)


def solution(mesh):
    in_specs = (P(("dp", "mp"), None), P(), P(None, "mp"), P("mp"), P("dp", "mp"))
    out_specs = (P("dp", "mp"), P(("dp", "mp"), None), P("dp"), P(("dp", "mp")))
    body = functools.partial(shards, mesh.shape["mp"], mesh.shape["dp"])
    return jax.shard_map(body, mesh=mesh, in_specs=in_specs, out_specs=out_specs, check_vma=False)
```

```python
import functools

import jax
import jax.numpy as jnp
import numpy as np
from jax import lax
from jax.experimental import pallas as pl
from jax.experimental.pallas import tpu as pltpu
from jax.sharding import PartitionSpec as P

HEAD_DIM = 128
SEQ_LEN = 32768
GROUP = 10
MESH = pl.DeviceIdType.MESH
CHUNK = 512
WCHUNK = 256
TILE_N = 256
TURNED = 2


def rope_tables(rows, tok_dev, stride):
    half = HEAD_DIM // 2
    row = np.arange(rows)
    place = (row // tok_dev * stride + row % tok_dev).astype(np.float32)
    inverse = np.exp(
        -np.log(np.float32(1000000.0))
        * (np.float32(2.0) * np.arange(half).astype(np.float32) / np.float32(HEAD_DIM))
    ).astype(np.float32)
    angle = (place[:, None] * inverse[None, :]).astype(np.float32)
    cosine, sine = np.cos(angle).astype(np.float32), np.sin(angle).astype(np.float32)

    def by_column(t):
        t = t.reshape(rows // (2 * tok_dev), 2, tok_dev, HEAD_DIM)
        return np.ascontiguousarray(np.swapaxes(t, 0, 1)).reshape(2, rows // 2, HEAD_DIM)

    return np.stack([by_column(np.concatenate([cosine, cosine], 1)), by_column(np.concatenate([-sine, sine], 1))])


def kernel(
    nz, ndp,
    tok_h, gain_h, w_h, bias_h, grad_h, rope_h,
    qkv, total_ng, tok, gain, factors, gg_ref, bg_ref,
    w, bias, grad, rope,
    low, lowx, nx, held, part, run, rfin, acc, cx, qt, qx, ng, gtot, gx, gy, gstage, gsend, grecv, gdone, gres, bacc,
    in_sem, send_sem, one_sem, low_r, wy_r, wx_r, ag_r, end_r, turn_r, c_r,
):
    f32, bf16 = jnp.float32, jnp.bfloat16
    dp, mp = lax.axis_index("dp"), lax.axis_index("mp")
    z, yl, core = mp // 2, lax.rem(mp, 2), lax.rem(dp, 2)
    nx_chips = ndp // 4
    row_of_x = dp // (2 * nx_chips) * (2 * nx_chips)
    x = lax.rem(dp // 2, nx_chips)
    odd = lax.rem(x, 2)
    rows, depth = tok.shape
    half = depth // 2
    col = nz * rows
    width = grad.shape[1]
    heads = width // HEAD_DIM
    chunks = half // CHUNK
    quarter = half // 4
    slab = half // nz

    def at(start, size, unit):
        return pl.ds(pl.multiple_of(start, unit), size)

    up = {"mp": lax.rem(z + 1, nz) * 2 + yl}
    down = {"mp": lax.rem(z + nz - 1, nz) * 2 + yl}
    pair = {"mp": mp + 1 - 2 * yl}
    far = {"dp": lax.rem(dp + ndp // 2, ndp), "mp": mp + 1 - 2 * yl}
    twin = {"dp": dp + 1 - 2 * core}
    east = {"dp": row_of_x + lax.rem(x + 1, nx_chips) * 2 + core}
    west = {"dp": row_of_x + lax.rem(x + nx_chips - 1, nx_chips) * 2 + core}
    along = (up, down)

    loads = [
        pltpu.make_async_copy(src, dst, in_sem.at[i])
        for i, (src, dst) in enumerate((
            (tok_h, tok), (gain_h, gain.at[0]), (grad_h, grad), (rope_h, rope),
            (bias_h, bias.at[0, pl.ds(0, width)]),
            (w_h.at[at(core * half, half, half), :], w.at[:, pl.ds(0, width)]),
        ))
    ]
    loads[0].start()
    loads[1].start()

    barrier = pltpu.get_barrier_semaphore()
    peers = (up, down, pair, far, twin, east, west)
    for there in peers:
        pl.semaphore_signal(barrier, inc=1, device_id=there, device_id_type=MESH)

    def remote(src, dst, send, recv, there):
        return pltpu.make_async_remote_copy(
            src_ref=src, dst_ref=dst, send_sem=send_sem.at[send], recv_sem=recv,
            device_id=there, device_id_type=MESH,
        )

    own_cols, pair_cols = pl.ds(0, width), pl.ds(width, width)

    def w_send(a, there):
        i = 2 * a + odd
        return remote(
            w_h.at[at(core * half + i * WCHUNK, WCHUNK, WCHUNK), :],
            w.at[at(i * WCHUNK, WCHUNK, WCHUNK), pair_cols], 0, wy_r.at[a], there,
        )

    def w_pass(a):
        ref = w.at[at((2 * a + odd) * WCHUNK, WCHUNK, WCHUNK), pair_cols]
        return remote(ref, ref, 0, wx_r.at[a], east if a % 2 == 0 else west)

    def w_last():
        i = 2 * chunks - 1 - odd
        return remote(
            w_h.at[at(core * half + i * WCHUNK, WCHUNK, WCHUNK), :],
            w.at[at(i * WCHUNK, WCHUNK, WCHUNK), pair_cols], 0, wx_r.at[chunks - 1], pair,
        )

    def w_come(k):
        ref = w.at[at((2 * k + 1 - odd) * WCHUNK, WCHUNK, WCHUNK), pair_cols]
        return remote(ref, ref, 0, wx_r.at[k], east)

    mine = at(core * col, col, col)
    other = at((1 - core) * col, col, col)
    home = at(core * col + z * rows, rows, rows)
    nx_send = remote(nx, held.at[home, :], 1, one_sem.at[0], twin)

    def ag(way, j, e):
        d = lax.rem(core + e // 4, 2)
        b = lax.rem(z + (nz - j if way == 0 else j), nz)
        ref = held.at[at(d * col + b * rows, rows, rows), at(lax.rem(e, 4) * quarter, quarter, quarter)]
        on = jnp.where(lax.rem(e, 2) == way, 16 + e // 2, 20)
        place = jnp.where(j < 2, j * 8 + e, jnp.where(j == 2, on, 20))
        return remote(ref, ref, 1, ag_r.at[way, place], along[way])

    loads[0].wait()
    loads[1].wait()
    for l in loads[2:]:
        l.start()
    total = jnp.zeros((rows, 1), f32)
    for q in range(8):
        v = tok[:, q * quarter:(q + 1) * quarter].astype(f32)
        total = total + jnp.sum(v * v, axis=1, keepdims=True)
    scale = lax.rsqrt(total / depth + 1e-06)

    def normed(ks):
        return (tok[:, ks].astype(f32) * scale * gain[:, ks]).astype(bf16)

    for q in range(4):
        held[home, q * quarter:(q + 1) * quarter] = normed(at(core * half + q * quarter, quarter, quarter))
    pl.semaphore_wait(barrier, len(peers))
    for q in range(4):
        for way in range(2):
            ag(way, 0, q).start()
    for q in range(4):
        nx[:, q * quarter:(q + 1) * quarter] = normed(at((1 - core) * half + q * quarter, quarter, quarter))
    nx_send.start()
    bias_send = remote(bias_h, bias.at[0, pair_cols], 4, one_sem.at[1], pair)
    bias_send.start()
    for a in (0, 1, 3, 5, 7):
        w_send(a, far).start()

    loads[2].wait()
    loads[3].wait()
    bacc[...] = jnp.zeros_like(bacc)

    @pl.loop(0, nz)
    def _(b):
        for side, y in ((0, yl), (1, 1 - yl)):
            here = at((2 * b + y) * rows, rows, rows)
            there = at(b * rows, rows, rows)
            cs, sn = rope[0, y, there, :], rope[1, y, there, :]
            for h in range(heads):
                hs = slice(h * HEAD_DIM, (h + 1) * HEAD_DIM)
                v = grad[here, hs].astype(f32)
                turned = v * cs - pltpu.roll(v, HEAD_DIM // 2, 1) * sn
                plain = lax.rem(mp * heads + h, GROUP) == GROUP - 1
                v = jnp.where(plain, v, turned)
                bacc[:, hs] += jnp.sum(v.reshape(rows // 8, 8, HEAD_DIM), axis=0)
                if side == 0:
                    low[at(core * col + b * rows, rows, rows), hs] = v.astype(bf16)
                else:
                    lowx[there, hs] = v.astype(bf16)

    low_pair = remote(lowx, low.at[mine, pair_cols], 0, low_r.at[0], pair)
    low_twin = remote(low.at[mine, own_cols], low.at[mine, own_cols], 0, low_r.at[1], twin)
    low_fwd = remote(low.at[mine, pair_cols], low.at[mine, pair_cols], 0, low_r.at[1], twin)
    low_pair.start()
    low_twin.start()
    for a in (2, 4, 6):
        w_send(a, pair).start()
    w_last().start()
    nx_send.wait_recv()
    for q in range(4):
        for way in range(2):
            ag(way, 0, 4 + q).start()
    bg_ref[...] = jnp.sum(bacc[...], axis=0, keepdims=True)

    def cols(k):
        return at(k * CHUNK, CHUNK, CHUNK)

    def backward(k):
        @pl.when(k == chunks - 1)
        def _():
            w_send(chunks - 1, far).wait_recv()

        w_come(k).wait_recv()
        part[:, cols(k)] = lax.dot_general(
            low[...], w[cols(k), :], (((1,), (1,)), ((), ())), preferred_element_type=f32
        )

    def rs(way, j, k):
        place = j * 8 + jnp.where(j < 2, k, k // 2)
        return remote(
            run.at[way, j, :, cols(k)], run.at[way, j + 1, :, cols(k)], 1, ag_r.at[way, place], along[way]
        )

    def rs_end(way, j, k, d):
        return remote(
            run.at[way, j, pl.ds(d * rows, rows), cols(k)],
            rfin.at[way, :, at(core * half + k * CHUNK, CHUNK, CHUNK)],
            1, end_r.at[jnp.where(j < 3, 0, jnp.where(k < chunks - 2, 1, 2))], dict(along[way], dp=dp - core + d),
        )

    def hops(way, k):
        return jnp.where(lax.rem(k, 2) == way, 4, 3)

    turning = (nz - 1, 1)

    def turned(way, k):
        return remote(
            run.at[way, 0, :, cols(k)], run.at[1 - way, 0, :, cols(k)], 1, turn_r.at[way, k], along[1 - way]
        )

    def rs_term(way, j, k, more):
        left = hops(way, k) - j
        t = lax.rem(z + (left if way == 0 else nz - left), nz)
        for d in range(2):
            ds = pl.ds(d * rows, rows)
            v = part[at(d * col + t * rows, rows, rows), cols(k)]
            if more:
                v = v + run[way, j, ds, cols(k)].astype(f32)
            run[way, j, ds, cols(k)] = v.astype(bf16)

    def rs_turn(k):
        for way in range(2):
            @pl.when(z == turning[way])
            def _():
                rs_term(way, 0, k, False)
                turned(way, k).start()

    def rs_first(way, k):
        joins = (k < TURNED) & (z == (2, nz - 2)[way])

        @pl.when((k >= TURNED) | (z != turning[way]))
        def _():
            @pl.when(joins)
            def _():
                turned(1 - way, jnp.where(k < TURNED, k, 0)).wait_recv()
                rs_term(way, 0, k, True)

            @pl.when(jnp.logical_not(joins))
            def _():
                rs_term(way, 0, k, False)

            rs(way, 0, k).start()

    def rs_step(way, j, k):
        left = hops(way, k) - j
        starts = (j == 1) & (k < TURNED) & (z == 0)

        @pl.when(starts)
        def _():
            rs_term(way, j, k, False)

        @pl.when(jnp.logical_not(starts))
        def _():
            rs(way, j - 1, k).wait_recv()
            rs_term(way, j, k, True)

        @pl.when(left > 1)
        def _():
            rs(way, j, k).start()

        @pl.when(left == 1)
        def _():
            for d in range(2):
                rs_end(way, j, k, d).start()

    own_half = at(core * half, half, half)
    swap = remote(
        part.at[at((1 - core) * col + z * rows, rows, rows), :], ng.at[:, own_half], 1, one_sem.at[2], twin
    )

    def ended(group):
        count = (chunks // 2, chunks // 2 - 1, 1)[group]
        ref = rfin.at[0, :, pl.ds(0, 4 * count * CHUNK)]
        remote(ref, ref, 1, end_r.at[group], up).wait_recv()

    def gain_share(k):
        full = at(core * half + k * CHUNK, CHUNK, CHUNK)
        for ds, to, ks in ((mine, gtot, full), (other, gx, cols(k))):
            share = jnp.sum(part[ds, cols(k)] * held[ds, cols(k)].astype(f32), axis=0, keepdims=True)
            to[:, ks] = share / gain[:, full]

    gx_send = remote(gx, gtot.at[:, own_half], 3, one_sem.at[3], twin)
    gy_send = remote(gtot.at[:, at((1 - yl) * half, half, half)], gy, 3, one_sem.at[7], pair)
    column_half = at(yl * half, half, half)
    g3_send = remote(gres.at[:, column_half], gres.at[:, column_half], 7, one_sem.at[8], pair)

    lines = slab // HEAD_DIM

    def line_of(zz, i):
        return at(yl * half + zz * slab + i * HEAD_DIM, HEAD_DIM, HEAD_DIM)

    def g1(k):
        to = lax.rem(z + k, nz)
        return remote(gsend.at[to], grecv.at[k - 1], 5, one_sem.at[4], {"mp": 2 * to + yl})

    def g2(k):
        to = lax.rem(z + k, nz)
        return remote(gdone.at[z], gdone.at[z], 6, one_sem.at[5], {"mp": 2 * to + yl})

    g1_all = remote(grecv, grecv, 5, one_sem.at[4], up)
    g2_all = remote(grecv, grecv, 6, one_sem.at[5], up)

    def tile(t):
        return at(t * TILE_N, TILE_N, TILE_N)

    def c_send(t):
        return remote(acc.at[other, tile(t)], cx.at[:, tile(t)], 2, c_r.at[0], twin)

    def forward(t):
        acc[:, tile(t)] = jnp.dot(held[...], w[:, tile(t)], preferred_element_type=f32)
        c_send(t).start()

    def q_send(h):
        return remote(
            qt.at[:, at(width + h * HEAD_DIM, HEAD_DIM, HEAD_DIM)], qx.at[:, at(h * HEAD_DIM, HEAD_DIM, HEAD_DIM)],
            2, one_sem.at[6], pair,
        )

    q_all = remote(qx, qx, 2, one_sem.at[6], pair)

    c_all = remote(cx, cx, 2, c_r.at[0], twin)

    def joined(t):
        for i in range(TILE_N // HEAD_DIM):
            h = t * (TILE_N // HEAD_DIM) + i
            hs = at(h * HEAD_DIM, HEAD_DIM, HEAD_DIM)
            v = acc[mine, hs] + cx[:, hs] + bias[:, hs]
            turned = v * rope[0, yl] + pltpu.roll(v, HEAD_DIM // 2, 1) * rope[1, yl]
            whole = jnp.where(h < heads, mp * heads + h, (mp + 1 - 2 * yl) * heads + h - heads)
            qt[:, hs] = jnp.where(lax.rem(whole, GROUP) == GROUP - 1, v, turned).astype(bf16)

            @pl.when(h >= heads)
            def _():
                q_send(h - heads).start()

    passes = (4, 9, 11, 14, 16, 19, 21)
    early = (12, 17, 18, 22, 23)
    ahead = 3

    @pl.loop(0, 24)
    def _(i):
        j, e = 1 + i // 8, lax.rem(i, 8)
        for way in range(2):
            @pl.when((j < 3) | (lax.rem(e, 2) == way))
            def _():
                ag(way, j - 1, e).wait_recv()
                ag(way, j, e).start()

        @pl.when(i >= 24 - ahead)
        def _():
            k = i - (24 - ahead)
            for way in range(2):
                rs_first(way, jnp.where(k < 1, k, k + 1))

        @pl.when(i == 13)
        def _():
            rs_turn(0)

        @pl.when(i == 18)
        def _():
            rs_turn(1)

        for a, step in enumerate(passes):
            @pl.when(i == step)
            def _():
                w_send(a, pair).wait_recv()
                w_pass(a).start()

        @pl.when(i == 6)
        def _():
            low_pair.wait_recv()
            low_fwd.start()

        @pl.when(i == 9)
        def _():
            loads[5].wait()
            remote(grad, grad, 0, low_r.at[1], twin).wait_recv()

        k, due = 0, i == early[0]
        for m in range(1, len(early)):
            k, due = jnp.where(i >= early[m], m, k), due | (i == early[m])

        @pl.when(due)
        def _():
            backward(k)

    @pl.loop(ahead, chunks)
    def _(m):
        k = jnp.where(m == ahead, 1, jnp.where(m < chunks - 2, m, 2 * chunks - 3 - m))

        @pl.when(m >= len(early))
        def _():
            backward(k)

        for way in range(2):
            rs_first(way, k)

    swap.start()
    for q in range(4):
        ks = pl.ds(q * quarter, quarter)
        ng[:, at(core * half + q * quarter, quarter, quarter)] = part[home, ks]
    for way in range(2):
        ref = held.at[pl.ds(0, 2 * rows), :]
        remote(ref, ref, 1, ag_r.at[way, 20], up).wait_recv()
    loads[4].wait()
    bias_send.wait_recv()

    @pl.loop(0, chunks)
    def _(k):
        gain_share(k)

    gx_send.start()

    @pl.loop(0, 20)
    def _(m):
        j, q = 1 + m // 8, lax.rem(m, 8)
        for way in range(2):
            rs_step(way, j, jnp.where(j < 3, q, 2 * q + way))

        @pl.when(m == 7)
        def _():
            c_all.wait_recv()

        @pl.when((m >= 7) & (m < 12))
        def _():
            joined(lax.rem(m, 5))

        @pl.when(m < 5)
        def _():
            forward(lax.rem(m + 2, 5))

        @pl.when(m == 1)
        def _():
            gx_send.wait_recv()
            gy_send.start()

        @pl.when(m == 4)
        def _():
            gy_send.wait_recv()
            gtot[:, column_half] += gy[...]
            for zz in range(nz):
                for i in range(lines):
                    gstage[zz, i:i + 1, :] = gtot[:, line_of(zz, i)]
            gsend[...] = gstage[...].astype(bf16)
            for k in range(1, nz):
                g1(k).start()

        @pl.when(m == 13)
        def _():
            g1_all.wait_recv()
            share = gstage[z]
            for k in range(1, nz):
                share = share + grecv[k - 1].astype(f32)
            gdone[z] = share.astype(bf16)
            for k in range(1, nz):
                g2(k).start()

        @pl.when(m == 16)
        def _():
            q_all.wait_recv()
            for b in range(nz):
                there = pl.ds(b * rows, rows)
                qkv[at((2 * b + yl) * rows, rows, rows), :] = qt[there, own_cols]
                qkv[at((2 * b + 1 - yl) * rows, rows, rows), :] = qx[there, :]

    g2_all.wait_recv()
    gstage[...] = gdone[...].astype(f32)
    for zz in range(nz):
        for i in range(lines):
            gres[:, line_of(zz, i)] = gstage[zz, i:i + 1, :]
    g3_send.start()
    swap.wait_recv()
    ended(0)
    for q in range(2 * chunks):
        ks = slice(q * CHUNK, (q + 1) * CHUNK)
        ng[:, ks] += rfin[1 - q % 2, :, ks].astype(f32)
    inner = jnp.zeros((rows, 1), f32)
    for group, ks_in in ((1, range(chunks - 2)), (2, range(chunks - 2, chunks))):
        ended(group)
        for side in range(2):
            for k in ks_in:
                q = side * chunks + k
                ks = slice(q * CHUNK, (q + 1) * CHUNK)
                v = ng[:, ks] + rfin[k % 2, :, ks].astype(f32)
                total_ng[:, ks] = v
                inner = inner + jnp.sum(v * tok[:, ks].astype(f32) * gain[:, ks], axis=1, keepdims=True)
    factors[0] = jnp.broadcast_to(scale, factors.shape[1:])
    factors[1] = jnp.broadcast_to(scale * scale * scale * (inner / depth), factors.shape[1:])

    g3_send.wait_recv()
    gg_ref[...] = gres[...]

    def sent(ref, send):
        remote(ref, ref, send, one_sem.at[0], twin).wait_send()

    sent(w_h.at[pl.ds(0, 2 * chunks * WCHUNK + 3 * col), :], 0)
    sent(part.at[pl.ds(0, (2 * 7 + 1) * rows + rows // 2), :], 1)
    sent(acc.at[pl.ds(0, col + col // 4), :], 2)
    sent(gtot, 3)
    bias_send.wait_send()
    sent(grecv, 5)
    sent(grecv, 6)
    g3_send.wait_send()


def finish(qkv, ng, tok, gain, factors, gg, bg, qkv_h, tg_h, gg_h, bg_h, tg, sem):
    parts = (sem.shape[0] - 2) // 2
    rows, depth = tok.shape
    piece, lines = rows // parts, qkv.shape[0] // parts
    copies = [
        pltpu.make_async_copy(src, dst, sem.at[i]) for i, (src, dst) in enumerate(((gg.at[0], gg_h), (bg.at[0], bg_h)))
    ]
    for q in range(parts):
        rs = slice(q * lines, (q + 1) * lines)
        copies.append(pltpu.make_async_copy(qkv.at[rs], qkv_h.at[rs], sem.at[2 + q]))
    for c in copies:
        c.start()
    for q in range(parts):
        rs = slice(q * piece, (q + 1) * piece)
        scale, weight = factors[0, rs, :1], factors[1, rs, :1]
        tg[rs] = scale * gain[...] * ng[rs] - tok[rs].astype(jnp.float32) * weight
        c = pltpu.make_async_copy(tg.at[rs], tg_h.at[rs], sem.at[2 + parts + q])
        c.start()
        copies.append(c)
    for c in copies:
        c.wait()


def shards(n, ndp, tokens, norm_gain, qkv_weight, qkv_bias, qkv_grad):
    rows, depth = tokens.shape
    every, width = qkv_grad.shape
    rope = rope_tables(every, rows, SEQ_LEN // n)
    bf16, f32 = jnp.bfloat16, jnp.float32
    half, col, nz = depth // 2, every // 2, n // 2
    slab = half // nz
    chunks = half // CHUNK
    dma = pltpu.SemaphoreType.DMA
    vm = pltpu.VMEM
    hbm = pl.BlockSpec(memory_space=pl.ANY)
    vmem = pl.BlockSpec(memory_space=pltpu.VMEM)
    results = pl.pallas_call(
        functools.partial(kernel, nz, ndp),
        out_shape=(
            vm((every, width), bf16),
            vm((rows, depth), f32),
            vm((rows, depth), bf16),
            vm((1, depth), f32),
            vm((2, rows, HEAD_DIM), f32),
            vm((1, depth), f32),
            vm((1, width), f32),
        ),
        in_specs=[hbm] * 6,
        out_specs=[vmem] * 7,
        scratch_shapes=[
            vm((half, 2 * width), bf16),
            vm((1, 2 * width), f32),
            vm((every, width), bf16),
            vm((2, 2, col, HEAD_DIM), f32),
            vm((every, 2 * width), bf16),
            vm((col, width), bf16),
            vm((rows, half), bf16),
            vm((every, half), bf16),
            vm((every, half), f32),
            vm((2, 4, 2 * rows, half), bf16),
            vm((2, rows, depth), bf16),
            vm((every, 2 * width), f32),
            vm((col, 2 * width), f32),
            vm((col, 2 * width), bf16),
            vm((col, width), bf16),
            vm((rows, depth), f32),
            vm((1, depth), f32),
            vm((1, half), f32),
            vm((1, half), f32),
            vm((nz, slab // HEAD_DIM, HEAD_DIM), f32),
            vm((nz, slab // HEAD_DIM, HEAD_DIM), bf16),
            vm((nz - 1, slab // HEAD_DIM, HEAD_DIM), bf16),
            vm((nz, slab // HEAD_DIM, HEAD_DIM), bf16),
            vm((1, depth), f32),
            vm((8, width), f32),
            dma((6,)),
            dma((8,)),
            dma((9,)),
            dma((2,)),
            dma((chunks,)),
            dma((chunks,)),
            dma((2, 21)),
            dma((3,)),
            dma((2, TURNED)),
            dma((1,)),
        ],
        compiler_params=pltpu.CompilerParams(
            collective_id=0, has_side_effects=True, vmem_limit_bytes=60000000
        ),
        cost_estimate=pl.CostEstimate(
            flops=4 * every * depth * width, bytes_accessed=2 * depth * width, transcendentals=0
        ),
    )(
        tokens, norm_gain, qkv_weight, qkv_bias, qkv_grad,
        jnp.asarray(rope),
    )
    return pl.pallas_call(
        finish,
        out_shape=(
            jax.ShapeDtypeStruct((every, width), bf16),
            jax.ShapeDtypeStruct((rows, depth), f32),
            jax.ShapeDtypeStruct((depth,), f32),
            jax.ShapeDtypeStruct((width,), f32),
        ),
        in_specs=[vmem] * 7,
        out_specs=[hbm] * 4,
        scratch_shapes=[vm((rows, depth), f32), dma((2 + 2 * 4,))],
        compiler_params=pltpu.CompilerParams(vmem_limit_bytes=1 << 21),
    )(*results)


def solution(mesh):
    in_specs = (P(("dp", "mp"), None), P(), P(None, "mp"), P("mp"), P("dp", "mp"))
    out_specs = (P("dp", "mp"), P(("dp", "mp"), None), P("dp"), P(("dp", "mp")))
    body = functools.partial(shards, mesh.shape["mp"], mesh.shape["dp"])
    return jax.shard_map(body, mesh=mesh, in_specs=in_specs, out_specs=out_specs, check_vma=False)
```
